32 devices in a mesh: groups: 2 (over y), dom: 8 (over z, core), tilt: 2 (over x), rep: 1.
Axes of the slice: x: 2, y: 2, z: 4, core: 2. Of those that a mesh axis runs over, the one named last changes fastest.
Arguments:
- patches: bfloat16 [4, 1024, 128, 128], P(('groups', 'tilt'), 'dom'), parts along dimension 0, may hold values from -6 to 6
- slot_view: int32 [4, 1024, 1], P(('groups', 'tilt'), 'dom'), parts along dimension 0, may hold values from 0 to 31, as said below
- slot_tilt: int32 [4, 1024], P(('groups', 'tilt'), 'dom'), parts along dimension 0, may hold values from 0 to 9
- slot_pos: bfloat16 [2, 4, 1024], P(None, ('groups', 'tilt'), 'dom'), parts along dimension 1, may hold values from 0 to 1
- defocus: bfloat16 [4, 1024], P(('groups', 'tilt'), 'dom'), parts along dimension 0, may hold values from 1 to 3
- projections: bfloat16 [64, 20, 2, 128, 128], P(('groups', 'dom'), 'tilt', None, 'rep'), parts along dimension 0, may hold values from -6 to 6
- warp_grid: float32 [40, 2, 256], P(('groups', 'tilt')), parts along dimension 0, may hold values from -6 to 6
Outputs:
- slot_terms: float32 [3, 4, 1024], P(None, ('groups', 'tilt'), 'dom'), parts along dimension 1
- new_warp: float32 [40, 2, 256], P(('groups', 'tilt')), parts along dimension 0
The draws below stay inside these ranges and needn't reach their ends.
There are 2 independent parts, one for each index of `groups`. The reference program is written for one: setup_inputs(seed, part) draws one part's arguments, and reference() takes and returns one part's arrays. A program takes and returns all parts, laid end to end along the dimension named above; each array names one. Nothing has to cross between parts.
Inputs may be any that keep to these rules, and one draw needn't show every extreme that they name: `slot_view`: view v is owned by dom index v // 4. Among the 128 slots of one device (one tilt index and one dom index) at most 24 name views of any one owner, and in every such block some owner is named exactly 24 times.
All inputs are finite; a program needn't handle non-finite values.
Results may differ from the reference program's by a relative error of at most 0.0018.
Values may be sent and summed in bfloat16 or wider, within the bound.
A program may use at most 64 MiB of HBM per device.

```python
import math
import jax
import jax.numpy as jnp
from jax import lax

PATCH = 128
GRID = 16
VIEW_DEV = 4
TILT_DEV = 10
SLOT_DEV = 128
VIEWS = 32
TILTS = 20
SLOTS = 1024
OWN_CAP = 24
NODES = 256
N_DOM = 8
N_TILT = 2


def draw_slot_view(key, part):
    block_total = N_TILT * N_DOM
    base_load = SLOT_DEV // N_DOM
    spare_load = OWN_CAP - base_load
    half_owners = N_DOM // 2
    hot_owner = jax.random.randint(jax.random.fold_in(key, 7), (), 0, N_DOM).astype(jnp.int32)

    def one_block(block_key):
        key_order, key_delta, key_shuffle, key_view = jax.random.split(block_key, 4)
        order = jax.random.permutation(key_order, N_DOM - 1).astype(jnp.int32)
        others = order + (order >= hot_owner).astype(jnp.int32)
        arrange = jnp.concatenate([hot_owner[None], others])
        delta = jax.random.randint(key_delta, (half_owners,), 0, spare_load + 1).astype(jnp.int32)
        delta = delta.at[0].set(spare_load)
        deltas = jnp.concatenate([delta, -delta])
        counts = jnp.zeros((N_DOM,), jnp.int32).at[arrange].set(base_load + deltas)
        ends = jnp.cumsum(counts)
        slot_iota = jnp.arange(SLOT_DEV, dtype=jnp.int32)
        owner = jnp.sum((ends[None, :] <= slot_iota[:, None]).astype(jnp.int32), axis=1)
        owner = owner[jax.random.permutation(key_shuffle, SLOT_DEV)]
        return owner * VIEW_DEV + jax.random.randint(key_view, (SLOT_DEV,), 0, VIEW_DEV).astype(jnp.int32)
    block_keys = jax.random.split(jax.random.fold_in(key, 3), block_total)
    views_all = jax.vmap(one_block)(block_keys)
    return views_all.reshape(N_TILT, SLOTS, 1).astype(jnp.int32)


def place_ends(array, stream_key, least, largest):
    longest = array.shape.index(max(array.shape))
    spots = []
    for shift in (0, 1):
        where = [jax.random.randint(jax.random.fold_in(stream_key, axis), (), 0, length) for axis, length in enumerate(array.shape)]
        where[longest] = (where[longest] + shift) % array.shape[longest]
        spots.append(tuple(where))
    return array.at[spots[0]].set(least).at[spots[1]].set(largest)


def levels(stream_key, extent, cuts, low, largest):
    def one(dim, parts):
        steps = jax.random.uniform(jax.random.fold_in(jax.random.fold_in(stream_key, 6), dim), (parts,), jnp.float32, low / len(cuts), largest / len(cuts))
        return jnp.repeat(jnp.exp(steps), extent[dim] // parts).reshape((-1,) + (1,) * (len(extent) - dim - 1))

    loudness = one(*cuts[0])
    for cut in cuts[1:]:
        loudness = loudness * one(*cut)
    return loudness


def gaussian(own_key, extent, scale, limit, shards=(), held_as=jnp.bfloat16):
    values = scale * jax.random.normal(own_key, extent, jnp.float32)
    if shards:
        values = values * levels(own_key, extent, shards, -0.22, 0.18)
    return jnp.clip(values, -limit, limit).astype(held_as)


def setup_inputs(seed: int = 0, part: int = 0) -> dict:
    splits = jax.random.split(jax.random.key(seed), 8)
    part_splits = jax.random.split(jax.random.fold_in(splits[7], part), 8)
    return {
        "patches": gaussian(part_splits[0], (N_TILT, SLOTS, PATCH, PATCH), 1.0, 6.0, ((0, 2), (1, 8))),
        "slot_view": draw_slot_view(jax.random.fold_in(jax.random.fold_in(splits[7], part), 71), part),
        "slot_tilt": place_ends(jax.random.randint(part_splits[2], (N_TILT, SLOTS), 0, TILT_DEV), jax.random.fold_in(part_splits[2], 1), 0, TILT_DEV - 1).astype(jnp.int32),
        "slot_pos": jnp.clip(1.0 * jax.random.uniform(part_splits[3], (2, N_TILT, SLOTS), jnp.float32) ** levels(part_splits[3], (2, N_TILT, SLOTS), ((1, 2), (2, 8)), -0.2, 0.2), 0.0, 1.0).astype(jnp.bfloat16),
        "defocus": jnp.clip(jnp.exp(math.log(3.0) - 1.0986123 * jax.random.uniform(part_splits[4], (N_TILT, SLOTS), jnp.float32) ** levels(part_splits[4], (N_TILT, SLOTS), ((0, 2), (1, 8)), -0.2, 0.2)), 1.0, 3.0).astype(jnp.bfloat16),
        "projections": gaussian(part_splits[5], (VIEWS, TILTS, 2, PATCH, PATCH), 1.0, 6.0, ((0, 8), (1, 2))),
        "warp_grid": gaussian(part_splits[6], (TILTS, 2, NODES), 1.5, 6.0, ((0, 2),), jnp.float32),
    }


AMPLITUDE = 0.07
TRUST_FLOOR = 0.02

def signed_freq(index, pixels):
    return jnp.where(index < pixels // 2, index, index - pixels).astype(jnp.float32)

def dft_tables(freq_rows, pixels):
    columns = jnp.arange(pixels, dtype=jnp.int32)
    table_scale = 1.0 / math.sqrt(pixels)
    turns_rows = (freq_rows[:, None] * columns[None, :] % pixels).astype(jnp.float32) * (2.0 * math.pi / pixels)
    turns_full = (columns[:, None] * columns[None, :] % pixels).astype(jnp.float32) * (2.0 * math.pi / pixels)
    row_table = jnp.concatenate([jnp.cos(turns_rows), jnp.sin(turns_rows)], axis=0) * table_scale
    col_table = jnp.concatenate([jnp.cos(turns_full), jnp.sin(turns_full)], axis=1) * table_scale
    return (row_table.astype(jnp.bfloat16), col_table.astype(jnp.bfloat16))

def node_weights(pos_x, pos_y, grid_side):
    knot_pos = jnp.arange(grid_side, dtype=jnp.int32).astype(jnp.float32)
    weight_x = jnp.maximum(0.0, 1.0 - jnp.abs(pos_x[:, None] * (grid_side - 1) - knot_pos[None, :]))
    weight_y = jnp.maximum(0.0, 1.0 - jnp.abs(pos_y[:, None] * (grid_side - 1) - knot_pos[None, :]))
    return (weight_y[:, :, None] * weight_x[:, None, :]).reshape(pos_x.shape[0], grid_side * grid_side)

def spectral_terms(spectrum, ref_blk, focus_blk, shift_blk, freq_rows, pixels):
    row_total = freq_rows.shape[0]
    v_one_cos = spectrum[:, :row_total, :pixels]
    v_one_sin = spectrum[:, :row_total, pixels:]
    v_two_cos = spectrum[:, row_total:, :pixels]
    v_two_sin = spectrum[:, row_total:, pixels:]
    real_part = v_one_cos - v_two_sin
    imag_part = -(v_one_sin + v_two_cos)
    freq_y = signed_freq(freq_rows, pixels)[None, :, None]
    freq_x = signed_freq(jnp.arange(pixels, dtype=jnp.int32), pixels)[None, None, :]
    nyquist = pixels / 2.0
    radius = (freq_y * freq_y + freq_x * freq_x) / (nyquist * nyquist)
    aberration = math.pi * focus_blk[:, None, None] * radius
    contrast = -(math.sqrt(1.0 - AMPLITUDE * AMPLITUDE) * jnp.sin(aberration) + AMPLITUDE * jnp.cos(aberration))
    phase_angle = 2.0 * math.pi / pixels * (freq_x * shift_blk[:, 0, None, None] + freq_y * shift_blk[:, 1, None, None])
    cosine = jnp.cos(phase_angle)
    sine_part = jnp.sin(phase_angle)
    ref_real = ref_blk[:, 0].astype(jnp.float32)
    ref_imag = ref_blk[:, 1].astype(jnp.float32)
    model_real = contrast * (ref_real * cosine + ref_imag * sine_part)
    model_imag = contrast * (ref_imag * cosine - ref_real * sine_part)
    diff_real = real_part - model_real
    diff_imag = imag_part - model_imag
    inverse_area = 1.0 / (pixels * pixels)
    energy = lax.optimization_barrier(jnp.sum(diff_real * diff_real + diff_imag * diff_imag, axis=(1, 2))) * inverse_area
    cross_term = diff_imag * model_real - diff_real * model_imag
    grad_x = 2.0 * inverse_area * lax.optimization_barrier(jnp.sum(2.0 * math.pi / pixels * freq_x * cross_term, axis=(1, 2)))
    grad_y = 2.0 * inverse_area * lax.optimization_barrier(jnp.sum(2.0 * math.pi / pixels * freq_y * cross_term, axis=(1, 2)))
    return jnp.stack([energy, grad_x, grad_y], axis=1)

def reference(patches, slot_view, slot_tilt, slot_pos, defocus, projections, warp_grid):
    slot_total = N_TILT * SLOTS
    tilt_index = (jnp.arange(N_TILT, dtype=jnp.int32)[:, None] * TILT_DEV + slot_tilt).reshape(slot_total).astype(jnp.int32)
    view_index = slot_view.reshape(slot_total).astype(jnp.int32)
    weights = node_weights(slot_pos[0].reshape(slot_total).astype(jnp.float32), slot_pos[1].reshape(slot_total).astype(jnp.float32), GRID)
    shifts = lax.optimization_barrier(jnp.sum(warp_grid[tilt_index] * weights[:, None, :], axis=2))
    focus = defocus.reshape(slot_total).astype(jnp.float32)
    freq_rows = jnp.arange(PATCH, dtype=jnp.int32)
    row_table, col_table = dft_tables(freq_rows, PATCH)
    block_len = math.gcd(slot_total, 32)
    block_count = slot_total // block_len

    def one_block(inputs):
        patch_blk, view_blk, tilt_blk, focus_blk, shift_blk = inputs
        ref_blk = projections[view_blk, tilt_blk]
        first_pass = jnp.einsum('fy,byx->bfx', row_table.astype(jnp.float32), patch_blk.astype(jnp.float32)).astype(jnp.bfloat16)
        spectrum = jnp.einsum('bfx,xk->bfk', first_pass.astype(jnp.float32), col_table.astype(jnp.float32))
        return spectral_terms(spectrum, ref_blk, focus_blk, shift_blk, freq_rows, PATCH)
    per_slot = lax.map(one_block, (patches.reshape(block_count, block_len, PATCH, PATCH), view_index.reshape(block_count, block_len), tilt_index.reshape(block_count, block_len), focus.reshape(block_count, block_len), shifts.reshape(block_count, block_len, 2))).reshape(slot_total, 3)
    slot_terms = per_slot.T.reshape(3, N_TILT, SLOTS)
    tilt_hits = (tilt_index[:, None] == jnp.arange(TILTS, dtype=jnp.int32)[None, :]).astype(jnp.float32)
    node_coef = (tilt_hits[:, :, None] * per_slot[:, None, 1:3]).reshape(slot_total, 2 * TILTS)
    gradient = jnp.dot(node_coef.T, weights, precision=lax.Precision.HIGHEST, preferred_element_type=jnp.float32).reshape(TILTS, 2, NODES)
    new_warp = warp_grid - gradient / jnp.sqrt(gradient * gradient + TRUST_FLOOR * TRUST_FLOOR)
    return (slot_terms, new_warp)
```

```python
import functools
import math

import jax
import jax.numpy as jnp
import numpy as np
from jax import lax
from jax.experimental import pallas as pl
from jax.experimental.pallas import tpu as pltpu
from jax.sharding import PartitionSpec as P

GRID = 16


AMPLITUDE = 0.07
TRUST_FLOOR = 0.02


def signed_freq(index, pixels):
    return jnp.where(index < pixels // 2, index, index - pixels).astype(jnp.float32)


def dft_tables(freq_rows, pixels):
    columns = jnp.arange(pixels, dtype=jnp.int32)
    table_scale = 1.0 / math.sqrt(pixels)
    turns_rows = (freq_rows[:, None] * columns[None, :] % pixels).astype(jnp.float32) * (
        2.0 * math.pi / pixels
    )
    turns_full = (columns[:, None] * columns[None, :] % pixels).astype(jnp.float32) * (
        2.0 * math.pi / pixels
    )
    row_table = jnp.concatenate([jnp.cos(turns_rows), jnp.sin(turns_rows)], axis=0) * table_scale
    col_table = jnp.concatenate([jnp.cos(turns_full), jnp.sin(turns_full)], axis=1) * table_scale
    return (row_table.astype(jnp.bfloat16), col_table.astype(jnp.bfloat16))


def node_weights(pos_x, pos_y, grid_side):
    knot_pos = jnp.arange(grid_side, dtype=jnp.int32).astype(jnp.float32)
    weight_x = jnp.maximum(0.0, 1.0 - jnp.abs(pos_x[:, None] * (grid_side - 1) - knot_pos[None, :]))
    weight_y = jnp.maximum(0.0, 1.0 - jnp.abs(pos_y[:, None] * (grid_side - 1) - knot_pos[None, :]))
    return (weight_y[:, :, None] * weight_x[:, None, :]).reshape(
        pos_x.shape[0], grid_side * grid_side
    )


def spectral_terms(spectrum, ref_blk, focus_blk, shift_blk, freq_rows, pixels):
    row_total = freq_rows.shape[0]
    v_one_cos = spectrum[:, :row_total, :pixels]
    v_one_sin = spectrum[:, :row_total, pixels:]
    v_two_cos = spectrum[:, row_total:, :pixels]
    v_two_sin = spectrum[:, row_total:, pixels:]
    real_part = v_one_cos - v_two_sin
    imag_part = -(v_one_sin + v_two_cos)
    freq_y = signed_freq(freq_rows, pixels)[None, :, None]
    freq_x = signed_freq(jnp.arange(pixels, dtype=jnp.int32), pixels)[None, None, :]
    nyquist = pixels / 2.0
    radius = (freq_y * freq_y + freq_x * freq_x) / (nyquist * nyquist)
    aberration = math.pi * focus_blk[:, None, None] * radius
    contrast = -(
        math.sqrt(1.0 - AMPLITUDE * AMPLITUDE) * jnp.sin(aberration)
        + AMPLITUDE * jnp.cos(aberration)
    )
    phase_angle = (
        2.0
        * math.pi
        / pixels
        * (freq_x * shift_blk[:, 0, None, None] + freq_y * shift_blk[:, 1, None, None])
    )
    cosine = jnp.cos(phase_angle)
    sine_part = jnp.sin(phase_angle)
    ref_real = ref_blk[:, 0].astype(jnp.float32)
    ref_imag = ref_blk[:, 1].astype(jnp.float32)
    model_real = contrast * (ref_real * cosine + ref_imag * sine_part)
    model_imag = contrast * (ref_imag * cosine - ref_real * sine_part)
    diff_real = real_part - model_real
    diff_imag = imag_part - model_imag
    inverse_area = 1.0 / (pixels * pixels)
    energy = jnp.sum(diff_real * diff_real + diff_imag * diff_imag, axis=(1, 2)) * inverse_area
    cross_term = diff_imag * model_real - diff_real * model_imag
    grad_x = 2.0 * inverse_area * jnp.sum(2.0 * math.pi / pixels * freq_x * cross_term, axis=(1, 2))
    grad_y = 2.0 * inverse_area * jnp.sum(2.0 * math.pi / pixels * freq_y * cross_term, axis=(1, 2))
    return jnp.stack([energy, grad_x, grad_y], axis=1)


def on_device(patches, slot_view, slot_tilt, slot_pos, defocus, projections, warp_grid):
    owners = lax.axis_size("dom")
    slot_count = patches.shape[1]
    pixels = patches.shape[-1]
    view_dev = projections.shape[0]
    tilt_dev = warp_grid.shape[0]
    node_count = warp_grid.shape[2]
    capacity = 3 * slot_count // (2 * owners)
    buffer_len = owners * capacity
    chosen_view = slot_view[0, :, 0]
    owner_of = chosen_view // view_dev
    owner_hits = (owner_of[:, None] == jnp.arange(owners, dtype=jnp.int32)[None, :]).astype(
        jnp.int32
    )
    earlier = jnp.cumsum(owner_hits, axis=0) - owner_hits
    slot_rank = jnp.sum(earlier * owner_hits, axis=1)
    target = owner_of * capacity + slot_rank
    matches = target[None, :] == jnp.arange(buffer_len, dtype=jnp.int32)[:, None]
    source = jnp.sum(
        jnp.where(matches, jnp.arange(slot_count, dtype=jnp.int32)[None, :], 0), axis=1
    )
    filled = jnp.any(matches, axis=1)
    patch_rows = jnp.where(filled[:, None, None], patches[0][source], jnp.zeros((), jnp.bfloat16))
    slot_meta = jnp.stack(
        [
            slot_tilt[0].astype(jnp.float32),
            (chosen_view % view_dev).astype(jnp.float32),
            defocus[0].astype(jnp.float32),
            slot_pos[0, 0].astype(jnp.float32),
            slot_pos[1, 0].astype(jnp.float32),
            jnp.ones((slot_count,), jnp.float32),
        ],
        axis=1,
    )
    meta_rows = jnp.where(filled[:, None], slot_meta[source], 0.0).astype(jnp.bfloat16)
    patch_buffer = patch_rows.reshape(owners, capacity, pixels, pixels)
    meta_buffer = meta_rows.reshape(owners, capacity, 6)
    row_span = projections.shape[3]
    freq_rows = lax.axis_index("rep") * row_span + jnp.arange(row_span, dtype=jnp.int32)
    row_table, col_table = dft_tables(freq_rows, pixels)
    row_total = freq_rows.shape[0]
    projected_flat = projections.reshape(view_dev * tilt_dev, 2, row_total, pixels)
    tilt_iota = jnp.arange(tilt_dev, dtype=jnp.int32)
    view_iota = jnp.arange(view_dev, dtype=jnp.int32)

    def one_block(inputs):
        patch_blk, index_blk, focus_blk, shift_blk = inputs
        ref_blk = projected_flat[index_blk]
        first_pass = jnp.einsum(
            "fy,byx->bfx", row_table, patch_blk, preferred_element_type=jnp.float32
        ).astype(jnp.bfloat16)
        spectrum = jnp.einsum(
            "bfx,xk->bfk", first_pass, col_table, preferred_element_type=jnp.float32
        )
        return spectral_terms(spectrum, ref_blk, focus_blk, shift_blk, freq_rows, pixels)

    patch_in = lax.all_to_all(patch_buffer, "dom", split_axis=0, concat_axis=0, tiled=True)
    meta_in = lax.all_to_all(meta_buffer, "dom", split_axis=0, concat_axis=0, tiled=True)
    senders = patch_in.shape[0]
    per_sender = patch_in.shape[1]
    slot_total = senders * per_sender
    meta_flat = meta_in.reshape(slot_total, 6).astype(jnp.float32)
    tilt_match = meta_flat[:, 0:1] == tilt_iota.astype(jnp.float32)[None, :]
    view_match = meta_flat[:, 1:2] == view_iota.astype(jnp.float32)[None, :]
    tilt_local = jnp.sum(jnp.where(tilt_match, tilt_iota[None, :], 0), axis=1)
    view_local = jnp.sum(jnp.where(view_match, view_iota[None, :], 0), axis=1)
    weights = node_weights(meta_flat[:, 3], meta_flat[:, 4], GRID)
    shifts = jnp.sum(warp_grid[tilt_local] * weights[:, None, :], axis=2)
    block_len = math.gcd(slot_total, 16)
    block_count = slot_total // block_len
    per_slot = lax.map(
        one_block,
        (
            patch_in.reshape(block_count, block_len, pixels, pixels),
            (view_local * tilt_dev + tilt_local).reshape(block_count, block_len),
            meta_flat[:, 2].reshape(block_count, block_len),
            shifts.reshape(block_count, block_len, 2),
        ),
    ).reshape(slot_total, 3)
    node_coef = (
        tilt_match.astype(jnp.float32)[:, :, None]
        * per_slot[:, None, 1:3]
        * meta_flat[:, 5, None, None]
    ).reshape(senders, per_sender, 2 * tilt_dev)
    returned = lax.all_to_all(
        per_slot.reshape(senders, per_sender, 3), "dom", split_axis=0, concat_axis=0, tiled=True
    )
    weight_all = weights.reshape(senders, per_sender, node_count)
    own_terms = returned.reshape(buffer_len, 3)[target]
    summed = lax.psum(own_terms, "rep")
    slot_terms = summed.T[:, None, :]
    gradient = jnp.dot(
        node_coef.reshape(-1, 2 * tilt_dev).T,
        weight_all.reshape(-1, node_count),
        precision=lax.Precision.HIGHEST,
        preferred_element_type=jnp.float32,
    ).reshape(tilt_dev, 2, node_count)
    whole_grad = lax.psum(gradient, ("dom", "rep"))
    new_warp = warp_grid - whole_grad / jnp.sqrt(
        whole_grad * whole_grad + TRUST_FLOOR * TRUST_FLOOR
    )
    return (slot_terms, new_warp)


CORES = 2
CHIPS = 4
EXTRA_ROWS = 8
SPEC_ROWS = 16
GUEST_CHUNKS = 4
DELTA = math.asin(AMPLITUDE)
F32 = jnp.float32
BF16 = jnp.bfloat16
OWN, NEAR, CROSS, ON_FAR, ON_OPP, NEAR_PAIR, OPP_PAIR, FAR_PAIR = range(8)


def exact(a, b, dims=(((1,), (0,)), ((), ()))):
    return lax.dot_general(
        a, b, dims, precision=lax.Precision.HIGHEST, preferred_element_type=F32
    )


def contract_last(a, b):
    return lax.dot_general(a, b, (((1,), (1,)), ((), ())), preferred_element_type=F32)


def tables(pixels):
    half = pixels // 2
    k = np.arange(pixels)
    angle = ((k[:, None] * k[None, :]) % pixels).astype(np.float32) * np.float32(
        2.0 * math.pi / pixels
    )
    scale = np.float32(1.0 / math.sqrt(pixels))
    cosine, sine = np.cos(angle) * scale, np.sin(angle) * scale
    pad = np.zeros((SPEC_ROWS - 2, pixels), np.float32)
    edge_c, edge_s = cosine[half : half + 1], sine[half : half + 1]
    first = np.concatenate(
        [cosine[:half], edge_c, edge_c, pad, sine[:half], edge_s, edge_s, pad], axis=0
    )
    second = np.concatenate(
        [np.concatenate([cosine, -sine], axis=1), np.concatenate([-sine, -cosine], axis=1)], axis=0
    )
    edge = np.zeros((SPEC_ROWS, pixels), np.float32)
    edge[2:4] = edge_c
    turn = ((k[:half, None] + k[None, :] == pixels) & (k[:half, None] > 0)).astype(np.float32)
    flip = (((k[:, None] + k[None, :]) % pixels == 0) & (k != half)[None, :]).astype(np.float32)
    unit = np.broadcast_to((k == half).astype(np.float32)[None, :], (16, pixels))
    table = np.arange(2 * pixels)
    focus = np.where(table < pixels, 1.0 + table / pixels, 2.0 + (table - pixels) / half)
    freq = np.where(k < half, k, k - pixels).astype(np.float64)
    chi = 2.0 * math.pi * focus[None, :] * (freq * freq / (half * half))[:, None]
    waves = np.concatenate([np.cos(chi), np.sin(chi)], axis=1)
    levels = np.concatenate([np.cos(chi + 2.0 * DELTA), -np.sin(chi + 2.0 * DELTA)], axis=1)
    low = [jnp.asarray(x, BF16) for x in (first, second, edge, turn, flip, unit, waves)]
    return low + [jnp.asarray(levels, F32)]


def fold_reference(pixels, real, imag, turn, flip, unit, waves, levels):
    half = pixels // 2
    lane = lax.broadcasted_iota(jnp.int32, (1, pixels), 1)
    turned = jnp.dot(turn, jnp.concatenate([real, imag], axis=1), preferred_element_type=F32)
    turned = jnp.concatenate([turned[:, :pixels], turned[:, pixels:]], axis=0).astype(BF16)
    mirror = jnp.dot(turned, flip, preferred_element_type=F32)
    r, i = real.astype(F32), imag.astype(F32)
    column = contract_last(unit, jnp.concatenate([real, imag], axis=0))[0:1]
    column = jnp.where(jnp.concatenate([lane, lane], axis=1) > half, column, 0.0)
    power = r * r + i * i
    mixed = jnp.dot(power.astype(BF16), waves, preferred_element_type=F32)
    swing = jnp.sum(mixed * levels, axis=0, keepdims=True)
    swing = swing[:, : 2 * pixels] + swing[:, 2 * pixels :]
    total = 0.5 * jnp.sum(power) - 0.5 * swing
    high = total.astype(BF16).astype(F32)
    low = total - high
    extra = jnp.concatenate(
        [
            r[half : half + 1], i[half : half + 1], column[:, :pixels], column[:, pixels:],
            high[:, :pixels], high[:, pixels:], low[:, :pixels], low[:, pixels:],
        ],
        axis=0,
    )
    return (r[:half] + mirror[:half]).astype(BF16), (i[:half] - mirror[half:]).astype(BF16), extra


def gather_kernel(cap, view_dev, chunks, view_ref, tilt_ref, pos_ref, focus_ref, warp_ref,
                  patch_hbm, proj_hbm, first_ref, second_ref, edge_ref, turn_ref, flip_ref,
                  unit_ref, waves_ref, levels_ref, terms_ref, new_ref, patch_ref, proj_ref,
                  own_ref, pair_ref, near_ref, near_pair_ref, opp_ref, opp_pair_ref, far_ref,
                  far_pair_ref, guest_ref, visit_ref, spec_ref, factor_ref, cols_ref, node_ref,
                  match_ref, sums_ref, visit_sums_ref, ints_ref, visit_ints_ref, ints_s,
                  visit_ints_s, grad_ref, held_ref, back_ref, back_in_ref, load_sem, send_sem,
                  recv_sem, guest_send, guest_recv, misc_send, misc_recv, grad_send, grad_recv):
    slots, pixels = patch_ref.shape[0], patch_ref.shape[1]
    half = pixels // 2
    refs = own_ref.shape[0]
    tilt_dev = warp_ref.shape[0]
    node_count = warp_ref.shape[2]
    per = refs // chunks
    guests = guest_ref.shape[0]
    per_guest = guests // GUEST_CHUNKS
    devices = CHIPS * CORES
    padded = devices * cap
    far_base = padded - guests
    wide = sums_ref.shape[1]
    me = lax.axis_index("dom")
    chip = me // CORES
    core = me % CORES
    partner = chip * CORES + (1 - core)
    mate_chip = chip + 1 - 2 * (chip % 2)
    mate = mate_chip * CORES + core
    cross = (CHIPS - 1 - chip) * CORES + core
    inner = (chip > 0) & (chip < CHIPS - 1)
    outer = jnp.logical_not(inner)
    barrier = pltpu.get_barrier_semaphore()
    for hop in range(1, devices):
        pl.semaphore_signal(
            barrier, inc=1, device_id={"dom": lax.rem(me + hop, devices)},
            device_id_type=pl.DeviceIdType.MESH,
        )

    def load_proj(c):
        rows = pl.ds(c * per, per)
        return pltpu.make_async_copy(proj_hbm.at[rows], proj_ref.at[rows], load_sem.at[c])

    load_patch = pltpu.make_async_copy(patch_hbm, patch_ref, load_sem.at[chunks])
    for c in range(chunks):
        load_proj(c).start()
    load_patch.start()

    def remote(src, dst, send, recv, target):
        return pltpu.make_async_remote_copy(
            src_ref=src, dst_ref=dst, send_sem=send, recv_sem=recv,
            device_id={"dom": target}, device_id_type=pl.DeviceIdType.MESH,
        )

    flows = {
        OWN: (own_ref, pair_ref, partner),
        NEAR: (own_ref, near_ref, mate),
        CROSS: (own_ref, opp_ref, cross),
        ON_FAR: (near_ref, far_ref, cross),
        ON_OPP: (opp_ref, opp_ref, mate),
        NEAR_PAIR: (near_ref, near_pair_ref, partner),
        OPP_PAIR: (opp_ref, opp_pair_ref, partner),
        FAR_PAIR: (far_ref, far_pair_ref, partner),
    }

    def flow(kind, c):
        src, dst, target = flows[kind]
        rows = pl.ds(c * per, per)
        return remote(
            src.at[rows], dst.at[rows], send_sem.at[kind, c], recv_sem.at[kind, c], target
        )

    def guest_copy(g):
        rows = pl.ds(g * per_guest, per_guest)
        return remote(
            guest_ref.at[rows], visit_ref.at[rows], guest_send.at[g], guest_recv.at[g], mate
        )

    ints_copy = remote(ints_ref, visit_ints_ref, misc_send.at[0], misc_recv.at[0], mate)
    back_copy = remote(back_ref, back_in_ref, misc_send.at[1], misc_recv.at[1], mate)

    def fold(c):
        load_proj(c).wait()

        def one(i, carry):
            n = c * per + i
            top, bottom, extra = fold_reference(
                pixels, proj_ref[n, 0], proj_ref[n, 1], turn_ref[...], flip_ref[...],
                unit_ref[...], waves_ref[...], levels_ref[...],
            )
            own_ref[n, :half] = top
            own_ref[n, half:pixels] = bottom
            own_ref[n, pixels:] = extra.astype(BF16)
            return carry

        lax.fori_loop(0, per, one, 0, unroll=2)

    def send_own(c):
        flow(NEAR, c).start()

        @pl.when(inner)
        def _():
            flow(CROSS, c).start()

        flow(OWN, c).start()

    lane = lax.broadcasted_iota(jnp.int32, (1, pixels), 1)
    line = jnp.where(lane < half, lane, lane - pixels).astype(F32)
    lane_f = lane.astype(F32)

    def route():
        chip_f, core_f, mate_f = chip.astype(F32), core.astype(F32), mate_chip.astype(F32)
        opp_f = (CHIPS - 1) - jnp.where(inner, chip_f, mate_f)
        view = view_ref[...].astype(F32)
        owner = jnp.floor((view + 0.5) * (1.0 / view_dev))
        owner_chip = jnp.floor((owner + 0.5) * (1.0 / CORES))
        owner_core = owner - CORES * owner_chip
        role = jnp.where(
            owner_chip == chip_f, 0.0,
            jnp.where(owner_chip == mate_f, 1.0, jnp.where(owner_chip == opp_f, 2.0, 3.0)),
        )
        key = role * CORES + jnp.where(owner_core == core_f, 0.0, 1.0)
        tilt = tilt_ref[...].astype(F32)
        which = (view - owner * view_dev) * tilt_dev + tilt
        pos = pos_ref[...].astype(F32)
        block = jnp.concatenate(
            [key, which, pos, focus_ref[...].astype(F32), tilt,
             jnp.zeros((slots - 6, slots), F32)],
            axis=0,
        )
        cols = block.T
        cols_ref[...] = cols
        row = lax.broadcasted_iota(jnp.int32, (slots, slots), 0)
        col = lax.broadcasted_iota(jnp.int32, (slots, slots), 1)
        ahead = jnp.where((cols[:, 0:1] == key) & (col < row), 1.0, 0.0)
        target = cols[:, 0:1] * cap + jnp.sum(ahead, axis=1, keepdims=True)
        place = lax.broadcasted_iota(jnp.int32, (1, wide), 1).astype(F32)
        match = jnp.where(target == place, 1.0, 0.0)
        match_ref[...] = match
        slot = lax.broadcasted_iota(jnp.int32, (slots, wide), 0).astype(F32)
        source = jnp.sum(match * slot, axis=0, keepdims=True)
        chosen = jnp.sum(match * cols[:, 1:2], axis=0, keepdims=True)
        ints = jnp.concatenate([source, chosen, jnp.zeros((6, wide), F32)], axis=0)
        ints_ref[...] = (ints + 0.5).astype(jnp.int32)

    def place_nodes():
        node = lax.broadcasted_iota(jnp.int32, (1, node_count), 1).astype(F32)
        node_y = jnp.floor((node + 0.5) * (1.0 / GRID))
        node_x = node - node_y * GRID
        weight_x = jnp.maximum(0.0, 1.0 - jnp.abs(cols_ref[:, 2:3] * (GRID - 1) - node_x))
        weight_y = jnp.maximum(0.0, 1.0 - jnp.abs(cols_ref[:, 3:4] * (GRID - 1) - node_y))
        weights = weight_y * weight_x
        node_ref[...] = weights
        hits = jnp.where(cols_ref[:, 5:6] == lane_f[:, :16], 1.0, 0.0)
        spare = jnp.zeros((16 - tilt_dev, node_count), F32)
        for axis in range(2):
            grid = jnp.concatenate([warp_ref[:, axis, :], spare], axis=0)
            shift = jnp.sum(exact(hits, grid) * weights, axis=1, keepdims=True)
            cols_ref[:, 6 + axis : 7 + axis] = shift

    step_angle = 2.0 * math.pi / pixels
    norm = 1.0 / (half * half)
    block_slots = 16

    def factors(block, carry):
        rows = pl.ds(pl.multiple_of(block * block_slots, block_slots), block_slots)
        cols = cols_ref[rows]
        focus, shift_x, shift_y = cols[:, 4:5], cols[:, 6:7], cols[:, 7:8]
        chi = math.pi * focus * (line * line * norm)
        phi_x = step_angle * shift_x * line
        phi_y = step_angle * shift_y * line
        c_x, s_x = jnp.cos(chi), jnp.sin(chi)
        s_y = s_x * math.cos(DELTA) + c_x * math.sin(DELTA)
        c_y = c_x * math.cos(DELTA) - s_x * math.sin(DELTA)
        p_x, q_x, p_y, q_y = jnp.cos(phi_x), jnp.sin(phi_x), jnp.cos(phi_y), jnp.sin(phi_y)
        tall = (s_y * p_y, s_y * q_y, c_y * p_y, c_y * q_y)
        a, b, c, d = c_x * p_x, c_x * q_x, s_x * p_x, s_x * q_x
        e, f, g, h = (v[:, half : half + 1] for v in (a, b, c, d))
        edge_re = -(tall[0] * e - tall[1] * f + tall[2] * g - tall[3] * h)
        edge_im = -(tall[0] * f + tall[1] * e + tall[2] * h + tall[3] * g)
        tall = tuple(jnp.where(lane == half + 1, pltpu.roll(v, 1, 1), v) for v in tall)
        place = jnp.where(focus < 2.0, (focus - 1.0) * pixels, pixels + (focus - 2.0) * half)
        hit_low = jnp.where(place == lane_f, -0.5, 0.0)
        hit_high = jnp.where(place == lane_f + pixels, -0.5, 0.0)
        zero = jnp.zeros_like(a)
        values = tall + (a, b, c, d, edge_re, edge_im, zero, zero,
                         hit_low, hit_high, hit_low, hit_high)
        for index, value in enumerate(values):
            factor_ref[rows, index] = value
        return carry

    row8 = lax.broadcasted_iota(jnp.int32, (8, pixels), 0)
    main_rows = half + SPEC_ROWS

    def spectra(indices, put):
        count = len(indices)
        blocks = [patch_ref[s] for s in indices]
        wides = []
        for n in range(0, count, 2):
            both = jnp.concatenate(blocks[n : n + 2], axis=1)
            v = jnp.dot(first_ref[...], both, preferred_element_type=F32)
            edge = contract_last(edge_ref[...], jnp.concatenate(blocks[n : n + 2], axis=0))
            for part in range(2):
                at = slice(part * pixels, (part + 1) * pixels)
                one = jnp.concatenate([v[:half, at], v[half:main_rows, at] + edge[:, at]], axis=0)
                wides.append(
                    jnp.concatenate([one.astype(BF16), v[main_rows:, at].astype(BF16)], axis=1)
                )
        spectrum = jnp.dot(
            jnp.concatenate(wides, axis=0), second_ref[...], preferred_element_type=F32
        )
        for n in range(count):
            factor = factor_ref[indices[n]]
            tall = factor[0:4]
            a, b, c, d = factor[4:5], factor[5:6], factor[6:7], factor[7:8]
            rows = jnp.concatenate(
                [
                    jnp.concatenate([-a, b, -c, d], axis=0),
                    jnp.concatenate([-b, -a, -d, -c], axis=0),
                ],
                axis=1,
            )
            tall_high = tall.astype(BF16).astype(F32)
            row_high = rows.astype(BF16).astype(F32)
            tall_low, row_low = tall - tall_high, rows - row_high
            tall_all = jnp.concatenate(
                [tall_high, tall_high, tall_low, jnp.zeros_like(tall_low)], axis=0
            ).astype(BF16)
            row_all = jnp.concatenate(
                [row_high, row_low, row_high, jnp.zeros_like(row_low)], axis=0
            ).astype(BF16)
            turn = lax.dot_general(
                tall_all, row_all, (((0,), (0,)), ((), ())), preferred_element_type=F32
            )
            base = n * main_rows
            x_re = spectrum[base : base + half, :pixels]
            x_im = spectrum[base : base + half, pixels:]
            t_re, t_im = turn[:half, :pixels], turn[:half, pixels:]
            put(n, slice(0, half), x_re * t_re - x_im * t_im)
            put(n, slice(half, pixels), x_re * t_im + x_im * t_re)
            power = x_re * x_re + x_im * x_im
            power = jnp.sum(power.reshape(half // 8, 8, pixels), axis=0) * 2.0 - jnp.where(
                row8 == 0, power[:8], 0.0
            )
            x_re = spectrum[base + half : base + half + 8, :pixels]
            x_im = spectrum[base + half : base + half + 8, pixels:]
            power = power + jnp.where(row8 == 0, x_re * x_re + x_im * x_im, 0.0)
            edge_turn = (row8 == 2) | (row8 == 3)
            t_re = jnp.where(edge_turn, factor[8:9], turn[half : half + 8, :pixels])
            t_im = jnp.where(edge_turn, factor[9:10], turn[half : half + 8, pixels:])
            y_re = x_re * t_re - x_im * t_im
            y_im = x_re * t_im + x_im * t_re
            odd = row8 % 2 == 1
            straight = jnp.where(odd, y_im, y_re)
            crossed = jnp.where(odd, -y_re, y_im)
            straight = jnp.where(row8 < 4, straight, factor[8:16])
            power = jnp.sum(power, axis=0, keepdims=True)
            high = power.astype(BF16).astype(F32)
            crossed = jnp.where(
                row8 < 4, crossed,
                jnp.where(row8 == 4, high, jnp.where(row8 == 5, power - high, 0.0)),
            )
            put(n, slice(pixels, pixels + 16), jnp.concatenate([straight, crossed], axis=0))

    weight_x = jnp.where(row8 < 2, line, jnp.where(row8 < 4, -float(half), 0.0))
    weight_y = jnp.where(row8 < 2, -float(half), jnp.where(row8 < 4, line, 0.0))
    freq_y = lax.broadcasted_iota(jnp.int32, (half, pixels), 0).astype(F32)

    def stack(x):
        return jnp.sum(x.reshape(half // 8, 8, pixels), axis=0)

    def meet(y, ref, out_ref, place):
        y = y.astype(F32)
        r = ref.astype(F32)
        y_re, y_im, straight = y[:half], y[half:pixels], y[pixels : pixels + 8]
        crossed = y[pixels + 8 :]
        r_re, r_im, extra = r[:half], r[half:pixels], r[pixels:]
        match = stack(y_re * r_re + y_im * r_im) + straight * extra
        swirl = y_im * r_re - y_re * r_im
        edge = crossed * extra
        energy = jnp.where((row8 == 4) | (row8 == 5), crossed, 0.0) - 2.0 * match
        grad_x = stack(swirl) * line + edge * weight_x
        grad_y = stack(swirl * freq_y) + edge * weight_y
        for index, value in enumerate((energy, grad_x, grad_y)):
            out_ref[index, pl.ds(place, 1)] = jnp.sum(value, axis=0, keepdims=True)

    def slot_at(p):
        return jnp.clip(ints_s[0, p], 0, slots - 1)

    def ref_at(held, p):
        return jnp.clip(held[1, p], 0, refs - 1)

    def process(refs_ref, role):
        def some(step, carry):
            for u in range(4):
                p = role * cap + step * 4 + u
                meet(spec_ref[slot_at(p)], refs_ref[ref_at(ints_s, p)], sums_ref, p)
            return carry

        lax.fori_loop(0, cap // 4, some, 0)

    def entertain(refs_ref, part):
        def some(step, carry):
            for u in range(4):
                g = part * cap + step * 4 + u
                p = far_base + g
                place = p - (wide - pixels)
                meet(visit_ref[g], refs_ref[ref_at(visit_ints_s, p)], visit_sums_ref, place)
            return carry

        lax.fori_loop(0, cap // 4, some, 0)

    def transform(low, high):
        def some(step, carry):
            base = low + step * 4

            def put(n, rows, value):
                spec_ref[base + n, rows] = value

            spectra([base + n for n in range(4)], put)
            return carry

        lax.fori_loop(0, (high - low) // 4, some, 0)

    def transform_guests(low, high):
        def some(step, carry):
            base = low + step * 4

            def put(n, rows, value):
                guest_ref[base + n, rows] = value.astype(BF16)

            spectra([slot_at(far_base + base + n) for n in range(4)], put)
            return carry

        lax.fori_loop(0, (high - low) // 4, some, 0)

    fold(0)
    pl.semaphore_wait(barrier, devices - 1)
    route()
    send_own(0)
    for c in range(1, chunks):
        fold(c)
        if c > 1:
            send_own(c - 1)
    ints_load = pltpu.make_async_copy(ints_ref, ints_s, load_sem.at[chunks + 1])
    ints_load.start()

    @pl.when(outer)
    def _():
        ints_copy.start()

    sums_ref[...] = jnp.zeros_like(sums_ref)
    visit_sums_ref[...] = jnp.zeros_like(visit_sums_ref)
    place_nodes()
    if chunks > 1:
        send_own(chunks - 1)
    lax.fori_loop(0, slots // block_slots, factors, 0)
    load_patch.wait()
    ints_load.wait()

    @pl.when(outer)
    def _():
        for g in range(GUEST_CHUNKS):
            transform_guests(g * per_guest, (g + 1) * per_guest)
            if g > 0:
                guest_copy(g - 1).start()

    def pass_on(c):
        flow(NEAR, c).wait_recv()

        @pl.when(inner)
        def _():
            flow(ON_FAR, c).start()
            flow(CROSS, c).wait_recv()
            flow(ON_OPP, c).start()
            flow(OPP_PAIR, c).start()

        flow(NEAR_PAIR, c).start()

    segments = 4
    seg = slots // segments
    done = 0
    for n in range(segments):
        transform(n * seg, (n + 1) * seg)
        if n == 0:
            @pl.when(outer)
            def _():
                guest_copy(GUEST_CHUNKS - 1).start()
        upto = chunks * (n + 1) // segments
        while done < upto:
            pass_on(done)
            done += 1

    process(own_ref, 0)
    for c in range(chunks):
        flow(OWN, c).wait_recv()
    process(pair_ref, 1)
    process(near_ref, 2)
    for c in range(chunks):
        flow(NEAR_PAIR, c).wait_recv()
    process(near_pair_ref, 3)

    @pl.when(outer)
    def _():
        for c in range(chunks):
            flow(ON_OPP, c).wait_recv()
            flow(OPP_PAIR, c).start()

    process(opp_ref, 4)
    for c in range(chunks):
        flow(OPP_PAIR, c).wait_recv()
    process(opp_pair_ref, 5)

    visit_load = pltpu.make_async_copy(visit_ints_ref, visit_ints_s, load_sem.at[chunks + 2])
    ones = jnp.ones((8, pixels), F32)

    @pl.when(inner)
    def _():
        ints_copy.wait_recv()
        visit_load.start()
        visit_load.wait()
        for c in range(chunks):
            flow(ON_FAR, c).wait_recv()
            flow(FAR_PAIR, c).start()
        process(far_ref, 6)
        for c in range(chunks):
            flow(FAR_PAIR, c).wait_recv()
        process(far_pair_ref, 7)
        for g in range(GUEST_CHUNKS):
            guest_copy(g).wait_recv()
        entertain(far_ref, 0)
        entertain(far_pair_ref, 1)
        parts = [exact(ones, visit_sums_ref[k], (((1,), (1,)), ((), ()))) for k in range(3)]
        back_ref[...] = jnp.where(row8 == 0, parts[0], jnp.where(row8 == 1, parts[1], parts[2]))
        back_copy.start()

    parts = [exact(ones, sums_ref[k], (((1,), (1,)), ((), ()))) for k in range(3)]
    row_wide = lax.broadcasted_iota(jnp.int32, (8, wide), 0)
    mixed = jnp.where(row_wide == 0, parts[0], jnp.where(row_wide == 1, parts[1], parts[2]))
    cols_ref[:8, :] = jnp.zeros((8, slots), F32)

    @pl.when(outer)
    def _():
        back_copy.wait_recv()
        cols_ref[:8, :] = back_in_ref[...]

    mixed = jnp.concatenate(
        [mixed[:, : wide - pixels], mixed[:, wide - pixels :] + cols_ref[:8, :]], axis=1
    )
    area = 1.0 / (pixels * pixels)
    mixed = mixed * jnp.where(row_wide == 0, area, 2.0 * area * step_angle)
    terms = exact(mixed, match_ref[...], (((1,), (1,)), ((), ())))
    terms_ref[...] = terms[:3]
    row16 = lax.broadcasted_iota(jnp.int32, (16, slots), 0)
    on_tilt = row16 == tilt_ref[...]
    for axis in range(2):
        coef = jnp.where(on_tilt, terms[1 + axis : 2 + axis], 0.0)
        grad = exact(coef, node_ref[...])
        grad_ref[:, axis * node_count : (axis + 1) * node_count] = grad[:tilt_dev]

    def grad_copy(hop):
        return remote(
            grad_ref, held_ref.at[hop - 1], grad_send.at[hop - 1], grad_recv.at[hop - 1],
            lax.rem(me + hop, devices),
        )

    for hop in range(1, devices):
        grad_copy(hop).start()
    for c in range(chunks):
        flow(OWN, c).wait_send()
        flow(NEAR, c).wait_send()
        flow(NEAR_PAIR, c).wait_send()
        flow(OPP_PAIR, c).wait_send()

    @pl.when(inner)
    def _():
        for c in range(chunks):
            flow(CROSS, c).wait_send()
            flow(ON_FAR, c).wait_send()
            flow(ON_OPP, c).wait_send()
            flow(FAR_PAIR, c).wait_send()
        back_copy.wait_send()

    @pl.when(outer)
    def _():
        ints_copy.wait_send()
        for g in range(GUEST_CHUNKS):
            guest_copy(g).wait_send()

    for hop in range(1, devices):
        grad_copy(hop).wait()
    total = grad_ref[...]
    for hop in range(1, devices):
        total = total + held_ref[hop - 1]
    change = total / jnp.sqrt(total * total + TRUST_FLOOR * TRUST_FLOOR)
    for axis in range(2):
        at = slice(axis * node_count, (axis + 1) * node_count)
        new_ref[:, axis, :] = warp_ref[:, axis, :] - change[:, at]


def on_device_gathered(
    patches, slot_view, slot_tilt, slot_pos, defocus, projections, warp_grid
):
    pixels = patches.shape[-1]
    slots = patches.shape[1]
    view_dev = projections.shape[0]
    tilt_dev = warp_grid.shape[0]
    node_count = warp_grid.shape[2]
    devices = CHIPS * CORES
    cap = 3 * slots // (2 * devices)
    refs = view_dev * tilt_dev
    chunks = math.gcd(refs, 5)
    guests = CORES * cap
    wide = 2 * pixels
    rows = pixels + EXTRA_ROWS
    spec_rows = pixels + 2 * EXTRA_ROWS
    vmem = pl.BlockSpec(memory_space=pltpu.VMEM)
    anywhere = pl.BlockSpec(memory_space=pl.ANY)
    dma = pltpu.SemaphoreType.DMA
    block = pltpu.VMEM((refs, rows, pixels), BF16)
    scratch = [
        pltpu.VMEM((slots, pixels, pixels), BF16),
        pltpu.VMEM((refs, 2, pixels, pixels), BF16),
    ] + [block] * 8 + [
        pltpu.VMEM((guests, spec_rows, pixels), BF16),
        pltpu.VMEM((guests, spec_rows, pixels), BF16),
        pltpu.VMEM((slots, spec_rows, pixels), F32),
        pltpu.VMEM((slots, 16, pixels), F32),
        pltpu.VMEM((slots, slots), F32),
        pltpu.VMEM((slots, node_count), F32),
        pltpu.VMEM((slots, wide), F32),
        pltpu.VMEM((3, wide, pixels), F32),
        pltpu.VMEM((3, pixels, pixels), F32),
        pltpu.VMEM((8, wide), jnp.int32),
        pltpu.VMEM((8, wide), jnp.int32),
        pltpu.SMEM((8, wide), jnp.int32),
        pltpu.SMEM((8, wide), jnp.int32),
        pltpu.VMEM((tilt_dev, 2 * node_count), F32),
        pltpu.VMEM((devices - 1, tilt_dev, 2 * node_count), F32),
        pltpu.VMEM((8, pixels), F32),
        pltpu.VMEM((8, pixels), F32),
        dma((chunks + 3,)),
        dma((8, chunks)),
        dma((8, chunks)),
        dma((GUEST_CHUNKS,)),
        dma((GUEST_CHUNKS,)),
        dma((2,)),
        dma((2,)),
        dma((devices - 1,)),
        dma((devices - 1,)),
    ]
    terms, new_warp = pl.pallas_call(
        functools.partial(gather_kernel, cap, view_dev, chunks),
        out_shape=(
            jax.ShapeDtypeStruct((3, slots), F32),
            jax.ShapeDtypeStruct(warp_grid.shape, F32),
        ),
        in_specs=[vmem] * 5 + [anywhere] * 2 + [vmem] * 8,
        out_specs=(vmem, vmem),
        scratch_shapes=scratch,
        compiler_params=pltpu.CompilerParams(
            collective_id=0, has_side_effects=True, vmem_limit_bytes=56 * 1024 * 1024
        ),
        name="gather_sums",
    )(
        slot_view.reshape(1, slots), slot_tilt, slot_pos.reshape(2, slots), defocus, warp_grid,
        patches[0], projections.reshape(refs, 2, pixels, pixels), *tables(pixels),
    )
    return (terms[:, None, :], new_warp)


def solution(mesh):
    on_chips = mesh.shape["rep"] == 1 and mesh.shape["dom"] == CHIPS * CORES
    body = on_device_gathered if on_chips else on_device
    in_specs = (
        P(("groups", "tilt"), "dom", None, None),
        P(("groups", "tilt"), "dom", None),
        P(("groups", "tilt"), "dom"),
        P(None, ("groups", "tilt"), "dom"),
        P(("groups", "tilt"), "dom"),
        P(("groups", "dom"), "tilt", None, "rep", None),
        P(("groups", "tilt"), None, None),
    )
    out_specs = (P(None, ("groups", "tilt"), "dom"), P(("groups", "tilt"), None, None))
    return jax.shard_map(
        body, mesh=mesh, in_specs=in_specs, out_specs=out_specs, check_vma=False
    )
```

```python
import functools
import math

import jax
import jax.numpy as jnp
import numpy as np
from jax import lax
from jax.experimental import pallas as pl
from jax.experimental.pallas import tpu as pltpu
from jax.sharding import PartitionSpec as P

GRID = 16


AMPLITUDE = 0.07
TRUST_FLOOR = 0.02


def signed_freq(index, pixels):
    return jnp.where(index < pixels // 2, index, index - pixels).astype(jnp.float32)


def dft_tables(freq_rows, pixels):
    columns = jnp.arange(pixels, dtype=jnp.int32)
    table_scale = 1.0 / math.sqrt(pixels)
    turns_rows = (freq_rows[:, None] * columns[None, :] % pixels).astype(jnp.float32) * (
        2.0 * math.pi / pixels
    )
    turns_full = (columns[:, None] * columns[None, :] % pixels).astype(jnp.float32) * (
        2.0 * math.pi / pixels
    )
    row_table = jnp.concatenate([jnp.cos(turns_rows), jnp.sin(turns_rows)], axis=0) * table_scale
    col_table = jnp.concatenate([jnp.cos(turns_full), jnp.sin(turns_full)], axis=1) * table_scale
    return (row_table.astype(jnp.bfloat16), col_table.astype(jnp.bfloat16))


def node_weights(pos_x, pos_y, grid_side):
    knot_pos = jnp.arange(grid_side, dtype=jnp.int32).astype(jnp.float32)
    weight_x = jnp.maximum(0.0, 1.0 - jnp.abs(pos_x[:, None] * (grid_side - 1) - knot_pos[None, :]))
    weight_y = jnp.maximum(0.0, 1.0 - jnp.abs(pos_y[:, None] * (grid_side - 1) - knot_pos[None, :]))
    return (weight_y[:, :, None] * weight_x[:, None, :]).reshape(
        pos_x.shape[0], grid_side * grid_side
    )


def spectral_terms(spectrum, ref_blk, focus_blk, shift_blk, freq_rows, pixels):
    row_total = freq_rows.shape[0]
    v_one_cos = spectrum[:, :row_total, :pixels]
    v_one_sin = spectrum[:, :row_total, pixels:]
    v_two_cos = spectrum[:, row_total:, :pixels]
    v_two_sin = spectrum[:, row_total:, pixels:]
    real_part = v_one_cos - v_two_sin
    imag_part = -(v_one_sin + v_two_cos)
    freq_y = signed_freq(freq_rows, pixels)[None, :, None]
    freq_x = signed_freq(jnp.arange(pixels, dtype=jnp.int32), pixels)[None, None, :]
    nyquist = pixels / 2.0
    radius = (freq_y * freq_y + freq_x * freq_x) / (nyquist * nyquist)
    aberration = math.pi * focus_blk[:, None, None] * radius
    contrast = -(
        math.sqrt(1.0 - AMPLITUDE * AMPLITUDE) * jnp.sin(aberration)
        + AMPLITUDE * jnp.cos(aberration)
    )
    phase_angle = (
        2.0
        * math.pi
        / pixels
        * (freq_x * shift_blk[:, 0, None, None] + freq_y * shift_blk[:, 1, None, None])
    )
    cosine = jnp.cos(phase_angle)
    sine_part = jnp.sin(phase_angle)
    ref_real = ref_blk[:, 0].astype(jnp.float32)
    ref_imag = ref_blk[:, 1].astype(jnp.float32)
    model_real = contrast * (ref_real * cosine + ref_imag * sine_part)
    model_imag = contrast * (ref_imag * cosine - ref_real * sine_part)
    diff_real = real_part - model_real
    diff_imag = imag_part - model_imag
    inverse_area = 1.0 / (pixels * pixels)
    energy = jnp.sum(diff_real * diff_real + diff_imag * diff_imag, axis=(1, 2)) * inverse_area
    cross_term = diff_imag * model_real - diff_real * model_imag
    grad_x = 2.0 * inverse_area * jnp.sum(2.0 * math.pi / pixels * freq_x * cross_term, axis=(1, 2))
    grad_y = 2.0 * inverse_area * jnp.sum(2.0 * math.pi / pixels * freq_y * cross_term, axis=(1, 2))
    return jnp.stack([energy, grad_x, grad_y], axis=1)


def on_device(patches, slot_view, slot_tilt, slot_pos, defocus, projections, warp_grid):
    owners = lax.axis_size("dom")
    slot_count = patches.shape[1]
    pixels = patches.shape[-1]
    view_dev = projections.shape[0]
    tilt_dev = warp_grid.shape[0]
    node_count = warp_grid.shape[2]
    capacity = 3 * slot_count // (2 * owners)
    buffer_len = owners * capacity
    chosen_view = slot_view[0, :, 0]
    owner_of = chosen_view // view_dev
    owner_hits = (owner_of[:, None] == jnp.arange(owners, dtype=jnp.int32)[None, :]).astype(
        jnp.int32
    )
    earlier = jnp.cumsum(owner_hits, axis=0) - owner_hits
    slot_rank = jnp.sum(earlier * owner_hits, axis=1)
    target = owner_of * capacity + slot_rank
    matches = target[None, :] == jnp.arange(buffer_len, dtype=jnp.int32)[:, None]
    source = jnp.sum(
        jnp.where(matches, jnp.arange(slot_count, dtype=jnp.int32)[None, :], 0), axis=1
    )
    filled = jnp.any(matches, axis=1)
    patch_rows = jnp.where(filled[:, None, None], patches[0][source], jnp.zeros((), jnp.bfloat16))
    slot_meta = jnp.stack(
        [
            slot_tilt[0].astype(jnp.float32),
            (chosen_view % view_dev).astype(jnp.float32),
            defocus[0].astype(jnp.float32),
            slot_pos[0, 0].astype(jnp.float32),
            slot_pos[1, 0].astype(jnp.float32),
            jnp.ones((slot_count,), jnp.float32),
        ],
        axis=1,
    )
    meta_rows = jnp.where(filled[:, None], slot_meta[source], 0.0).astype(jnp.bfloat16)
    patch_buffer = patch_rows.reshape(owners, capacity, pixels, pixels)
    meta_buffer = meta_rows.reshape(owners, capacity, 6)
    row_span = projections.shape[3]
    freq_rows = lax.axis_index("rep") * row_span + jnp.arange(row_span, dtype=jnp.int32)
    row_table, col_table = dft_tables(freq_rows, pixels)
    row_total = freq_rows.shape[0]
    projected_flat = projections.reshape(view_dev * tilt_dev, 2, row_total, pixels)
    tilt_iota = jnp.arange(tilt_dev, dtype=jnp.int32)
    view_iota = jnp.arange(view_dev, dtype=jnp.int32)

    def one_block(inputs):
        patch_blk, index_blk, focus_blk, shift_blk = inputs
        ref_blk = projected_flat[index_blk]
        first_pass = jnp.einsum(
            "fy,byx->bfx", row_table, patch_blk, preferred_element_type=jnp.float32
        ).astype(jnp.bfloat16)
        spectrum = jnp.einsum(
            "bfx,xk->bfk", first_pass, col_table, preferred_element_type=jnp.float32
        )
        return spectral_terms(spectrum, ref_blk, focus_blk, shift_blk, freq_rows, pixels)

    patch_in = lax.all_to_all(patch_buffer, "dom", split_axis=0, concat_axis=0, tiled=True)
    meta_in = lax.all_to_all(meta_buffer, "dom", split_axis=0, concat_axis=0, tiled=True)
    senders = patch_in.shape[0]
    per_sender = patch_in.shape[1]
    slot_total = senders * per_sender
    meta_flat = meta_in.reshape(slot_total, 6).astype(jnp.float32)
    tilt_match = meta_flat[:, 0:1] == tilt_iota.astype(jnp.float32)[None, :]
    view_match = meta_flat[:, 1:2] == view_iota.astype(jnp.float32)[None, :]
    tilt_local = jnp.sum(jnp.where(tilt_match, tilt_iota[None, :], 0), axis=1)
    view_local = jnp.sum(jnp.where(view_match, view_iota[None, :], 0), axis=1)
    weights = node_weights(meta_flat[:, 3], meta_flat[:, 4], GRID)
    shifts = jnp.sum(warp_grid[tilt_local] * weights[:, None, :], axis=2)
    block_len = math.gcd(slot_total, 16)
    block_count = slot_total // block_len
    per_slot = lax.map(
        one_block,
        (
            patch_in.reshape(block_count, block_len, pixels, pixels),
            (view_local * tilt_dev + tilt_local).reshape(block_count, block_len),
            meta_flat[:, 2].reshape(block_count, block_len),
            shifts.reshape(block_count, block_len, 2),
        ),
    ).reshape(slot_total, 3)
    node_coef = (
        tilt_match.astype(jnp.float32)[:, :, None]
        * per_slot[:, None, 1:3]
        * meta_flat[:, 5, None, None]
    ).reshape(senders, per_sender, 2 * tilt_dev)
    returned = lax.all_to_all(
        per_slot.reshape(senders, per_sender, 3), "dom", split_axis=0, concat_axis=0, tiled=True
    )
    weight_all = weights.reshape(senders, per_sender, node_count)
    own_terms = returned.reshape(buffer_len, 3)[target]
    summed = lax.psum(own_terms, "rep")
    slot_terms = summed.T[:, None, :]
    gradient = jnp.dot(
        node_coef.reshape(-1, 2 * tilt_dev).T,
        weight_all.reshape(-1, node_count),
        precision=lax.Precision.HIGHEST,
        preferred_element_type=jnp.float32,
    ).reshape(tilt_dev, 2, node_count)
    whole_grad = lax.psum(gradient, ("dom", "rep"))
    new_warp = warp_grid - whole_grad / jnp.sqrt(
        whole_grad * whole_grad + TRUST_FLOOR * TRUST_FLOOR
    )
    return (slot_terms, new_warp)


CORES = 2
CHIPS = 4
EXTRA_ROWS = 8
SPEC_ROWS = 16
DELTA = math.asin(AMPLITUDE)
F32 = jnp.float32
BF16 = jnp.bfloat16
OWN, NEAR, CROSS, ON_FAR, ON_OPP, NEAR_PAIR, OPP_PAIR, FAR_PAIR = range(8)


def exact(a, b, dims=(((1,), (0,)), ((), ()))):
    return lax.dot_general(
        a, b, dims, precision=lax.Precision.HIGHEST, preferred_element_type=F32
    )


def contract_last(a, b):
    return lax.dot_general(a, b, (((1,), (1,)), ((), ())), preferred_element_type=F32)


def tables(pixels):
    half = pixels // 2
    k = np.arange(pixels)
    angle = ((k[:, None] * k[None, :]) % pixels).astype(np.float32) * np.float32(
        2.0 * math.pi / pixels
    )
    scale = np.float32(1.0 / math.sqrt(pixels))
    cosine, sine = np.cos(angle) * scale, np.sin(angle) * scale
    pad = np.zeros((SPEC_ROWS - 2, pixels), np.float32)
    edge_c, edge_s = cosine[half : half + 1], sine[half : half + 1]
    first = np.concatenate(
        [cosine[:half], edge_c, edge_c, pad, sine[:half], edge_s, edge_s, pad], axis=0
    )
    second = np.concatenate(
        [np.concatenate([cosine, -sine], axis=1), np.concatenate([-sine, -cosine], axis=1)], axis=0
    )
    edge = np.zeros((SPEC_ROWS, pixels), np.float32)
    edge[2:4] = edge_c
    turn = ((k[:half, None] + k[None, :] == pixels) & (k[:half, None] > 0)).astype(np.float32)
    flip = (((k[:, None] + k[None, :]) % pixels == 0) & (k != half)[None, :]).astype(np.float32)
    unit = np.broadcast_to((k == half).astype(np.float32)[None, :], (16, pixels))
    table = np.arange(2 * pixels)
    focus = np.where(table < pixels, 1.0 + table / pixels, 2.0 + (table - pixels) / half)
    freq = np.where(k < half, k, k - pixels).astype(np.float64)
    chi = 2.0 * math.pi * focus[None, :] * (freq * freq / (half * half))[:, None]
    waves = np.concatenate([np.cos(chi), np.sin(chi)], axis=1)
    levels = np.concatenate([np.cos(chi + 2.0 * DELTA), -np.sin(chi + 2.0 * DELTA)], axis=1)
    low = [jnp.asarray(x, BF16) for x in (first, second, edge, turn, flip, unit, waves)]
    return low + [jnp.asarray(levels, F32)]


def fold_reference(pixels, real, imag, turn, flip, unit, waves, levels):
    half = pixels // 2
    lane = lax.broadcasted_iota(jnp.int32, (1, pixels), 1)
    turned = jnp.dot(turn, jnp.concatenate([real, imag], axis=1), preferred_element_type=F32)
    turned = jnp.concatenate([turned[:, :pixels], turned[:, pixels:]], axis=0).astype(BF16)
    mirror = jnp.dot(turned, flip, preferred_element_type=F32)
    r, i = real.astype(F32), imag.astype(F32)
    column = contract_last(unit, jnp.concatenate([real, imag], axis=0))[0:1]
    column = jnp.where(jnp.concatenate([lane, lane], axis=1) > half, column, 0.0)
    power = r * r + i * i
    mixed = jnp.dot(power.astype(BF16), waves, preferred_element_type=F32)
    swing = jnp.sum(mixed * levels, axis=0, keepdims=True)
    swing = swing[:, : 2 * pixels] + swing[:, 2 * pixels :]
    total = 0.5 * jnp.sum(power) - 0.5 * swing
    high = total.astype(BF16).astype(F32)
    low = total - high
    extra = jnp.concatenate(
        [
            r[half : half + 1], i[half : half + 1], column[:, :pixels], column[:, pixels:],
            high[:, :pixels], high[:, pixels:], low[:, :pixels], low[:, pixels:],
        ],
        axis=0,
    )
    return (r[:half] + mirror[:half]).astype(BF16), (i[:half] - mirror[half:]).astype(BF16), extra


def gather_kernel(cap, view_dev, bounds, guest_bounds, view_ref, tilt_ref, pos_ref, focus_ref,
                  warp_ref, patch_hbm, proj_hbm, first_hbm, second_hbm, edge_hbm, turn_hbm,
                  flip_hbm, unit_hbm, waves_hbm, levels_hbm, terms_ref, new_ref, first_ref,
                  second_ref, edge_ref, turn_ref, flip_ref, unit_ref, waves_ref, levels_ref,
                  patch_ref, proj_ref, own_ref, pair_ref, near_ref, near_pair_ref, opp_ref,
                  opp_pair_ref, far_ref, far_pair_ref, guest_ref, visit_ref, spec_ref,
                  visit_spec_ref, factor_ref, visit_factor_ref, cols_ref, visit_cols_ref,
                  node_ref, visit_node_ref, match_ref, sums_ref, visit_sums_ref, ints_ref,
                  visit_ints_ref, ints_s, visit_ints_s, meta_ref, visit_meta_ref, grad_ref,
                  held_ref, back_ref, back_in_ref, load_sem, table_sem, send_sem, recv_sem,
                  guest_send, guest_recv, misc_send, misc_recv, grad_send, grad_recv):
    slots, pixels = patch_ref.shape[0], patch_ref.shape[1]
    half = pixels // 2
    refs = own_ref.shape[0]
    tilt_dev = warp_ref.shape[0]
    node_count = warp_ref.shape[2]
    chunks = len(bounds) - 1
    guests = guest_ref.shape[0]
    guest_chunks = len(guest_bounds) - 1
    devices = CHIPS * CORES
    padded = devices * cap
    far_base = padded - guests
    wide = sums_ref.shape[1]
    shift_lanes = wide - pixels
    me = lax.axis_index("dom")
    chip = me // CORES
    core = me % CORES
    partner = chip * CORES + (1 - core)
    mate_chip = chip + 1 - 2 * (chip % 2)
    mate = mate_chip * CORES + core
    cross = (CHIPS - 1 - chip) * CORES + core
    inner = (chip > 0) & (chip < CHIPS - 1)
    outer = jnp.logical_not(inner)
    barrier = pltpu.get_barrier_semaphore()

    def greet(device):
        pl.semaphore_signal(
            barrier, inc=1, device_id={"dom": device}, device_id_type=pl.DeviceIdType.MESH
        )

    greet(mate)
    greet(partner)

    @pl.when(inner)
    def _():
        greet(cross)

    def load_proj(c):
        rows = pl.ds(bounds[c], bounds[c + 1] - bounds[c])
        return pltpu.make_async_copy(proj_hbm.at[rows], proj_ref.at[rows], load_sem.at[c])

    load_patch = pltpu.make_async_copy(patch_hbm, patch_ref, load_sem.at[chunks])
    sources = (turn_hbm, flip_hbm, unit_hbm, waves_hbm, levels_hbm, first_hbm, second_hbm, edge_hbm)
    targets = (turn_ref, flip_ref, unit_ref, waves_ref, levels_ref, first_ref, second_ref, edge_ref)
    load_tables = [
        pltpu.make_async_copy(a, b, table_sem.at[n]) for n, (a, b) in enumerate(zip(sources, targets))
    ]
    fold_tables = 5
    load_proj(0).start()
    for load in load_tables:
        load.start()
    for c in range(1, chunks):
        load_proj(c).start()
    load_patch.start()

    def remote(src, dst, send, recv, target):
        return pltpu.make_async_remote_copy(
            src_ref=src, dst_ref=dst, send_sem=send, recv_sem=recv,
            device_id={"dom": target}, device_id_type=pl.DeviceIdType.MESH,
        )

    flows = {
        OWN: (own_ref, pair_ref, partner),
        NEAR: (own_ref, near_ref, mate),
        CROSS: (own_ref, opp_ref, cross),
        ON_FAR: (near_ref, far_ref, cross),
        ON_OPP: (opp_ref, opp_ref, mate),
        NEAR_PAIR: (near_ref, near_pair_ref, partner),
        OPP_PAIR: (opp_ref, opp_pair_ref, partner),
        FAR_PAIR: (far_ref, far_pair_ref, partner),
    }

    def flow(kind, c):
        src, dst, target = flows[kind]
        rows = pl.ds(bounds[c], bounds[c + 1] - bounds[c])
        return remote(
            src.at[rows], dst.at[rows], send_sem.at[kind, c], recv_sem.at[kind, c], target
        )

    def guest_copy(g):
        rows = pl.ds(guest_bounds[g], guest_bounds[g + 1] - guest_bounds[g])
        return remote(
            guest_ref.at[rows], visit_ref.at[rows], guest_send.at[g], guest_recv.at[g], mate
        )

    meta_copy = remote(meta_ref, visit_meta_ref, misc_send.at[0], misc_recv.at[0], mate)
    back_copy = remote(back_ref, back_in_ref, misc_send.at[1], misc_recv.at[1], mate)

    def fold(c):
        load_proj(c).wait()

        def one(i, carry):
            n = bounds[c] + i
            top, bottom, extra = fold_reference(
                pixels, proj_ref[n, 0], proj_ref[n, 1], turn_ref[...], flip_ref[...],
                unit_ref[...], waves_ref[...], levels_ref[...],
            )
            own_ref[n, :half] = top
            own_ref[n, half:pixels] = bottom
            own_ref[n, pixels:] = extra.astype(BF16)
            return carry

        lax.fori_loop(0, bounds[c + 1] - bounds[c], one, 0, unroll=2)

    def send_own(c):
        flow(NEAR, c).start()

        @pl.when(inner)
        def _():
            flow(CROSS, c).start()

        flow(OWN, c).start()

    lane = lax.broadcasted_iota(jnp.int32, (1, pixels), 1)
    line = jnp.where(lane < half, lane, lane - pixels).astype(F32)
    lane_f = lane.astype(F32)

    def route():
        chip_f, core_f, mate_f = chip.astype(F32), core.astype(F32), mate_chip.astype(F32)
        opp_f = (CHIPS - 1) - jnp.where(inner, chip_f, mate_f)
        view = view_ref[...].astype(F32)
        owner = jnp.floor((view + 0.5) * (1.0 / view_dev))
        owner_chip = jnp.floor((owner + 0.5) * (1.0 / CORES))
        owner_core = owner - CORES * owner_chip
        role = jnp.where(
            owner_chip == chip_f, 0.0,
            jnp.where(owner_chip == mate_f, 1.0, jnp.where(owner_chip == opp_f, 2.0, 3.0)),
        )
        key = role * CORES + jnp.where(owner_core == core_f, 0.0, 1.0)
        tilt = tilt_ref[...].astype(F32)
        which = (view - owner * view_dev) * tilt_dev + tilt
        pos = pos_ref[...].astype(F32)
        block = jnp.concatenate(
            [key, which, pos, focus_ref[...].astype(F32), tilt,
             jnp.zeros((slots - 6, slots), F32)],
            axis=0,
        )
        cols = block.T
        cols_ref[...] = cols
        row = lax.broadcasted_iota(jnp.int32, (slots, slots), 0)
        col = lax.broadcasted_iota(jnp.int32, (slots, slots), 1)
        ahead = jnp.where((cols[:, 0:1] == key) & (col < row), 1.0, 0.0)
        target = cols[:, 0:1] * cap + jnp.sum(ahead, axis=1, keepdims=True)
        place = lax.broadcasted_iota(jnp.int32, (1, wide), 1).astype(F32)
        match = jnp.where(target == place, 1.0, 0.0)
        match_ref[...] = match
        slot = lax.broadcasted_iota(jnp.int32, (slots, wide), 0).astype(F32)
        source = jnp.sum(match * slot, axis=0, keepdims=True)
        chosen = jnp.sum(match * cols[:, 1:2], axis=0, keepdims=True)
        ints = jnp.concatenate([source, chosen, jnp.zeros((6, wide), F32)], axis=0)
        ints_ref[...] = (ints + 0.5).astype(jnp.int32)

    def node_weights_of(cols):
        node = lax.broadcasted_iota(jnp.int32, (1, node_count), 1).astype(F32)
        node_y = jnp.floor((node + 0.5) * (1.0 / GRID))
        node_x = node - node_y * GRID
        weight_x = jnp.maximum(0.0, 1.0 - jnp.abs(cols[:, 2:3] * (GRID - 1) - node_x))
        weight_y = jnp.maximum(0.0, 1.0 - jnp.abs(cols[:, 3:4] * (GRID - 1) - node_y))
        return weight_y * weight_x

    def place_nodes():
        weights = node_weights_of(cols_ref)
        node_ref[...] = weights
        hits = jnp.where(cols_ref[:, 5:6] == lane_f[:, :16], 1.0, 0.0)
        spare = jnp.zeros((16 - tilt_dev, node_count), F32)
        for axis in range(2):
            grid = jnp.concatenate([warp_ref[:, axis, :], spare], axis=0)
            shift = jnp.sum(exact(hits, grid) * weights, axis=1, keepdims=True)
            cols_ref[:, 6 + axis : 7 + axis] = shift
        meta_ref[...] = exact(cols_ref[...].T[:8], match_ref[...])

    step_angle = 2.0 * math.pi / pixels
    norm = 1.0 / (half * half)
    block_slots = 16

    def factors(cols_ref, factor_ref, block, carry):
        rows = pl.ds(pl.multiple_of(block * block_slots, block_slots), block_slots)
        cols = cols_ref[rows]
        focus, shift_x, shift_y = cols[:, 4:5], cols[:, 6:7], cols[:, 7:8]
        chi = math.pi * focus * (line * line * norm)
        phi_x = step_angle * shift_x * line
        phi_y = step_angle * shift_y * line
        c_x, s_x = jnp.cos(chi), jnp.sin(chi)
        s_y = s_x * math.cos(DELTA) + c_x * math.sin(DELTA)
        c_y = c_x * math.cos(DELTA) - s_x * math.sin(DELTA)
        p_x, q_x, p_y, q_y = jnp.cos(phi_x), jnp.sin(phi_x), jnp.cos(phi_y), jnp.sin(phi_y)
        tall = (s_y * p_y, s_y * q_y, c_y * p_y, c_y * q_y)
        a, b, c, d = c_x * p_x, c_x * q_x, s_x * p_x, s_x * q_x
        e, f, g, h = (v[:, half : half + 1] for v in (a, b, c, d))
        edge_re = -(tall[0] * e - tall[1] * f + tall[2] * g - tall[3] * h)
        edge_im = -(tall[0] * f + tall[1] * e + tall[2] * h + tall[3] * g)
        tall = tuple(jnp.where(lane == half + 1, pltpu.roll(v, 1, 1), v) for v in tall)
        place = jnp.where(focus < 2.0, (focus - 1.0) * pixels, pixels + (focus - 2.0) * half)
        hit_low = jnp.where(place == lane_f, -0.5, 0.0)
        hit_high = jnp.where(place == lane_f + pixels, -0.5, 0.0)
        zero = jnp.zeros_like(a)
        values = tall + (a, b, c, d, edge_re, edge_im, zero, zero,
                         hit_low, hit_high, hit_low, hit_high)
        for index, value in enumerate(values):
            factor_ref[rows, index] = value
        return carry

    row8 = lax.broadcasted_iota(jnp.int32, (8, pixels), 0)
    main_rows = half + SPEC_ROWS

    def spectra(blocks, factor_blocks, put):
        count = len(blocks)
        wides = []
        for n in range(0, count, 2):
            both = jnp.concatenate(blocks[n : n + 2], axis=1)
            v = jnp.dot(first_ref[...], both, preferred_element_type=F32)
            edge = contract_last(edge_ref[...], jnp.concatenate(blocks[n : n + 2], axis=0))
            for part in range(2):
                at = slice(part * pixels, (part + 1) * pixels)
                one = jnp.concatenate([v[:half, at], v[half:main_rows, at] + edge[:, at]], axis=0)
                wides.append(
                    jnp.concatenate([one.astype(BF16), v[main_rows:, at].astype(BF16)], axis=1)
                )
        spectrum = jnp.dot(
            jnp.concatenate(wides, axis=0), second_ref[...], preferred_element_type=F32
        )
        for n in range(count):
            factor = factor_blocks[n]
            tall = factor[0:4]
            a, b, c, d = factor[4:5], factor[5:6], factor[6:7], factor[7:8]
            rows = jnp.concatenate(
                [
                    jnp.concatenate([-a, b, -c, d], axis=0),
                    jnp.concatenate([-b, -a, -d, -c], axis=0),
                ],
                axis=1,
            )
            tall_high = tall.astype(BF16).astype(F32)
            row_high = rows.astype(BF16).astype(F32)
            tall_low, row_low = tall - tall_high, rows - row_high
            tall_all = jnp.concatenate(
                [tall_high, tall_high, tall_low, jnp.zeros_like(tall_low)], axis=0
            ).astype(BF16)
            row_all = jnp.concatenate(
                [row_high, row_low, row_high, jnp.zeros_like(row_low)], axis=0
            ).astype(BF16)
            turn = lax.dot_general(
                tall_all, row_all, (((0,), (0,)), ((), ())), preferred_element_type=F32
            )
            base = n * main_rows
            x_re = spectrum[base : base + half, :pixels]
            x_im = spectrum[base : base + half, pixels:]
            t_re, t_im = turn[:half, :pixels], turn[:half, pixels:]
            put(n, slice(0, half), x_re * t_re - x_im * t_im)
            put(n, slice(half, pixels), x_re * t_im + x_im * t_re)
            power = x_re * x_re + x_im * x_im
            power = jnp.sum(power.reshape(half // 8, 8, pixels), axis=0) * 2.0 - jnp.where(
                row8 == 0, power[:8], 0.0
            )
            x_re = spectrum[base + half : base + half + 8, :pixels]
            x_im = spectrum[base + half : base + half + 8, pixels:]
            power = power + jnp.where(row8 == 0, x_re * x_re + x_im * x_im, 0.0)
            edge_turn = (row8 == 2) | (row8 == 3)
            t_re = jnp.where(edge_turn, factor[8:9], turn[half : half + 8, :pixels])
            t_im = jnp.where(edge_turn, factor[9:10], turn[half : half + 8, pixels:])
            y_re = x_re * t_re - x_im * t_im
            y_im = x_re * t_im + x_im * t_re
            odd = row8 % 2 == 1
            straight = jnp.where(odd, y_im, y_re)
            crossed = jnp.where(odd, -y_re, y_im)
            straight = jnp.where(row8 < 4, straight, factor[8:16])
            power = jnp.sum(power, axis=0, keepdims=True)
            high = power.astype(BF16).astype(F32)
            crossed = jnp.where(
                row8 < 4, crossed,
                jnp.where(row8 == 4, high, jnp.where(row8 == 5, power - high, 0.0)),
            )
            put(n, slice(pixels, pixels + 16), jnp.concatenate([straight, crossed], axis=0))

    weight_x = jnp.where(row8 < 2, line, jnp.where(row8 < 4, -float(half), 0.0))
    weight_y = jnp.where(row8 < 2, -float(half), jnp.where(row8 < 4, line, 0.0))
    freq_y = lax.broadcasted_iota(jnp.int32, (half, pixels), 0).astype(F32)

    def stack(x):
        return jnp.sum(x.reshape(half // 8, 8, pixels), axis=0)

    def meet(y, ref, out_ref, place):
        y = y.astype(F32)
        r = ref.astype(F32)
        y_re, y_im, straight = y[:half], y[half:pixels], y[pixels : pixels + 8]
        crossed = y[pixels + 8 :]
        r_re, r_im, extra = r[:half], r[half:pixels], r[pixels:]
        match = stack(y_re * r_re + y_im * r_im) + straight * extra
        swirl = y_im * r_re - y_re * r_im
        edge = crossed * extra
        energy = jnp.where((row8 == 4) | (row8 == 5), crossed, 0.0) - 2.0 * match
        grad_x = stack(swirl) * line + edge * weight_x
        grad_y = stack(swirl * freq_y) + edge * weight_y
        for index, value in enumerate((energy, grad_x, grad_y)):
            out_ref[index, pl.ds(place, 1)] = jnp.sum(value, axis=0, keepdims=True)

    def slot_at(p):
        return jnp.clip(ints_s[0, p], 0, slots - 1)

    def ref_at(held, p):
        return jnp.clip(held[1, p], 0, refs - 1)

    def process(refs_ref, role):
        def some(step, carry):
            for u in range(4):
                p = role * cap + step * 4 + u
                meet(spec_ref[slot_at(p)], refs_ref[ref_at(ints_s, p)], sums_ref, p)
            return carry

        lax.fori_loop(0, cap // 4, some, 0)

    def entertain(low, high):
        def some(refs_ref, step, carry):
            for u in range(4):
                g = step * 4 + u
                p = far_base + g
                held = refs_ref[ref_at(visit_ints_s, p)]
                meet(visit_spec_ref[g], held, visit_sums_ref, p - shift_lanes)
            return carry

        for refs_ref, least, most in ((far_ref, 0, cap), (far_pair_ref, cap, 2 * cap)):
            a, b = max(low, least), min(high, most)
            if b > a:
                lax.fori_loop(a // 4, b // 4, functools.partial(some, refs_ref), 0)

    def transform(low, high):
        def some(step, carry):
            base = low + step * 4

            def put(n, rows, value):
                spec_ref[base + n, rows] = value

            four = [base + n for n in range(4)]
            spectra([patch_ref[s] for s in four], [factor_ref[s] for s in four], put)
            return carry

        lax.fori_loop(0, (high - low) // 4, some, 0)

    def transform_visit(low, high):
        def some(step, carry):
            base = low + step * 4

            def put(n, rows, value):
                visit_spec_ref[base + n, rows] = value

            four = [base + n for n in range(4)]
            spectra(
                [visit_ref[g] for g in four],
                [visit_factor_ref[far_base - shift_lanes + g] for g in four],
                put,
            )
            return carry

        lax.fori_loop(0, (high - low) // 4, some, 0)

    def pack(g, carry):
        guest_ref[g] = patch_ref[slot_at(far_base + g)]
        return carry

    for load in load_tables[:fold_tables]:
        load.wait()
    fold(0)
    fold(1)

    @pl.when(inner)
    def _():
        pl.semaphore_wait(barrier, 3)

    @pl.when(outer)
    def _():
        pl.semaphore_wait(barrier, 2)

    send_own(0)
    for c in range(2, chunks):
        fold(c)
        send_own(c - 1)
    route()
    ints_load = pltpu.make_async_copy(ints_ref, ints_s, load_sem.at[chunks + 1])
    ints_load.start()
    sums_ref[...] = jnp.zeros_like(sums_ref)
    visit_sums_ref[...] = jnp.zeros_like(visit_sums_ref)
    send_own(chunks - 1)
    place_nodes()
    load_patch.wait()
    ints_load.wait()

    @pl.when(outer)
    def _():
        lax.fori_loop(0, guests, pack, 0, unroll=4)

    lax.fori_loop(
        0, slots // block_slots, functools.partial(factors, cols_ref, factor_ref), 0
    )

    @pl.when(outer)
    def _():
        meta_copy.start()
        for g in range(guest_chunks):
            guest_copy(g).start()

    for load in load_tables[fold_tables:]:
        load.wait()

    def pass_on(c):
        flow(NEAR, c).wait_recv()

        @pl.when(inner)
        def _():
            flow(ON_FAR, c).start()
            flow(CROSS, c).wait_recv()
            flow(ON_OPP, c).start()
            flow(OPP_PAIR, c).start()

        flow(NEAR_PAIR, c).start()

    segments = 4
    seg = slots // segments
    done = 0
    for n in range(segments):
        transform(n * seg, (n + 1) * seg)
        upto = chunks * (n + 1) // segments
        while done < upto:
            pass_on(done)
            done += 1

    process(own_ref, 0)
    for c in range(chunks):
        flow(OWN, c).wait_recv()
    process(pair_ref, 1)
    process(near_ref, 2)
    for c in range(chunks):
        flow(NEAR_PAIR, c).wait_recv()
    process(near_pair_ref, 3)

    @pl.when(outer)
    def _():
        for c in range(chunks):
            flow(ON_OPP, c).wait_recv()
            flow(OPP_PAIR, c).start()

    process(opp_ref, 4)
    for c in range(chunks):
        flow(OPP_PAIR, c).wait_recv()
    process(opp_pair_ref, 5)

    visit_load = pltpu.make_async_copy(visit_ints_ref, visit_ints_s, load_sem.at[chunks + 2])
    ones = jnp.ones((8, pixels), F32)
    row16 = lax.broadcasted_iota(jnp.int32, (16, slots), 0)
    area = 1.0 / (pixels * pixels)
    scale = jnp.where(row8 == 0, area, 2.0 * area * step_angle)

    def gather_rows(from_ref):
        parts = [exact(ones, from_ref[k], (((1,), (1,)), ((), ()))) for k in range(3)]
        row = lax.broadcasted_iota(jnp.int32, parts[0].shape, 0)
        return jnp.where(row == 0, parts[0], jnp.where(row == 1, parts[1], parts[2])) * scale[:, 0:1]

    def gradient(on_tilt, terms, node_ref, first):
        for axis in range(2):
            coef = jnp.where(on_tilt, terms[1 + axis : 2 + axis], 0.0)
            grad = exact(coef, node_ref[...])[:tilt_dev]
            at = slice(axis * node_count, (axis + 1) * node_count)
            grad_ref[:, at] = grad if first else grad_ref[:, at] + grad

    def welcome():
        meta_copy.wait_recv()
        meta = visit_meta_ref[...]
        visit_ints_ref[...] = (meta + 0.5).astype(jnp.int32)
        visit_load.start()
        block = jnp.concatenate(
            [meta[:, shift_lanes:], jnp.zeros((pixels - 8, pixels), F32)], axis=0
        )
        visit_cols_ref[...] = block.T
        visit_node_ref[...] = node_weights_of(visit_cols_ref)
        first = (far_base - shift_lanes) // block_slots
        last = first + guests // block_slots
        lax.fori_loop(
            first, last, functools.partial(factors, visit_cols_ref, visit_factor_ref), 0
        )
        visit_load.wait()

    def bring_far(c):
        flow(ON_FAR, c).wait_recv()
        flow(FAR_PAIR, c).start()

    @pl.when(inner)
    def _():
        welcome()
        brought = 0
        for g in range(guest_chunks - 1):
            upto = chunks * (g + 1) // (guest_chunks - 1)
            while brought < min(upto, chunks - 1):
                bring_far(brought)
                brought += 1
            guest_copy(g).wait_recv()
            transform_visit(guest_bounds[g], guest_bounds[g + 1])
        bring_far(chunks - 1)
        process(far_ref, 6)
        for c in range(chunks):
            flow(FAR_PAIR, c).wait_recv()
        process(far_pair_ref, 7)
        entertain(0, guest_bounds[guest_chunks - 1])

    terms = exact(gather_rows(sums_ref), match_ref[...], (((1,), (1,)), ((), ())))
    on_tilt = row16 == tilt_ref[...]
    gradient(on_tilt, terms, node_ref, True)

    @pl.when(inner)
    def _():
        guest_copy(guest_chunks - 1).wait_recv()
        transform_visit(guest_bounds[guest_chunks - 1], guests)
        entertain(guest_bounds[guest_chunks - 1], guests)
        back = gather_rows(visit_sums_ref)
        back_ref[...] = back
        invited = visit_meta_ref[0:1, shift_lanes:] > 0.5
        visit_tilt = jnp.where(invited, jnp.floor(visit_meta_ref[5:6, shift_lanes:] + 0.5), -1.0)
        row = lax.broadcasted_iota(jnp.int32, (16, pixels), 0).astype(F32)
        gradient(row == visit_tilt, back, visit_node_ref, False)
        back_copy.start()

    def grad_copy(hop):
        return remote(
            grad_ref, held_ref.at[hop - 1], grad_send.at[hop - 1], grad_recv.at[hop - 1],
            lax.rem(me + hop, devices),
        )

    for c in range(chunks):
        flow(OWN, c).wait_send()
        flow(NEAR, c).wait_send()
        flow(NEAR_PAIR, c).wait_send()
        flow(OPP_PAIR, c).wait_send()

    @pl.when(inner)
    def _():
        for c in range(chunks):
            flow(CROSS, c).wait_send()
            flow(ON_FAR, c).wait_send()
            flow(ON_OPP, c).wait_send()
            flow(FAR_PAIR, c).wait_send()

    @pl.when(outer)
    def _():
        meta_copy.wait_send()
        for g in range(guest_chunks):
            guest_copy(g).wait_send()

    for hop in range(1, devices):
        grad_copy(hop).start()
    back_in = jnp.zeros((8, pixels), F32)
    cols_ref[:8, :] = back_in

    @pl.when(outer)
    def _():
        back_copy.wait_recv()
        cols_ref[:8, :] = back_in_ref[...]

    terms = terms + exact(cols_ref[:8, :], match_ref[:, shift_lanes:], (((1,), (1,)), ((), ())))
    for index in range(3):
        terms_ref[index] = terms[index : index + 1]

    @pl.when(inner)
    def _():
        back_copy.wait_send()

    for hop in range(1, devices):
        grad_copy(hop).wait()
    total = grad_ref[...]
    for hop in range(1, devices):
        total = total + held_ref[hop - 1]
    change = total / jnp.sqrt(total * total + TRUST_FLOOR * TRUST_FLOOR)
    for axis in range(2):
        at = slice(axis * node_count, (axis + 1) * node_count)
        new_ref[:, axis, :] = warp_ref[:, axis, :] - change[:, at]


def on_device_gathered(
    patches, slot_view, slot_tilt, slot_pos, defocus, projections, warp_grid
):
    pixels = patches.shape[-1]
    slots = patches.shape[1]
    view_dev = projections.shape[0]
    tilt_dev = warp_grid.shape[0]
    node_count = warp_grid.shape[2]
    devices = CHIPS * CORES
    cap = 3 * slots // (2 * devices)
    refs = view_dev * tilt_dev
    per = refs // math.gcd(refs, 5)
    bounds = sorted({0, per // 4, per // 2} | set(range(per, refs + 1, per)))
    chunks = len(bounds) - 1
    guests = CORES * cap
    guest_bounds = [0, guests // 3, 2 * guests // 3, 11 * guests // 12, guests]
    guest_chunks = len(guest_bounds) - 1
    wide = 2 * pixels
    rows = pixels + EXTRA_ROWS
    spec_rows = pixels + 2 * EXTRA_ROWS
    vmem = pl.BlockSpec(memory_space=pltpu.VMEM)
    anywhere = pl.BlockSpec(memory_space=pl.ANY)
    dma = pltpu.SemaphoreType.DMA
    block = pltpu.VMEM((refs, rows, pixels), BF16)
    held_tables = tables(pixels)
    scratch = [pltpu.VMEM(x.shape, x.dtype) for x in held_tables] + [
        pltpu.VMEM((slots, pixels, pixels), BF16),
        pltpu.VMEM((refs, 2, pixels, pixels), BF16),
    ] + [block] * 8 + [
        pltpu.VMEM((guests, pixels, pixels), BF16),
        pltpu.VMEM((guests, pixels, pixels), BF16),
        pltpu.VMEM((slots, spec_rows, pixels), F32),
        pltpu.VMEM((guests, spec_rows, pixels), F32),
        pltpu.VMEM((slots, 16, pixels), F32),
        pltpu.VMEM((pixels, 16, pixels), F32),
        pltpu.VMEM((slots, slots), F32),
        pltpu.VMEM((pixels, pixels), F32),
        pltpu.VMEM((slots, node_count), F32),
        pltpu.VMEM((pixels, node_count), F32),
        pltpu.VMEM((slots, wide), F32),
        pltpu.VMEM((3, wide, pixels), F32),
        pltpu.VMEM((3, pixels, pixels), F32),
        pltpu.VMEM((8, wide), jnp.int32),
        pltpu.VMEM((8, wide), jnp.int32),
        pltpu.SMEM((8, wide), jnp.int32),
        pltpu.SMEM((8, wide), jnp.int32),
        pltpu.VMEM((8, wide), F32),
        pltpu.VMEM((8, wide), F32),
        pltpu.VMEM((tilt_dev, 2 * node_count), F32),
        pltpu.VMEM((devices - 1, tilt_dev, 2 * node_count), F32),
        pltpu.VMEM((8, pixels), F32),
        pltpu.VMEM((8, pixels), F32),
        dma((chunks + 3,)),
        dma((len(held_tables),)),
        dma((8, chunks)),
        dma((8, chunks)),
        dma((guest_chunks,)),
        dma((guest_chunks,)),
        dma((2,)),
        dma((2,)),
        dma((devices - 1,)),
        dma((devices - 1,)),
    ]
    terms, new_warp = pl.pallas_call(
        functools.partial(gather_kernel, cap, view_dev, bounds, guest_bounds),
        out_shape=(
            pltpu.VMEM((3, 1, slots), F32),
            pltpu.VMEM(warp_grid.shape, F32),
        ),
        in_specs=[vmem] * 5 + [anywhere] * 10,
        out_specs=(vmem, vmem),
        scratch_shapes=scratch,
        compiler_params=pltpu.CompilerParams(
            collective_id=0, has_side_effects=True, vmem_limit_bytes=56 * 1024 * 1024
        ),
        name="gather_sums",
    )(
        slot_view.reshape(1, slots), slot_tilt, slot_pos.reshape(2, slots), defocus, warp_grid,
        patches[0], projections.reshape(refs, 2, pixels, pixels), *held_tables,
    )
    return (terms, new_warp)


def solution(mesh):
    on_chips = mesh.shape["rep"] == 1 and mesh.shape["dom"] == CHIPS * CORES
    body = on_device_gathered if on_chips else on_device
    in_specs = (
        P(("groups", "tilt"), "dom", None, None),
        P(("groups", "tilt"), "dom", None),
        P(("groups", "tilt"), "dom"),
        P(None, ("groups", "tilt"), "dom"),
        P(("groups", "tilt"), "dom"),
        P(("groups", "dom"), "tilt", None, "rep", None),
        P(("groups", "tilt"), None, None),
    )
    out_specs = (P(None, ("groups", "tilt"), "dom"), P(("groups", "tilt"), None, None))
    return jax.shard_map(
        body, mesh=mesh, in_specs=in_specs, out_specs=out_specs, check_vma=False
    )
```

```python
import functools
import math

import jax
import jax.numpy as jnp
import numpy as np
from jax import lax
from jax.experimental import pallas as pl
from jax.experimental.pallas import tpu as pltpu
from jax.sharding import PartitionSpec as P

GRID = 16


AMPLITUDE = 0.07
TRUST_FLOOR = 0.02


def signed_freq(index, pixels):
    return jnp.where(index < pixels // 2, index, index - pixels).astype(jnp.float32)


def dft_tables(freq_rows, pixels):
    columns = jnp.arange(pixels, dtype=jnp.int32)
    table_scale = 1.0 / math.sqrt(pixels)
    turns_rows = (freq_rows[:, None] * columns[None, :] % pixels).astype(jnp.float32) * (
        2.0 * math.pi / pixels
    )
    turns_full = (columns[:, None] * columns[None, :] % pixels).astype(jnp.float32) * (
        2.0 * math.pi / pixels
    )
    row_table = jnp.concatenate([jnp.cos(turns_rows), jnp.sin(turns_rows)], axis=0) * table_scale
    col_table = jnp.concatenate([jnp.cos(turns_full), jnp.sin(turns_full)], axis=1) * table_scale
    return (row_table.astype(jnp.bfloat16), col_table.astype(jnp.bfloat16))


def node_weights(pos_x, pos_y, grid_side):
    knot_pos = jnp.arange(grid_side, dtype=jnp.int32).astype(jnp.float32)
    weight_x = jnp.maximum(0.0, 1.0 - jnp.abs(pos_x[:, None] * (grid_side - 1) - knot_pos[None, :]))
    weight_y = jnp.maximum(0.0, 1.0 - jnp.abs(pos_y[:, None] * (grid_side - 1) - knot_pos[None, :]))
    return (weight_y[:, :, None] * weight_x[:, None, :]).reshape(
        pos_x.shape[0], grid_side * grid_side
    )


def spectral_terms(spectrum, ref_blk, focus_blk, shift_blk, freq_rows, pixels):
    row_total = freq_rows.shape[0]
    v_one_cos = spectrum[:, :row_total, :pixels]
    v_one_sin = spectrum[:, :row_total, pixels:]
    v_two_cos = spectrum[:, row_total:, :pixels]
    v_two_sin = spectrum[:, row_total:, pixels:]
    real_part = v_one_cos - v_two_sin
    imag_part = -(v_one_sin + v_two_cos)
    freq_y = signed_freq(freq_rows, pixels)[None, :, None]
    freq_x = signed_freq(jnp.arange(pixels, dtype=jnp.int32), pixels)[None, None, :]
    nyquist = pixels / 2.0
    radius = (freq_y * freq_y + freq_x * freq_x) / (nyquist * nyquist)
    aberration = math.pi * focus_blk[:, None, None] * radius
    contrast = -(
        math.sqrt(1.0 - AMPLITUDE * AMPLITUDE) * jnp.sin(aberration)
        + AMPLITUDE * jnp.cos(aberration)
    )
    phase_angle = (
        2.0
        * math.pi
        / pixels
        * (freq_x * shift_blk[:, 0, None, None] + freq_y * shift_blk[:, 1, None, None])
    )
    cosine = jnp.cos(phase_angle)
    sine_part = jnp.sin(phase_angle)
    ref_real = ref_blk[:, 0].astype(jnp.float32)
    ref_imag = ref_blk[:, 1].astype(jnp.float32)
    model_real = contrast * (ref_real * cosine + ref_imag * sine_part)
    model_imag = contrast * (ref_imag * cosine - ref_real * sine_part)
    diff_real = real_part - model_real
    diff_imag = imag_part - model_imag
    inverse_area = 1.0 / (pixels * pixels)
    energy = jnp.sum(diff_real * diff_real + diff_imag * diff_imag, axis=(1, 2)) * inverse_area
    cross_term = diff_imag * model_real - diff_real * model_imag
    grad_x = 2.0 * inverse_area * jnp.sum(2.0 * math.pi / pixels * freq_x * cross_term, axis=(1, 2))
    grad_y = 2.0 * inverse_area * jnp.sum(2.0 * math.pi / pixels * freq_y * cross_term, axis=(1, 2))
    return jnp.stack([energy, grad_x, grad_y], axis=1)


def on_device(patches, slot_view, slot_tilt, slot_pos, defocus, projections, warp_grid):
    owners = lax.axis_size("dom")
    slot_count = patches.shape[1]
    pixels = patches.shape[-1]
    view_dev = projections.shape[0]
    tilt_dev = warp_grid.shape[0]
    node_count = warp_grid.shape[2]
    capacity = 3 * slot_count // (2 * owners)
    buffer_len = owners * capacity
    chosen_view = slot_view[0, :, 0]
    owner_of = chosen_view // view_dev
    owner_hits = (owner_of[:, None] == jnp.arange(owners, dtype=jnp.int32)[None, :]).astype(
        jnp.int32
    )
    earlier = jnp.cumsum(owner_hits, axis=0) - owner_hits
    slot_rank = jnp.sum(earlier * owner_hits, axis=1)
    target = owner_of * capacity + slot_rank
    matches = target[None, :] == jnp.arange(buffer_len, dtype=jnp.int32)[:, None]
    source = jnp.sum(
        jnp.where(matches, jnp.arange(slot_count, dtype=jnp.int32)[None, :], 0), axis=1
    )
    filled = jnp.any(matches, axis=1)
    patch_rows = jnp.where(filled[:, None, None], patches[0][source], jnp.zeros((), jnp.bfloat16))
    slot_meta = jnp.stack(
        [
            slot_tilt[0].astype(jnp.float32),
            (chosen_view % view_dev).astype(jnp.float32),
            defocus[0].astype(jnp.float32),
            slot_pos[0, 0].astype(jnp.float32),
            slot_pos[1, 0].astype(jnp.float32),
            jnp.ones((slot_count,), jnp.float32),
        ],
        axis=1,
    )
    meta_rows = jnp.where(filled[:, None], slot_meta[source], 0.0).astype(jnp.bfloat16)
    patch_buffer = patch_rows.reshape(owners, capacity, pixels, pixels)
    meta_buffer = meta_rows.reshape(owners, capacity, 6)
    row_span = projections.shape[3]
    freq_rows = lax.axis_index("rep") * row_span + jnp.arange(row_span, dtype=jnp.int32)
    row_table, col_table = dft_tables(freq_rows, pixels)
    row_total = freq_rows.shape[0]
    projected_flat = projections.reshape(view_dev * tilt_dev, 2, row_total, pixels)
    tilt_iota = jnp.arange(tilt_dev, dtype=jnp.int32)
    view_iota = jnp.arange(view_dev, dtype=jnp.int32)

    def one_block(inputs):
        patch_blk, index_blk, focus_blk, shift_blk = inputs
        ref_blk = projected_flat[index_blk]
        first_pass = jnp.einsum(
            "fy,byx->bfx", row_table, patch_blk, preferred_element_type=jnp.float32
        ).astype(jnp.bfloat16)
        spectrum = jnp.einsum(
            "bfx,xk->bfk", first_pass, col_table, preferred_element_type=jnp.float32
        )
        return spectral_terms(spectrum, ref_blk, focus_blk, shift_blk, freq_rows, pixels)

    patch_in = lax.all_to_all(patch_buffer, "dom", split_axis=0, concat_axis=0, tiled=True)
    meta_in = lax.all_to_all(meta_buffer, "dom", split_axis=0, concat_axis=0, tiled=True)
    senders = patch_in.shape[0]
    per_sender = patch_in.shape[1]
    slot_total = senders * per_sender
    meta_flat = meta_in.reshape(slot_total, 6).astype(jnp.float32)
    tilt_match = meta_flat[:, 0:1] == tilt_iota.astype(jnp.float32)[None, :]
    view_match = meta_flat[:, 1:2] == view_iota.astype(jnp.float32)[None, :]
    tilt_local = jnp.sum(jnp.where(tilt_match, tilt_iota[None, :], 0), axis=1)
    view_local = jnp.sum(jnp.where(view_match, view_iota[None, :], 0), axis=1)
    weights = node_weights(meta_flat[:, 3], meta_flat[:, 4], GRID)
    shifts = jnp.sum(warp_grid[tilt_local] * weights[:, None, :], axis=2)
    block_len = math.gcd(slot_total, 16)
    block_count = slot_total // block_len
    per_slot = lax.map(
        one_block,
        (
            patch_in.reshape(block_count, block_len, pixels, pixels),
            (view_local * tilt_dev + tilt_local).reshape(block_count, block_len),
            meta_flat[:, 2].reshape(block_count, block_len),
            shifts.reshape(block_count, block_len, 2),
        ),
    ).reshape(slot_total, 3)
    node_coef = (
        tilt_match.astype(jnp.float32)[:, :, None]
        * per_slot[:, None, 1:3]
        * meta_flat[:, 5, None, None]
    ).reshape(senders, per_sender, 2 * tilt_dev)
    returned = lax.all_to_all(
        per_slot.reshape(senders, per_sender, 3), "dom", split_axis=0, concat_axis=0, tiled=True
    )
    weight_all = weights.reshape(senders, per_sender, node_count)
    own_terms = returned.reshape(buffer_len, 3)[target]
    summed = lax.psum(own_terms, "rep")
    slot_terms = summed.T[:, None, :]
    gradient = jnp.dot(
        node_coef.reshape(-1, 2 * tilt_dev).T,
        weight_all.reshape(-1, node_count),
        precision=lax.Precision.HIGHEST,
        preferred_element_type=jnp.float32,
    ).reshape(tilt_dev, 2, node_count)
    whole_grad = lax.psum(gradient, ("dom", "rep"))
    new_warp = warp_grid - whole_grad / jnp.sqrt(
        whole_grad * whole_grad + TRUST_FLOOR * TRUST_FLOOR
    )
    return (slot_terms, new_warp)


CORES = 2
CHIPS = 4
EXTRA_ROWS = 8
SPEC_ROWS = 16
DELTA = math.asin(AMPLITUDE)
F32 = jnp.float32
BF16 = jnp.bfloat16
OWN, NEAR, CROSS, ON_FAR, ON_OPP, NEAR_PAIR, OPP_PAIR, FAR_PAIR = range(8)


def exact(a, b, dims=(((1,), (0,)), ((), ()))):
    return lax.dot_general(
        a, b, dims, precision=lax.Precision.HIGHEST, preferred_element_type=F32
    )


def contract_last(a, b):
    return lax.dot_general(a, b, (((1,), (1,)), ((), ())), preferred_element_type=F32)


def tables(pixels):
    half = pixels // 2
    k = np.arange(pixels)
    angle = ((k[:, None] * k[None, :]) % pixels).astype(np.float32) * np.float32(
        2.0 * math.pi / pixels
    )
    scale = np.float32(1.0 / math.sqrt(pixels))
    cosine, sine = np.cos(angle) * scale, np.sin(angle) * scale
    pad = np.zeros((SPEC_ROWS - 2, pixels), np.float32)
    edge_c, edge_s = cosine[half : half + 1], sine[half : half + 1]
    first = np.concatenate(
        [cosine[:half], edge_c, edge_c, pad, sine[:half], edge_s, edge_s, pad], axis=0
    )
    second = np.concatenate(
        [np.concatenate([cosine, -sine], axis=1), np.concatenate([-sine, -cosine], axis=1)], axis=0
    )
    edge = np.zeros((SPEC_ROWS, pixels), np.float32)
    edge[2:4] = edge_c
    turn = ((k[:half, None] + k[None, :] == pixels) & (k[:half, None] > 0)).astype(np.float32)
    flip = (((k[:, None] + k[None, :]) % pixels == 0) & (k != half)[None, :]).astype(np.float32)
    unit = np.broadcast_to((k == half).astype(np.float32)[None, :], (16, pixels))
    table = np.arange(2 * pixels)
    focus = np.where(table < pixels, 1.0 + table / pixels, 2.0 + (table - pixels) / half)
    freq = np.where(k < half, k, k - pixels).astype(np.float64)
    chi = 2.0 * math.pi * focus[None, :] * (freq * freq / (half * half))[:, None]
    waves = np.concatenate([np.cos(chi), np.sin(chi)], axis=1)
    levels = np.concatenate([np.cos(chi + 2.0 * DELTA), -np.sin(chi + 2.0 * DELTA)], axis=1)
    low = [jnp.asarray(x, BF16) for x in (first, second, edge, turn, flip, unit, waves)]
    return low + [jnp.asarray(levels, F32)]


def fold_reference(pixels, real, imag, turn, flip, unit, waves, levels):
    half = pixels // 2
    lane = lax.broadcasted_iota(jnp.int32, (1, pixels), 1)
    turned = jnp.dot(turn, jnp.concatenate([real, imag], axis=1), preferred_element_type=F32)
    turned = jnp.concatenate([turned[:, :pixels], turned[:, pixels:]], axis=0).astype(BF16)
    mirror = jnp.dot(turned, flip, preferred_element_type=F32)
    r, i = real.astype(F32), imag.astype(F32)
    column = contract_last(unit, jnp.concatenate([real, imag], axis=0))[0:1]
    column = jnp.where(jnp.concatenate([lane, lane], axis=1) > half, column, 0.0)
    power = r * r + i * i
    mixed = jnp.dot(power.astype(BF16), waves, preferred_element_type=F32)
    swing = jnp.sum(mixed * levels, axis=0, keepdims=True)
    swing = swing[:, : 2 * pixels] + swing[:, 2 * pixels :]
    total = 0.5 * jnp.sum(power) - 0.5 * swing
    high = total.astype(BF16).astype(F32)
    low = total - high
    extra = jnp.concatenate(
        [
            r[half : half + 1], i[half : half + 1], column[:, :pixels], column[:, pixels:],
            high[:, :pixels], high[:, pixels:], low[:, :pixels], low[:, pixels:],
        ],
        axis=0,
    )
    return (r[:half] + mirror[:half]).astype(BF16), (i[:half] - mirror[half:]).astype(BF16), extra


def gather_kernel(cap, view_dev, bounds, guest_bounds, view_ref, tilt_ref, pos_ref, focus_ref,
                  warp_ref, patch_hbm, proj_hbm, first_hbm, second_hbm, edge_hbm, turn_hbm,
                  flip_hbm, unit_hbm, waves_hbm, levels_hbm, terms_ref, new_ref, first_ref,
                  second_ref, edge_ref, turn_ref, flip_ref, unit_ref, waves_ref, levels_ref,
                  patch_ref, proj_ref, own_ref, pair_ref, near_ref, near_pair_ref, opp_ref,
                  opp_pair_ref, far_ref, far_pair_ref, guest_ref, visit_ref, guest_last_ref,
                  visit_last_ref, spec_ref,
                  visit_spec_ref, factor_ref, visit_factor_ref, cols_ref, visit_cols_ref,
                  node_ref, visit_node_ref, match_ref, sums_ref, visit_sums_ref, ints_ref,
                  visit_ints_ref, ints_s, visit_ints_s, meta_ref, visit_meta_ref, grad_ref,
                  sent_ref, held_ref, back_ref, back_in_ref, load_sem, table_sem, send_sem, recv_sem,
                  guest_send, guest_recv, misc_send, misc_recv, grad_send, grad_recv):
    slots, pixels = patch_ref.shape[0], patch_ref.shape[1]
    half = pixels // 2
    refs = own_ref.shape[0]
    tilt_dev = warp_ref.shape[0]
    node_count = warp_ref.shape[2]
    chunks = len(bounds) - 1
    guests = guest_ref.shape[0]
    guest_chunks = len(guest_bounds) - 1
    last_guest = guest_bounds[guest_chunks - 1]
    devices = CHIPS * CORES
    padded = devices * cap
    far_base = padded - guests
    wide = sums_ref.shape[1]
    shift_lanes = wide - pixels
    me = lax.axis_index("dom")
    chip = me // CORES
    core = me % CORES
    partner = chip * CORES + (1 - core)
    mate_chip = chip + 1 - 2 * (chip % 2)
    mate = mate_chip * CORES + core
    cross = (CHIPS - 1 - chip) * CORES + core
    inner = (chip > 0) & (chip < CHIPS - 1)
    outer = jnp.logical_not(inner)
    barrier = pltpu.get_barrier_semaphore()

    def greet(device):
        pl.semaphore_signal(
            barrier, inc=1, device_id={"dom": device}, device_id_type=pl.DeviceIdType.MESH
        )

    greet(mate)
    greet(partner)

    @pl.when(inner)
    def _():
        greet(cross)

    def load_proj(c):
        rows = pl.ds(bounds[c], bounds[c + 1] - bounds[c])
        return pltpu.make_async_copy(proj_hbm.at[rows], proj_ref.at[rows], load_sem.at[c])

    load_patch = pltpu.make_async_copy(patch_hbm, patch_ref, load_sem.at[chunks])
    sources = (turn_hbm, flip_hbm, unit_hbm, waves_hbm, levels_hbm, first_hbm, second_hbm, edge_hbm)
    targets = (turn_ref, flip_ref, unit_ref, waves_ref, levels_ref, first_ref, second_ref, edge_ref)
    load_tables = [
        pltpu.make_async_copy(a, b, table_sem.at[n]) for n, (a, b) in enumerate(zip(sources, targets))
    ]
    fold_tables = 5
    load_proj(0).start()
    for load in load_tables:
        load.start()
    for c in range(1, chunks):
        load_proj(c).start()
    load_patch.start()

    def remote(src, dst, send, recv, target):
        return pltpu.make_async_remote_copy(
            src_ref=src, dst_ref=dst, send_sem=send, recv_sem=recv,
            device_id={"dom": target}, device_id_type=pl.DeviceIdType.MESH,
        )

    flows = {
        OWN: (own_ref, pair_ref, partner),
        NEAR: (own_ref, near_ref, mate),
        CROSS: (own_ref, opp_ref, cross),
        ON_FAR: (near_ref, far_ref, cross),
        ON_OPP: (opp_ref, opp_ref, mate),
        NEAR_PAIR: (near_ref, near_pair_ref, partner),
        OPP_PAIR: (opp_ref, opp_pair_ref, partner),
        FAR_PAIR: (far_ref, far_pair_ref, partner),
    }

    def flow(kind, c):
        src, dst, target = flows[kind]
        rows = pl.ds(bounds[c], bounds[c + 1] - bounds[c])
        return remote(
            src.at[rows], dst.at[rows], send_sem.at[kind, c], recv_sem.at[kind, c], target
        )

    def guest_copy(g):
        if g == guest_chunks - 1:
            return remote(
                guest_last_ref, visit_last_ref, guest_send.at[g], guest_recv.at[g], mate
            )
        rows = pl.ds(guest_bounds[g], guest_bounds[g + 1] - guest_bounds[g])
        return remote(
            guest_ref.at[rows], visit_ref.at[rows], guest_send.at[g], guest_recv.at[g], mate
        )

    meta_copy = remote(meta_ref, visit_meta_ref, misc_send.at[0], misc_recv.at[0], mate)
    back_copy = remote(back_ref, back_in_ref, misc_send.at[1], misc_recv.at[1], mate)

    def fold(c):
        load_proj(c).wait()

        def one(i, carry):
            n = bounds[c] + i
            top, bottom, extra = fold_reference(
                pixels, proj_ref[n, 0], proj_ref[n, 1], turn_ref[...], flip_ref[...],
                unit_ref[...], waves_ref[...], levels_ref[...],
            )
            own_ref[n, :half] = top
            own_ref[n, half:pixels] = bottom
            own_ref[n, pixels:] = extra.astype(BF16)
            return carry

        lax.fori_loop(0, bounds[c + 1] - bounds[c], one, 0, unroll=2)

    def send_own(c):
        flow(NEAR, c).start()

        @pl.when(inner)
        def _():
            flow(CROSS, c).start()

        flow(OWN, c).start()

    lane = lax.broadcasted_iota(jnp.int32, (1, pixels), 1)
    line = jnp.where(lane < half, lane, lane - pixels).astype(F32)
    lane_f = lane.astype(F32)

    def route():
        chip_f, core_f, mate_f = chip.astype(F32), core.astype(F32), mate_chip.astype(F32)
        opp_f = (CHIPS - 1) - jnp.where(inner, chip_f, mate_f)
        view = view_ref[...].astype(F32)
        owner = jnp.floor((view + 0.5) * (1.0 / view_dev))
        owner_chip = jnp.floor((owner + 0.5) * (1.0 / CORES))
        owner_core = owner - CORES * owner_chip
        role = jnp.where(
            owner_chip == chip_f, 0.0,
            jnp.where(owner_chip == mate_f, 1.0, jnp.where(owner_chip == opp_f, 2.0, 3.0)),
        )
        key = role * CORES + jnp.where(owner_core == core_f, 0.0, 1.0)
        tilt = tilt_ref[...].astype(F32)
        which = (view - owner * view_dev) * tilt_dev + tilt
        pos = pos_ref[...].astype(F32)
        block = jnp.concatenate(
            [key, which, pos, focus_ref[...].astype(F32), tilt,
             jnp.zeros((slots - 6, slots), F32)],
            axis=0,
        )
        cols = block.T
        cols_ref[...] = cols
        row = lax.broadcasted_iota(jnp.int32, (slots, slots), 0)
        col = lax.broadcasted_iota(jnp.int32, (slots, slots), 1)
        ahead = jnp.where((cols[:, 0:1] == key) & (col < row), 1.0, 0.0)
        target = cols[:, 0:1] * cap + jnp.sum(ahead, axis=1, keepdims=True)
        place = lax.broadcasted_iota(jnp.int32, (1, wide), 1).astype(F32)
        match = jnp.where(target == place, 1.0, 0.0)
        match_ref[...] = match
        slot = lax.broadcasted_iota(jnp.int32, (slots, wide), 0).astype(F32)
        source = jnp.sum(match * slot, axis=0, keepdims=True)
        chosen = jnp.sum(match * cols[:, 1:2], axis=0, keepdims=True)
        ints = jnp.concatenate([source, chosen, jnp.zeros((6, wide), F32)], axis=0)
        ints_ref[...] = (ints + 0.5).astype(jnp.int32)

    def node_weights_of(cols):
        node = lax.broadcasted_iota(jnp.int32, (1, node_count), 1).astype(F32)
        node_y = jnp.floor((node + 0.5) * (1.0 / GRID))
        node_x = node - node_y * GRID
        weight_x = jnp.maximum(0.0, 1.0 - jnp.abs(cols[:, 2:3] * (GRID - 1) - node_x))
        weight_y = jnp.maximum(0.0, 1.0 - jnp.abs(cols[:, 3:4] * (GRID - 1) - node_y))
        return weight_y * weight_x

    def place_nodes():
        weights = node_weights_of(cols_ref)
        hits = jnp.where(cols_ref[:, 5:6] == lane_f[:, :16], 1.0, 0.0)
        spare = jnp.zeros((16 - tilt_dev, node_count), F32)
        for axis in range(2):
            grid = jnp.concatenate([warp_ref[:, axis, :], spare], axis=0)
            shift = jnp.sum(exact(hits, grid) * weights, axis=1, keepdims=True)
            cols_ref[:, 6 + axis : 7 + axis] = shift
        meta = exact(cols_ref[...].T[:8], match_ref[...])
        meta_ref[...] = meta
        spare = jnp.zeros((pixels - 8, pixels), F32)
        for at in range(0, wide, pixels):
            cols = jnp.concatenate([meta[:, at : at + pixels], spare], axis=0).T
            node_ref[at : at + pixels] = node_weights_of(cols)

    step_angle = 2.0 * math.pi / pixels
    norm = 1.0 / (half * half)
    block_slots = 16

    def factors(cols_ref, factor_ref, block, carry):
        rows = pl.ds(pl.multiple_of(block * block_slots, block_slots), block_slots)
        cols = cols_ref[rows]
        focus, shift_x, shift_y = cols[:, 4:5], cols[:, 6:7], cols[:, 7:8]
        chi = math.pi * focus * (line * line * norm)
        phi_x = step_angle * shift_x * line
        phi_y = step_angle * shift_y * line
        c_x, s_x = jnp.cos(chi), jnp.sin(chi)
        s_y = s_x * math.cos(DELTA) + c_x * math.sin(DELTA)
        c_y = c_x * math.cos(DELTA) - s_x * math.sin(DELTA)
        p_x, q_x, p_y, q_y = jnp.cos(phi_x), jnp.sin(phi_x), jnp.cos(phi_y), jnp.sin(phi_y)
        tall = (s_y * p_y, s_y * q_y, c_y * p_y, c_y * q_y)
        a, b, c, d = c_x * p_x, c_x * q_x, s_x * p_x, s_x * q_x
        e, f, g, h = (v[:, half : half + 1] for v in (a, b, c, d))
        edge_re = -(tall[0] * e - tall[1] * f + tall[2] * g - tall[3] * h)
        edge_im = -(tall[0] * f + tall[1] * e + tall[2] * h + tall[3] * g)
        tall = tuple(jnp.where(lane == half + 1, pltpu.roll(v, 1, 1), v) for v in tall)
        place = jnp.where(focus < 2.0, (focus - 1.0) * pixels, pixels + (focus - 2.0) * half)
        hit_low = jnp.where(place == lane_f, -0.5, 0.0)
        hit_high = jnp.where(place == lane_f + pixels, -0.5, 0.0)
        zero = jnp.zeros_like(a)
        values = tall + (a, b, c, d, edge_re, edge_im, zero, zero,
                         hit_low, hit_high, hit_low, hit_high)
        for index, value in enumerate(values):
            factor_ref[rows, index] = value
        return carry

    row8 = lax.broadcasted_iota(jnp.int32, (8, pixels), 0)
    main_rows = half + SPEC_ROWS

    def spectra(blocks, factor_blocks, put):
        count = len(blocks)
        wides = []
        for n in range(0, count, 2):
            both = jnp.concatenate(blocks[n : n + 2], axis=1)
            v = jnp.dot(first_ref[...], both, preferred_element_type=F32)
            edge = contract_last(edge_ref[...], jnp.concatenate(blocks[n : n + 2], axis=0))
            for part in range(2):
                at = slice(part * pixels, (part + 1) * pixels)
                one = jnp.concatenate([v[:half, at], v[half:main_rows, at] + edge[:, at]], axis=0)
                wides.append(
                    jnp.concatenate([one.astype(BF16), v[main_rows:, at].astype(BF16)], axis=1)
                )
        spectrum = jnp.dot(
            jnp.concatenate(wides, axis=0), second_ref[...], preferred_element_type=F32
        )
        for n in range(count):
            factor = factor_blocks[n]
            tall = factor[0:4]
            a, b, c, d = factor[4:5], factor[5:6], factor[6:7], factor[7:8]
            rows = jnp.concatenate(
                [
                    jnp.concatenate([-a, b, -c, d], axis=0),
                    jnp.concatenate([-b, -a, -d, -c], axis=0),
                ],
                axis=1,
            )
            tall_high = tall.astype(BF16).astype(F32)
            row_high = rows.astype(BF16).astype(F32)
            tall_low, row_low = tall - tall_high, rows - row_high
            tall_all = jnp.concatenate(
                [tall_high, tall_high, tall_low, jnp.zeros_like(tall_low)], axis=0
            ).astype(BF16)
            row_all = jnp.concatenate(
                [row_high, row_low, row_high, jnp.zeros_like(row_low)], axis=0
            ).astype(BF16)
            turn = lax.dot_general(
                tall_all, row_all, (((0,), (0,)), ((), ())), preferred_element_type=F32
            )
            base = n * main_rows
            x_re = spectrum[base : base + half, :pixels]
            x_im = spectrum[base : base + half, pixels:]
            t_re, t_im = turn[:half, :pixels], turn[:half, pixels:]
            put(n, slice(0, half), x_re * t_re - x_im * t_im)
            put(n, slice(half, pixels), x_re * t_im + x_im * t_re)
            power = x_re * x_re + x_im * x_im
            power = jnp.sum(power.reshape(half // 8, 8, pixels), axis=0) * 2.0 - jnp.where(
                row8 == 0, power[:8], 0.0
            )
            x_re = spectrum[base + half : base + half + 8, :pixels]
            x_im = spectrum[base + half : base + half + 8, pixels:]
            power = power + jnp.where(row8 == 0, x_re * x_re + x_im * x_im, 0.0)
            edge_turn = (row8 == 2) | (row8 == 3)
            t_re = jnp.where(edge_turn, factor[8:9], turn[half : half + 8, :pixels])
            t_im = jnp.where(edge_turn, factor[9:10], turn[half : half + 8, pixels:])
            y_re = x_re * t_re - x_im * t_im
            y_im = x_re * t_im + x_im * t_re
            odd = row8 % 2 == 1
            straight = jnp.where(odd, y_im, y_re)
            crossed = jnp.where(odd, -y_re, y_im)
            straight = jnp.where(row8 < 4, straight, factor[8:16])
            power = jnp.sum(power, axis=0, keepdims=True)
            high = power.astype(BF16).astype(F32)
            crossed = jnp.where(
                row8 < 4, crossed,
                jnp.where(row8 == 4, high, jnp.where(row8 == 5, power - high, 0.0)),
            )
            put(n, slice(pixels, pixels + 16), jnp.concatenate([straight, crossed], axis=0))

    weight_x = jnp.where(row8 < 2, line, jnp.where(row8 < 4, -float(half), 0.0))
    weight_y = jnp.where(row8 < 2, -float(half), jnp.where(row8 < 4, line, 0.0))
    freq_y = lax.broadcasted_iota(jnp.int32, (half, pixels), 0).astype(F32)

    def stack(x):
        return jnp.sum(x.reshape(half // 8, 8, pixels), axis=0)

    def compare(y, ref):
        y = y.astype(F32)
        r = ref.astype(F32)
        y_re, y_im, straight = y[:half], y[half:pixels], y[pixels : pixels + 8]
        crossed = y[pixels + 8 :]
        r_re, r_im, extra = r[:half], r[half:pixels], r[pixels:]
        match = stack(y_re * r_re + y_im * r_im) + straight * extra
        swirl = y_im * r_re - y_re * r_im
        edge = crossed * extra
        energy = jnp.where((row8 == 4) | (row8 == 5), crossed, 0.0) - 2.0 * match
        grad_x = stack(swirl) * line + edge * weight_x
        grad_y = stack(swirl * freq_y) + edge * weight_y
        return energy, grad_x, grad_y

    def meet(y, ref, out_ref, place):
        found = compare(y, ref)
        for index, value in enumerate(found):
            out_ref[index, pl.ds(place, 1)] = jnp.sum(value, axis=0, keepdims=True)
        return found

    def slot_at(p):
        return jnp.clip(ints_s[0, p], 0, slots - 1)

    def ref_at(held, p):
        return jnp.clip(held[1, p], 0, refs - 1)

    def process(refs_ref, role):
        def some(step, carry):
            for u in range(4):
                p = role * cap + step * 4 + u
                meet(spec_ref[slot_at(p)], refs_ref[ref_at(ints_s, p)], sums_ref, p)
            return carry

        lax.fori_loop(0, cap // 4, some, 0)

    def entertain(low, high):
        def some(refs_ref, step, carry):
            for u in range(4):
                g = step * 4 + u
                p = far_base + g
                held = refs_ref[ref_at(visit_ints_s, p)]
                meet(visit_spec_ref[g], held, visit_sums_ref, p - shift_lanes)
            return carry

        for refs_ref, least, most in ((far_ref, 0, cap), (far_pair_ref, cap, 2 * cap)):
            a, b = max(low, least), min(high, most)
            if b > a:
                lax.fori_loop(a // 4, b // 4, functools.partial(some, refs_ref), 0)

    def transform(low, high):
        def some(step, carry):
            base = low + step * 4

            def put(n, rows, value):
                spec_ref[base + n, rows] = value

            four = [base + n for n in range(4)]
            spectra([patch_ref[s] for s in four], [factor_ref[s] for s in four], put)
            return carry

        lax.fori_loop(0, (high - low) // 4, some, 0)

    def transform_visit(low, high):
        def some(step, carry):
            base = low + step * 4

            def put(n, rows, value):
                visit_spec_ref[base + n, rows] = value

            four = [base + n for n in range(4)]
            spectra(
                [visit_ref[g] for g in four],
                [visit_factor_ref[far_base - shift_lanes + g] for g in four],
                put,
            )
            return carry

        lax.fori_loop(0, (high - low) // 4, some, 0)

    def pack(g, carry):
        guest_ref[g] = patch_ref[slot_at(far_base + g)]
        return carry

    for load in load_tables[:fold_tables]:
        load.wait()
    fold(0)
    fold(1)

    @pl.when(inner)
    def _():
        pl.semaphore_wait(barrier, 3)

    @pl.when(outer)
    def _():
        pl.semaphore_wait(barrier, 2)

    send_own(0)
    for c in range(2, chunks):
        fold(c)
        send_own(c - 1)
    route()
    ints_load = pltpu.make_async_copy(ints_ref, ints_s, load_sem.at[chunks + 1])
    ints_load.start()
    sums_ref[...] = jnp.zeros_like(sums_ref)
    visit_sums_ref[...] = jnp.zeros_like(visit_sums_ref)
    send_own(chunks - 1)
    place_nodes()
    load_patch.wait()
    ints_load.wait()

    @pl.when(outer)
    def _():
        lax.fori_loop(0, last_guest, pack, 0, unroll=4)

    lax.fori_loop(
        0, slots // block_slots, functools.partial(factors, cols_ref, factor_ref), 0
    )

    @pl.when(outer)
    def _():
        meta_copy.start()
        for g in range(guest_chunks - 1):
            guest_copy(g).start()

    for load in load_tables[fold_tables:]:
        load.wait()

    def pass_on(c):
        flow(NEAR, c).wait_recv()

        @pl.when(inner)
        def _():
            flow(ON_FAR, c).start()
            flow(CROSS, c).wait_recv()
            flow(ON_OPP, c).start()
            flow(OPP_PAIR, c).start()

        flow(NEAR_PAIR, c).start()

    segments = 4
    seg = slots // segments
    done = 0
    for n in range(segments):
        transform(n * seg, (n + 1) * seg)
        upto = chunks * (n + 1) // segments
        while done < upto:
            pass_on(done)
            done += 1

    @pl.when(outer)
    def _():
        for g in range(last_guest, guests):
            guest_last_ref[g - last_guest] = spec_ref[slot_at(far_base + g)].astype(BF16)

    process(own_ref, 0)

    @pl.when(outer)
    def _():
        guest_copy(guest_chunks - 1).start()

    for c in range(chunks):
        flow(OWN, c).wait_recv()
    process(pair_ref, 1)
    process(near_ref, 2)
    for c in range(chunks):
        flow(NEAR_PAIR, c).wait_recv()
    process(near_pair_ref, 3)

    @pl.when(outer)
    def _():
        for c in range(chunks):
            flow(ON_OPP, c).wait_recv()
            flow(OPP_PAIR, c).start()

    process(opp_ref, 4)
    for c in range(chunks):
        flow(OPP_PAIR, c).wait_recv()
    process(opp_pair_ref, 5)

    visit_load = pltpu.make_async_copy(visit_ints_ref, visit_ints_s, load_sem.at[chunks + 2])
    ones = jnp.ones((8, pixels), F32)
    area = 1.0 / (pixels * pixels)
    scale = jnp.where(row8 == 0, area, 2.0 * area * step_angle)

    def gather_rows(from_ref):
        parts = [exact(ones, from_ref[k], (((1,), (1,)), ((), ()))) for k in range(3)]
        row = lax.broadcasted_iota(jnp.int32, parts[0].shape, 0)
        return jnp.where(row == 0, parts[0], jnp.where(row == 1, parts[1], parts[2])) * scale[:, 0:1]

    def gradient(on_tilt, terms, node_ref, first):
        for axis in range(2):
            coef = jnp.where(on_tilt, terms[1 + axis : 2 + axis], 0.0)
            grad = exact(coef, node_ref[...])[:tilt_dev]
            at = slice(axis * node_count, (axis + 1) * node_count)
            grad_ref[:, at] = grad if first else grad_ref[:, at] + grad

    def welcome():
        meta_copy.wait_recv()
        meta = visit_meta_ref[...]
        visit_ints_ref[...] = (meta + 0.5).astype(jnp.int32)
        visit_load.start()
        block = jnp.concatenate(
            [meta[:, shift_lanes:], jnp.zeros((pixels - 8, pixels), F32)], axis=0
        )
        visit_cols_ref[...] = block.T
        visit_node_ref[...] = node_weights_of(visit_cols_ref)
        first = (far_base - shift_lanes) // block_slots
        last = first + guests // block_slots
        lax.fori_loop(
            first, last, functools.partial(factors, visit_cols_ref, visit_factor_ref), 0
        )
        visit_load.wait()

    def bring_far(c):
        flow(ON_FAR, c).wait_recv()
        flow(FAR_PAIR, c).start()

    @pl.when(inner)
    def _():
        welcome()
        brought = 0
        for g in range(guest_chunks - 2):
            while brought < chunks - guest_chunks + 2 + g:
                bring_far(brought)
                brought += 1
            guest_copy(g).wait_recv()
            transform_visit(guest_bounds[g], guest_bounds[g + 1])
        while brought < chunks:
            bring_far(brought)
            brought += 1
        process(far_ref, 6)
        entertain(0, cap)
        for c in range(chunks):
            flow(FAR_PAIR, c).wait_recv()
        process(far_pair_ref, 7)
        entertain(cap, guest_bounds[guest_chunks - 2])
        guest_copy(guest_chunks - 2).wait_recv()
        transform_visit(guest_bounds[guest_chunks - 2], last_guest)
        entertain(guest_bounds[guest_chunks - 2], last_guest)

    def tilts_at(meta):
        tilt = jnp.where(meta[4:5] > 0.5, jnp.floor(meta[5:6] + 0.5), -1.0)
        return lax.broadcasted_iota(jnp.int32, (16, meta.shape[1]), 0).astype(F32) == tilt

    places = gather_rows(sums_ref)
    gradient(tilts_at(meta_ref[...]), places, node_ref, True)

    lane_blocks = range(0, 2 * node_count, pixels)

    def pack_sent(value):
        sent_ref[...] = jnp.concatenate(
            [value[:, at : at + pixels] for at in lane_blocks], axis=0
        ).astype(BF16)

    def grad_copy(hop):
        return remote(
            sent_ref, held_ref.at[hop - 1], grad_send.at[hop - 1], grad_recv.at[hop - 1],
            lax.rem(me + hop, devices),
        )

    @pl.when(inner)
    def _():
        gradient(
            tilts_at(visit_meta_ref[:, shift_lanes:]), gather_rows(visit_sums_ref),
            visit_node_ref, False,
        )

    for c in range(chunks):
        flow(OWN, c).wait_send()
        flow(NEAR, c).wait_send()
        flow(NEAR_PAIR, c).wait_send()
        flow(OPP_PAIR, c).wait_send()

    @pl.when(inner)
    def _():
        for c in range(chunks):
            flow(CROSS, c).wait_send()
            flow(ON_FAR, c).wait_send()
            flow(ON_OPP, c).wait_send()
            flow(FAR_PAIR, c).wait_send()

    @pl.when(outer)
    def _():
        meta_copy.wait_send()
        for g in range(guest_chunks):
            guest_copy(g).wait_send()
        pack_sent(grad_ref[...])

    @pl.when(inner)
    def _():
        guest_copy(guest_chunks - 1).wait_recv()
        total = [grad_ref[:, a * node_count : (a + 1) * node_count] for a in range(2)]
        tilt_col = lax.broadcasted_iota(jnp.int32, (tilt_dev, 1), 0).astype(F32)
        for g in range(last_guest, guests):
            p = far_base + g
            q = p - shift_lanes
            held = far_pair_ref[ref_at(visit_ints_s, p)]
            found = meet(visit_last_ref[g - last_guest], held, visit_sums_ref, q)
            cols = visit_cols_ref[q : q + 1, :]
            here = (jnp.abs(cols[:, 5:6] - tilt_col) < 0.5) & (cols[:, 4:5] > 0.5)
            weights = visit_node_ref[q : q + 1, :]
            for axis in range(2):
                value = jnp.sum(found[1 + axis], axis=(0, 1), keepdims=True)
                value = value * (2.0 * area * step_angle)
                total[axis] = total[axis] + jnp.where(here, value, 0.0) * weights
        for axis in range(2):
            at = slice(axis * node_count, (axis + 1) * node_count)
            grad_ref[:, at] = total[axis]
        pack_sent(jnp.concatenate(total, axis=1))

    for hop in range(1, devices):
        grad_copy(hop).start()

    @pl.when(inner)
    def _():
        back_ref[...] = gather_rows(visit_sums_ref)
        back_copy.start()

    back_in = jnp.zeros((8, pixels), F32)
    cols_ref[:8, :] = back_in

    @pl.when(outer)
    def _():
        back_copy.wait_recv()
        cols_ref[:8, :] = back_in_ref[...]

    places = jnp.concatenate(
        [places[:, :shift_lanes], places[:, shift_lanes:] + cols_ref[:8, :]], axis=1
    )
    terms = exact(places, match_ref[...], (((1,), (1,)), ((), ())))
    for index in range(3):
        terms_ref[index] = terms[index : index + 1]

    @pl.when(inner)
    def _():
        back_copy.wait_send()

    for hop in range(1, devices):
        grad_copy(hop).wait()
    others = held_ref[0].astype(F32)
    for hop in range(2, devices):
        others = others + held_ref[hop - 1].astype(F32)
    total = grad_ref[...] + jnp.concatenate(
        [others[n * tilt_dev : (n + 1) * tilt_dev] for n in range(len(lane_blocks))], axis=1
    )
    change = total / jnp.sqrt(total * total + TRUST_FLOOR * TRUST_FLOOR)
    for axis in range(2):
        at = slice(axis * node_count, (axis + 1) * node_count)
        new_ref[:, axis, :] = warp_ref[:, axis, :] - change[:, at]


def on_device_gathered(
    patches, slot_view, slot_tilt, slot_pos, defocus, projections, warp_grid
):
    pixels = patches.shape[-1]
    slots = patches.shape[1]
    view_dev = projections.shape[0]
    tilt_dev = warp_grid.shape[0]
    node_count = warp_grid.shape[2]
    devices = CHIPS * CORES
    cap = 3 * slots // (2 * devices)
    if slots != pixels or cap % 24 or node_count != GRID * GRID:
        return on_device(
            patches, slot_view, slot_tilt, slot_pos, defocus, projections, warp_grid
        )
    refs = view_dev * tilt_dev
    bounds = sorted({refs * n // 40 for n in (0, 1, 2, 4, 7, 12, 20, 28, 36, 40)})
    chunks = len(bounds) - 1
    guests = CORES * cap
    guest_bounds = [guests * n // 12 for n in (0, 4, 7, 9, 10, 11, 12)]
    guest_chunks = len(guest_bounds) - 1
    wide = 2 * pixels
    rows = pixels + EXTRA_ROWS
    spec_rows = pixels + 2 * EXTRA_ROWS
    vmem = pl.BlockSpec(memory_space=pltpu.VMEM)
    anywhere = pl.BlockSpec(memory_space=pl.ANY)
    dma = pltpu.SemaphoreType.DMA
    block = pltpu.VMEM((refs, rows, pixels), BF16)
    held_tables = tables(pixels)
    scratch = [pltpu.VMEM(x.shape, x.dtype) for x in held_tables] + [
        pltpu.VMEM((slots, pixels, pixels), BF16),
        pltpu.VMEM((refs, 2, pixels, pixels), BF16),
    ] + [block] * 8 + [
        pltpu.VMEM((guests, pixels, pixels), BF16),
        pltpu.VMEM((guests, pixels, pixels), BF16),
        pltpu.VMEM((guests - guest_bounds[-2], spec_rows, pixels), BF16),
        pltpu.VMEM((guests - guest_bounds[-2], spec_rows, pixels), BF16),
        pltpu.VMEM((slots, spec_rows, pixels), F32),
        pltpu.VMEM((guests, spec_rows, pixels), F32),
        pltpu.VMEM((slots, 16, pixels), F32),
        pltpu.VMEM((pixels, 16, pixels), F32),
        pltpu.VMEM((slots, slots), F32),
        pltpu.VMEM((pixels, pixels), F32),
        pltpu.VMEM((wide, node_count), F32),
        pltpu.VMEM((pixels, node_count), F32),
        pltpu.VMEM((slots, wide), F32),
        pltpu.VMEM((3, wide, pixels), F32),
        pltpu.VMEM((3, pixels, pixels), F32),
        pltpu.VMEM((8, wide), jnp.int32),
        pltpu.VMEM((8, wide), jnp.int32),
        pltpu.SMEM((8, wide), jnp.int32),
        pltpu.SMEM((8, wide), jnp.int32),
        pltpu.VMEM((8, wide), F32),
        pltpu.VMEM((8, wide), F32),
        pltpu.VMEM((tilt_dev, 2 * node_count), F32),
        pltpu.VMEM((2 * node_count // pixels * tilt_dev, pixels), BF16),
        pltpu.VMEM((devices - 1, 2 * node_count // pixels * tilt_dev, pixels), BF16),
        pltpu.VMEM((8, pixels), F32),
        pltpu.VMEM((8, pixels), F32),
        dma((chunks + 3,)),
        dma((len(held_tables),)),
        dma((8, chunks)),
        dma((8, chunks)),
        dma((guest_chunks,)),
        dma((guest_chunks,)),
        dma((2,)),
        dma((2,)),
        dma((devices - 1,)),
        dma((devices - 1,)),
    ]
    terms, new_warp = pl.pallas_call(
        functools.partial(gather_kernel, cap, view_dev, bounds, guest_bounds),
        out_shape=(
            pltpu.VMEM((3, 1, slots), F32),
            pltpu.VMEM(warp_grid.shape, F32),
        ),
        in_specs=[vmem] * 5 + [anywhere] * 10,
        out_specs=(vmem, vmem),
        scratch_shapes=scratch,
        compiler_params=pltpu.CompilerParams(
            collective_id=0, has_side_effects=True, vmem_limit_bytes=56 * 1024 * 1024
        ),
        name="gather_sums",
    )(
        slot_view.reshape(1, slots), slot_tilt, slot_pos.reshape(2, slots), defocus, warp_grid,
        patches[0], projections.reshape(refs, 2, pixels, pixels), *held_tables,
    )
    return (terms, new_warp)


def solution(mesh):
    on_chips = mesh.shape["rep"] == 1 and mesh.shape["dom"] == CHIPS * CORES
    body = on_device_gathered if on_chips else on_device
    in_specs = (
        P(("groups", "tilt"), "dom", None, None),
        P(("groups", "tilt"), "dom", None),
        P(("groups", "tilt"), "dom"),
        P(None, ("groups", "tilt"), "dom"),
        P(("groups", "tilt"), "dom"),
        P(("groups", "dom"), "tilt", None, "rep", None),
        P(("groups", "tilt"), None, None),
    )
    out_specs = (P(None, ("groups", "tilt"), "dom"), P(("groups", "tilt"), None, None))
    return jax.shard_map(
        body, mesh=mesh, in_specs=in_specs, out_specs=out_specs, check_vma=False
    )
```

```python
import functools
import math

import jax
import jax.numpy as jnp
import numpy as np
from jax import lax
from jax.experimental import pallas as pl
from jax.experimental.pallas import tpu as pltpu
from jax.sharding import PartitionSpec as P

GRID = 16


AMPLITUDE = 0.07
TRUST_FLOOR = 0.02


def signed_freq(index, pixels):
    return jnp.where(index < pixels // 2, index, index - pixels).astype(jnp.float32)


def dft_tables(freq_rows, pixels):
    columns = jnp.arange(pixels, dtype=jnp.int32)
    table_scale = 1.0 / math.sqrt(pixels)
    turns_rows = (freq_rows[:, None] * columns[None, :] % pixels).astype(jnp.float32) * (
        2.0 * math.pi / pixels
    )
    turns_full = (columns[:, None] * columns[None, :] % pixels).astype(jnp.float32) * (
        2.0 * math.pi / pixels
    )
    row_table = jnp.concatenate([jnp.cos(turns_rows), jnp.sin(turns_rows)], axis=0) * table_scale
    col_table = jnp.concatenate([jnp.cos(turns_full), jnp.sin(turns_full)], axis=1) * table_scale
    return (row_table.astype(jnp.bfloat16), col_table.astype(jnp.bfloat16))


def node_weights(pos_x, pos_y, grid_side):
    knot_pos = jnp.arange(grid_side, dtype=jnp.int32).astype(jnp.float32)
    weight_x = jnp.maximum(0.0, 1.0 - jnp.abs(pos_x[:, None] * (grid_side - 1) - knot_pos[None, :]))
    weight_y = jnp.maximum(0.0, 1.0 - jnp.abs(pos_y[:, None] * (grid_side - 1) - knot_pos[None, :]))
    return (weight_y[:, :, None] * weight_x[:, None, :]).reshape(
        pos_x.shape[0], grid_side * grid_side
    )


def spectral_terms(spectrum, ref_blk, focus_blk, shift_blk, freq_rows, pixels):
    row_total = freq_rows.shape[0]
    v_one_cos = spectrum[:, :row_total, :pixels]
    v_one_sin = spectrum[:, :row_total, pixels:]
    v_two_cos = spectrum[:, row_total:, :pixels]
    v_two_sin = spectrum[:, row_total:, pixels:]
    real_part = v_one_cos - v_two_sin
    imag_part = -(v_one_sin + v_two_cos)
    freq_y = signed_freq(freq_rows, pixels)[None, :, None]
    freq_x = signed_freq(jnp.arange(pixels, dtype=jnp.int32), pixels)[None, None, :]
    nyquist = pixels / 2.0
    radius = (freq_y * freq_y + freq_x * freq_x) / (nyquist * nyquist)
    aberration = math.pi * focus_blk[:, None, None] * radius
    contrast = -(
        math.sqrt(1.0 - AMPLITUDE * AMPLITUDE) * jnp.sin(aberration)
        + AMPLITUDE * jnp.cos(aberration)
    )
    phase_angle = (
        2.0
        * math.pi
        / pixels
        * (freq_x * shift_blk[:, 0, None, None] + freq_y * shift_blk[:, 1, None, None])
    )
    cosine = jnp.cos(phase_angle)
    sine_part = jnp.sin(phase_angle)
    ref_real = ref_blk[:, 0].astype(jnp.float32)
    ref_imag = ref_blk[:, 1].astype(jnp.float32)
    model_real = contrast * (ref_real * cosine + ref_imag * sine_part)
    model_imag = contrast * (ref_imag * cosine - ref_real * sine_part)
    diff_real = real_part - model_real
    diff_imag = imag_part - model_imag
    inverse_area = 1.0 / (pixels * pixels)
    energy = jnp.sum(diff_real * diff_real + diff_imag * diff_imag, axis=(1, 2)) * inverse_area
    cross_term = diff_imag * model_real - diff_real * model_imag
    grad_x = 2.0 * inverse_area * jnp.sum(2.0 * math.pi / pixels * freq_x * cross_term, axis=(1, 2))
    grad_y = 2.0 * inverse_area * jnp.sum(2.0 * math.pi / pixels * freq_y * cross_term, axis=(1, 2))
    return jnp.stack([energy, grad_x, grad_y], axis=1)


def on_device(patches, slot_view, slot_tilt, slot_pos, defocus, projections, warp_grid):
    owners = lax.axis_size("dom")
    slot_count = patches.shape[1]
    pixels = patches.shape[-1]
    view_dev = projections.shape[0]
    tilt_dev = warp_grid.shape[0]
    node_count = warp_grid.shape[2]
    capacity = 3 * slot_count // (2 * owners)
    buffer_len = owners * capacity
    chosen_view = slot_view[0, :, 0]
    owner_of = chosen_view // view_dev
    owner_hits = (owner_of[:, None] == jnp.arange(owners, dtype=jnp.int32)[None, :]).astype(
        jnp.int32
    )
    earlier = jnp.cumsum(owner_hits, axis=0) - owner_hits
    slot_rank = jnp.sum(earlier * owner_hits, axis=1)
    target = owner_of * capacity + slot_rank
    matches = target[None, :] == jnp.arange(buffer_len, dtype=jnp.int32)[:, None]
    source = jnp.sum(
        jnp.where(matches, jnp.arange(slot_count, dtype=jnp.int32)[None, :], 0), axis=1
    )
    filled = jnp.any(matches, axis=1)
    patch_rows = jnp.where(filled[:, None, None], patches[0][source], jnp.zeros((), jnp.bfloat16))
    slot_meta = jnp.stack(
        [
            slot_tilt[0].astype(jnp.float32),
            (chosen_view % view_dev).astype(jnp.float32),
            defocus[0].astype(jnp.float32),
            slot_pos[0, 0].astype(jnp.float32),
            slot_pos[1, 0].astype(jnp.float32),
            jnp.ones((slot_count,), jnp.float32),
        ],
        axis=1,
    )
    meta_rows = jnp.where(filled[:, None], slot_meta[source], 0.0).astype(jnp.bfloat16)
    patch_buffer = patch_rows.reshape(owners, capacity, pixels, pixels)
    meta_buffer = meta_rows.reshape(owners, capacity, 6)
    row_span = projections.shape[3]
    freq_rows = lax.axis_index("rep") * row_span + jnp.arange(row_span, dtype=jnp.int32)
    row_table, col_table = dft_tables(freq_rows, pixels)
    row_total = freq_rows.shape[0]
    projected_flat = projections.reshape(view_dev * tilt_dev, 2, row_total, pixels)
    tilt_iota = jnp.arange(tilt_dev, dtype=jnp.int32)
    view_iota = jnp.arange(view_dev, dtype=jnp.int32)

    def one_block(inputs):
        patch_blk, index_blk, focus_blk, shift_blk = inputs
        ref_blk = projected_flat[index_blk]
        first_pass = jnp.einsum(
            "fy,byx->bfx", row_table, patch_blk, preferred_element_type=jnp.float32
        ).astype(jnp.bfloat16)
        spectrum = jnp.einsum(
            "bfx,xk->bfk", first_pass, col_table, preferred_element_type=jnp.float32
        )
        return spectral_terms(spectrum, ref_blk, focus_blk, shift_blk, freq_rows, pixels)

    patch_in = lax.all_to_all(patch_buffer, "dom", split_axis=0, concat_axis=0, tiled=True)
    meta_in = lax.all_to_all(meta_buffer, "dom", split_axis=0, concat_axis=0, tiled=True)
    senders = patch_in.shape[0]
    per_sender = patch_in.shape[1]
    slot_total = senders * per_sender
    meta_flat = meta_in.reshape(slot_total, 6).astype(jnp.float32)
    tilt_match = meta_flat[:, 0:1] == tilt_iota.astype(jnp.float32)[None, :]
    view_match = meta_flat[:, 1:2] == view_iota.astype(jnp.float32)[None, :]
    tilt_local = jnp.sum(jnp.where(tilt_match, tilt_iota[None, :], 0), axis=1)
    view_local = jnp.sum(jnp.where(view_match, view_iota[None, :], 0), axis=1)
    weights = node_weights(meta_flat[:, 3], meta_flat[:, 4], GRID)
    shifts = jnp.sum(warp_grid[tilt_local] * weights[:, None, :], axis=2)
    block_len = math.gcd(slot_total, 16)
    block_count = slot_total // block_len
    per_slot = lax.map(
        one_block,
        (
            patch_in.reshape(block_count, block_len, pixels, pixels),
            (view_local * tilt_dev + tilt_local).reshape(block_count, block_len),
            meta_flat[:, 2].reshape(block_count, block_len),
            shifts.reshape(block_count, block_len, 2),
        ),
    ).reshape(slot_total, 3)
    node_coef = (
        tilt_match.astype(jnp.float32)[:, :, None]
        * per_slot[:, None, 1:3]
        * meta_flat[:, 5, None, None]
    ).reshape(senders, per_sender, 2 * tilt_dev)
    returned = lax.all_to_all(
        per_slot.reshape(senders, per_sender, 3), "dom", split_axis=0, concat_axis=0, tiled=True
    )
    weight_all = weights.reshape(senders, per_sender, node_count)
    own_terms = returned.reshape(buffer_len, 3)[target]
    summed = lax.psum(own_terms, "rep")
    slot_terms = summed.T[:, None, :]
    gradient = jnp.dot(
        node_coef.reshape(-1, 2 * tilt_dev).T,
        weight_all.reshape(-1, node_count),
        precision=lax.Precision.HIGHEST,
        preferred_element_type=jnp.float32,
    ).reshape(tilt_dev, 2, node_count)
    whole_grad = lax.psum(gradient, ("dom", "rep"))
    new_warp = warp_grid - whole_grad / jnp.sqrt(
        whole_grad * whole_grad + TRUST_FLOOR * TRUST_FLOOR
    )
    return (slot_terms, new_warp)


CORES = 2
CHIPS = 4
EXTRA_ROWS = 8
SPEC_ROWS = 16
DELTA = math.asin(AMPLITUDE)
F32 = jnp.float32
BF16 = jnp.bfloat16
OWN, NEAR, CROSS, ON_FAR, ON_OPP, NEAR_PAIR, OPP_PAIR, FAR_PAIR = range(8)


def exact(a, b, dims=(((1,), (0,)), ((), ()))):
    return lax.dot_general(
        a, b, dims, precision=lax.Precision.HIGHEST, preferred_element_type=F32
    )


def contract_last(a, b):
    return lax.dot_general(a, b, (((1,), (1,)), ((), ())), preferred_element_type=F32)


def tables(pixels):
    half = pixels // 2
    k = np.arange(pixels)
    angle = ((k[:, None] * k[None, :]) % pixels).astype(np.float32) * np.float32(
        2.0 * math.pi / pixels
    )
    scale = np.float32(1.0 / math.sqrt(pixels))
    cosine, sine = np.cos(angle) * scale, np.sin(angle) * scale
    pad = np.zeros((SPEC_ROWS - 2, pixels), np.float32)
    edge_c, edge_s = cosine[half : half + 1], sine[half : half + 1]
    first = np.concatenate(
        [cosine[:half], edge_c, edge_c, pad, sine[:half], edge_s, edge_s, pad], axis=0
    )
    second = np.concatenate(
        [np.concatenate([cosine, -sine], axis=1), np.concatenate([-sine, -cosine], axis=1)], axis=0
    )
    edge = np.zeros((SPEC_ROWS, pixels), np.float32)
    edge[2:4] = edge_c
    turn = ((k[:half, None] + k[None, :] == pixels) & (k[:half, None] > 0)).astype(np.float32)
    flip = (((k[:, None] + k[None, :]) % pixels == 0) & (k != half)[None, :]).astype(np.float32)
    unit = np.broadcast_to((k == half).astype(np.float32)[None, :], (16, pixels))
    table = np.arange(2 * pixels)
    focus = np.where(table < pixels, 1.0 + table / pixels, 2.0 + (table - pixels) / half)
    freq = np.where(k < half, k, k - pixels).astype(np.float64)
    chi = 2.0 * math.pi * focus[None, :] * (freq * freq / (half * half))[:, None]
    waves = np.concatenate([np.cos(chi), np.sin(chi)], axis=1)
    levels = np.concatenate([np.cos(chi + 2.0 * DELTA), -np.sin(chi + 2.0 * DELTA)], axis=1)
    low = [jnp.asarray(x, BF16) for x in (first, second, edge, turn, flip, unit, waves)]
    return low + [jnp.asarray(levels, F32)]


def fold_reference(pixels, real, imag, turn, flip, unit, waves, levels):
    half = pixels // 2
    lane = lax.broadcasted_iota(jnp.int32, (1, pixels), 1)
    turned = jnp.dot(turn, jnp.concatenate([real, imag], axis=1), preferred_element_type=F32)
    turned = jnp.concatenate([turned[:, :pixels], turned[:, pixels:]], axis=0).astype(BF16)
    mirror = jnp.dot(turned, flip, preferred_element_type=F32)
    r, i = real.astype(F32), imag.astype(F32)
    column = contract_last(unit, jnp.concatenate([real, imag], axis=0))[0:1]
    column = jnp.where(jnp.concatenate([lane, lane], axis=1) > half, column, 0.0)
    power = r * r + i * i
    mixed = jnp.dot(power.astype(BF16), waves, preferred_element_type=F32)
    swing = jnp.sum(mixed * levels, axis=0, keepdims=True)
    swing = swing[:, : 2 * pixels] + swing[:, 2 * pixels :]
    total = 0.5 * jnp.sum(power) - 0.5 * swing
    high = total.astype(BF16).astype(F32)
    low = total - high
    extra = jnp.concatenate(
        [
            r[half : half + 1], i[half : half + 1], column[:, :pixels], column[:, pixels:],
            high[:, :pixels], high[:, pixels:], low[:, :pixels], low[:, pixels:],
        ],
        axis=0,
    )
    return (r[:half] + mirror[:half]).astype(BF16), (i[:half] - mirror[half:]).astype(BF16), extra


def gather_kernel(cap, view_dev, bounds, guest_bounds, view_ref, tilt_ref, pos_ref, focus_ref,
                  warp_ref, patch_hbm, proj_hbm, first_hbm, second_hbm, edge_hbm, turn_hbm,
                  flip_hbm, unit_hbm, waves_hbm, levels_hbm, terms_ref, new_ref, first_ref,
                  second_ref, edge_ref, turn_ref, flip_ref, unit_ref, waves_ref, levels_ref,
                  patch_ref, proj_ref, own_ref, pair_ref, near_ref, near_pair_ref, opp_ref,
                  opp_pair_ref, far_ref, far_pair_ref, guest_ref, visit_ref, guest_last_ref,
                  visit_last_ref, spec_ref,
                  visit_spec_ref, factor_ref, visit_factor_ref, cols_ref, visit_cols_ref,
                  node_ref, visit_node_ref, match_ref, sums_ref, visit_sums_ref, ints_ref,
                  visit_ints_ref, ints_s, visit_ints_s, meta_ref, visit_meta_ref, grad_ref,
                  sent_ref, mate_grad_ref, held_ref, back_ref, back_in_ref, load_sem, table_sem, send_sem, recv_sem,
                  guest_send, guest_recv, misc_send, misc_recv, grad_send, grad_recv):
    slots, pixels = patch_ref.shape[0], patch_ref.shape[1]
    half = pixels // 2
    refs = own_ref.shape[0]
    tilt_dev = warp_ref.shape[0]
    node_count = warp_ref.shape[2]
    chunks = len(bounds) - 1
    guests = guest_ref.shape[0]
    guest_chunks = len(guest_bounds) - 1
    last_guest = guest_bounds[guest_chunks - 1]
    devices = CHIPS * CORES
    padded = devices * cap
    far_base = padded - guests
    wide = sums_ref.shape[1]
    shift_lanes = wide - pixels
    me = lax.axis_index("dom")
    chip = me // CORES
    core = me % CORES
    partner = chip * CORES + (1 - core)
    mate_chip = chip + 1 - 2 * (chip % 2)
    mate = mate_chip * CORES + core
    cross = (CHIPS - 1 - chip) * CORES + core
    inner = (chip > 0) & (chip < CHIPS - 1)
    outer = jnp.logical_not(inner)
    barrier = pltpu.get_barrier_semaphore()

    def greet(device):
        pl.semaphore_signal(
            barrier, inc=1, device_id={"dom": device}, device_id_type=pl.DeviceIdType.MESH
        )

    greet(mate)
    greet(partner)

    @pl.when(inner)
    def _():
        greet(cross)

    def load_proj(c):
        rows = pl.ds(bounds[c], bounds[c + 1] - bounds[c])
        return pltpu.make_async_copy(proj_hbm.at[rows], proj_ref.at[rows], load_sem.at[c])

    load_patch = pltpu.make_async_copy(patch_hbm, patch_ref, load_sem.at[chunks])
    sources = (turn_hbm, flip_hbm, unit_hbm, waves_hbm, levels_hbm, first_hbm, second_hbm, edge_hbm)
    targets = (turn_ref, flip_ref, unit_ref, waves_ref, levels_ref, first_ref, second_ref, edge_ref)
    load_tables = [
        pltpu.make_async_copy(a, b, table_sem.at[n]) for n, (a, b) in enumerate(zip(sources, targets))
    ]
    fold_tables = 5
    load_proj(0).start()
    for load in load_tables:
        load.start()
    for c in range(1, chunks):
        load_proj(c).start()
    load_patch.start()

    def remote(src, dst, send, recv, target):
        return pltpu.make_async_remote_copy(
            src_ref=src, dst_ref=dst, send_sem=send, recv_sem=recv,
            device_id={"dom": target}, device_id_type=pl.DeviceIdType.MESH,
        )

    flows = {
        OWN: (own_ref, pair_ref, partner),
        NEAR: (own_ref, near_ref, mate),
        CROSS: (own_ref, opp_ref, cross),
        ON_FAR: (near_ref, far_ref, cross),
        ON_OPP: (opp_ref, opp_ref, mate),
        NEAR_PAIR: (near_ref, near_pair_ref, partner),
        OPP_PAIR: (opp_ref, opp_pair_ref, partner),
        FAR_PAIR: (far_ref, far_pair_ref, partner),
    }

    def flow(kind, c):
        src, dst, target = flows[kind]
        rows = pl.ds(bounds[c], bounds[c + 1] - bounds[c])
        return remote(
            src.at[rows], dst.at[rows], send_sem.at[kind, c], recv_sem.at[kind, c], target
        )

    def guest_copy(g):
        if g == guest_chunks - 1:
            return remote(
                guest_last_ref, visit_last_ref, guest_send.at[g], guest_recv.at[g], mate
            )
        rows = pl.ds(guest_bounds[g], guest_bounds[g + 1] - guest_bounds[g])
        return remote(
            guest_ref.at[rows], visit_ref.at[rows], guest_send.at[g], guest_recv.at[g], mate
        )

    meta_copy = remote(meta_ref, visit_meta_ref, misc_send.at[0], misc_recv.at[0], mate)
    back_copy = remote(back_ref, back_in_ref, misc_send.at[1], misc_recv.at[1], mate)

    def fold(c):
        load_proj(c).wait()

        def one(i, carry):
            n = bounds[c] + i
            top, bottom, extra = fold_reference(
                pixels, proj_ref[n, 0], proj_ref[n, 1], turn_ref[...], flip_ref[...],
                unit_ref[...], waves_ref[...], levels_ref[...],
            )
            own_ref[n, :half] = top
            own_ref[n, half:pixels] = bottom
            own_ref[n, pixels:] = extra.astype(BF16)
            return carry

        lax.fori_loop(0, bounds[c + 1] - bounds[c], one, 0, unroll=2)

    def send_own(c):
        flow(NEAR, c).start()

        @pl.when(inner)
        def _():
            flow(CROSS, c).start()

        flow(OWN, c).start()

    lane = lax.broadcasted_iota(jnp.int32, (1, pixels), 1)
    line = jnp.where(lane < half, lane, lane - pixels).astype(F32)
    lane_f = lane.astype(F32)

    def route():
        chip_f, core_f, mate_f = chip.astype(F32), core.astype(F32), mate_chip.astype(F32)
        opp_f = (CHIPS - 1) - jnp.where(inner, chip_f, mate_f)
        view = view_ref[...].astype(F32)
        owner = jnp.floor((view + 0.5) * (1.0 / view_dev))
        owner_chip = jnp.floor((owner + 0.5) * (1.0 / CORES))
        owner_core = owner - CORES * owner_chip
        role = jnp.where(
            owner_chip == chip_f, 0.0,
            jnp.where(owner_chip == mate_f, 1.0, jnp.where(owner_chip == opp_f, 2.0, 3.0)),
        )
        key = role * CORES + jnp.where(owner_core == core_f, 0.0, 1.0)
        tilt = tilt_ref[...].astype(F32)
        which = (view - owner * view_dev) * tilt_dev + tilt
        pos = pos_ref[...].astype(F32)
        block = jnp.concatenate(
            [key, which, pos, focus_ref[...].astype(F32), tilt,
             jnp.zeros((slots - 6, slots), F32)],
            axis=0,
        )
        cols = block.T
        cols_ref[...] = cols
        row = lax.broadcasted_iota(jnp.int32, (slots, slots), 0)
        col = lax.broadcasted_iota(jnp.int32, (slots, slots), 1)
        ahead = jnp.where((cols[:, 0:1] == key) & (col < row), 1.0, 0.0)
        target = cols[:, 0:1] * cap + jnp.sum(ahead, axis=1, keepdims=True)
        place = lax.broadcasted_iota(jnp.int32, (1, wide), 1).astype(F32)
        match = jnp.where(target == place, 1.0, 0.0)
        match_ref[...] = match
        slot = lax.broadcasted_iota(jnp.int32, (slots, wide), 0).astype(F32)
        source = jnp.sum(match * slot, axis=0, keepdims=True)
        chosen = jnp.sum(match * cols[:, 1:2], axis=0, keepdims=True)
        ints = jnp.concatenate([source, chosen, jnp.zeros((6, wide), F32)], axis=0)
        ints_ref[...] = (ints + 0.5).astype(jnp.int32)

    def node_weights_of(cols):
        node = lax.broadcasted_iota(jnp.int32, (1, node_count), 1).astype(F32)
        node_y = jnp.floor((node + 0.5) * (1.0 / GRID))
        node_x = node - node_y * GRID
        weight_x = jnp.maximum(0.0, 1.0 - jnp.abs(cols[:, 2:3] * (GRID - 1) - node_x))
        weight_y = jnp.maximum(0.0, 1.0 - jnp.abs(cols[:, 3:4] * (GRID - 1) - node_y))
        return weight_y * weight_x

    def place_nodes():
        weights = node_weights_of(cols_ref)
        hits = jnp.where(cols_ref[:, 5:6] == lane_f[:, :16], 1.0, 0.0)
        spare = jnp.zeros((16 - tilt_dev, node_count), F32)
        for axis in range(2):
            grid = jnp.concatenate([warp_ref[:, axis, :], spare], axis=0)
            shift = jnp.sum(exact(hits, grid) * weights, axis=1, keepdims=True)
            cols_ref[:, 6 + axis : 7 + axis] = shift
        meta = exact(cols_ref[...].T[:8], match_ref[...])
        meta_ref[...] = meta
        spare = jnp.zeros((pixels - 8, pixels), F32)
        for at in range(0, wide, pixels):
            cols = jnp.concatenate([meta[:, at : at + pixels], spare], axis=0).T
            node_ref[at : at + pixels] = node_weights_of(cols)

    step_angle = 2.0 * math.pi / pixels
    norm = 1.0 / (half * half)
    block_slots = 16

    def factors(cols_ref, factor_ref, block, carry):
        rows = pl.ds(pl.multiple_of(block * block_slots, block_slots), block_slots)
        cols = cols_ref[rows]
        focus, shift_x, shift_y = cols[:, 4:5], cols[:, 6:7], cols[:, 7:8]
        chi = math.pi * focus * (line * line * norm)
        phi_x = step_angle * shift_x * line
        phi_y = step_angle * shift_y * line
        c_x, s_x = jnp.cos(chi), jnp.sin(chi)
        s_y = s_x * math.cos(DELTA) + c_x * math.sin(DELTA)
        c_y = c_x * math.cos(DELTA) - s_x * math.sin(DELTA)
        p_x, q_x, p_y, q_y = jnp.cos(phi_x), jnp.sin(phi_x), jnp.cos(phi_y), jnp.sin(phi_y)
        tall = (s_y * p_y, s_y * q_y, c_y * p_y, c_y * q_y)
        a, b, c, d = c_x * p_x, c_x * q_x, s_x * p_x, s_x * q_x
        e, f, g, h = (v[:, half : half + 1] for v in (a, b, c, d))
        edge_re = -(tall[0] * e - tall[1] * f + tall[2] * g - tall[3] * h)
        edge_im = -(tall[0] * f + tall[1] * e + tall[2] * h + tall[3] * g)
        tall = tuple(jnp.where(lane == half + 1, pltpu.roll(v, 1, 1), v) for v in tall)
        place = jnp.where(focus < 2.0, (focus - 1.0) * pixels, pixels + (focus - 2.0) * half)
        hit_low = jnp.where(place == lane_f, -0.5, 0.0)
        hit_high = jnp.where(place == lane_f + pixels, -0.5, 0.0)
        zero = jnp.zeros_like(a)
        values = tall + (a, b, c, d, edge_re, edge_im, zero, zero,
                         hit_low, hit_high, hit_low, hit_high)
        for index, value in enumerate(values):
            factor_ref[rows, index] = value
        return carry

    row8 = lax.broadcasted_iota(jnp.int32, (8, pixels), 0)
    main_rows = half + SPEC_ROWS

    def spectra(blocks, factor_blocks, put):
        count = len(blocks)
        wides = []
        for n in range(0, count, 2):
            both = jnp.concatenate(blocks[n : n + 2], axis=1)
            v = jnp.dot(first_ref[...], both, preferred_element_type=F32)
            edge = contract_last(edge_ref[...], jnp.concatenate(blocks[n : n + 2], axis=0))
            for part in range(2):
                at = slice(part * pixels, (part + 1) * pixels)
                one = jnp.concatenate([v[:half, at], v[half:main_rows, at] + edge[:, at]], axis=0)
                wides.append(
                    jnp.concatenate([one.astype(BF16), v[main_rows:, at].astype(BF16)], axis=1)
                )
        spectrum = jnp.dot(
            jnp.concatenate(wides, axis=0), second_ref[...], preferred_element_type=F32
        )
        for n in range(count):
            factor = factor_blocks[n]
            tall = factor[0:4]
            a, b, c, d = factor[4:5], factor[5:6], factor[6:7], factor[7:8]
            rows = jnp.concatenate(
                [
                    jnp.concatenate([-a, b, -c, d], axis=0),
                    jnp.concatenate([-b, -a, -d, -c], axis=0),
                ],
                axis=1,
            )
            tall_high = tall.astype(BF16).astype(F32)
            row_high = rows.astype(BF16).astype(F32)
            tall_low, row_low = tall - tall_high, rows - row_high
            tall_all = jnp.concatenate(
                [tall_high, tall_high, tall_low, jnp.zeros_like(tall_low)], axis=0
            ).astype(BF16)
            row_all = jnp.concatenate(
                [row_high, row_low, row_high, jnp.zeros_like(row_low)], axis=0
            ).astype(BF16)
            turn = lax.dot_general(
                tall_all, row_all, (((0,), (0,)), ((), ())), preferred_element_type=F32
            )
            base = n * main_rows
            x_re = spectrum[base : base + half, :pixels]
            x_im = spectrum[base : base + half, pixels:]
            t_re, t_im = turn[:half, :pixels], turn[:half, pixels:]
            put(n, slice(0, half), x_re * t_re - x_im * t_im)
            put(n, slice(half, pixels), x_re * t_im + x_im * t_re)
            power = x_re * x_re + x_im * x_im
            power = jnp.sum(power.reshape(half // 8, 8, pixels), axis=0) * 2.0 - jnp.where(
                row8 == 0, power[:8], 0.0
            )
            x_re = spectrum[base + half : base + half + 8, :pixels]
            x_im = spectrum[base + half : base + half + 8, pixels:]
            power = power + jnp.where(row8 == 0, x_re * x_re + x_im * x_im, 0.0)
            edge_turn = (row8 == 2) | (row8 == 3)
            t_re = jnp.where(edge_turn, factor[8:9], turn[half : half + 8, :pixels])
            t_im = jnp.where(edge_turn, factor[9:10], turn[half : half + 8, pixels:])
            y_re = x_re * t_re - x_im * t_im
            y_im = x_re * t_im + x_im * t_re
            odd = row8 % 2 == 1
            straight = jnp.where(odd, y_im, y_re)
            crossed = jnp.where(odd, -y_re, y_im)
            straight = jnp.where(row8 < 4, straight, factor[8:16])
            power = jnp.sum(power, axis=0, keepdims=True)
            high = power.astype(BF16).astype(F32)
            crossed = jnp.where(
                row8 < 4, crossed,
                jnp.where(row8 == 4, high, jnp.where(row8 == 5, power - high, 0.0)),
            )
            put(n, slice(pixels, pixels + 16), jnp.concatenate([straight, crossed], axis=0))

    weight_x = jnp.where(row8 < 2, line, jnp.where(row8 < 4, -float(half), 0.0))
    weight_y = jnp.where(row8 < 2, -float(half), jnp.where(row8 < 4, line, 0.0))
    freq_y = lax.broadcasted_iota(jnp.int32, (half, pixels), 0).astype(F32)

    def stack(x):
        return jnp.sum(x.reshape(half // 8, 8, pixels), axis=0)

    def compare(y, ref):
        y = y.astype(F32)
        r = ref.astype(F32)
        y_re, y_im, straight = y[:half], y[half:pixels], y[pixels : pixels + 8]
        crossed = y[pixels + 8 :]
        r_re, r_im, extra = r[:half], r[half:pixels], r[pixels:]
        match = stack(y_re * r_re + y_im * r_im) + straight * extra
        swirl = y_im * r_re - y_re * r_im
        edge = crossed * extra
        energy = jnp.where((row8 == 4) | (row8 == 5), crossed, 0.0) - 2.0 * match
        grad_x = stack(swirl) * line + edge * weight_x
        grad_y = stack(swirl * freq_y) + edge * weight_y
        return energy, grad_x, grad_y

    def meet(y, ref, out_ref, place):
        found = compare(y, ref)
        for index, value in enumerate(found):
            out_ref[index, pl.ds(place, 1)] = jnp.sum(value, axis=0, keepdims=True)
        return found

    def slot_at(p):
        return jnp.clip(ints_s[0, p], 0, slots - 1)

    def ref_at(held, p):
        return jnp.clip(held[1, p], 0, refs - 1)

    def process(refs_ref, role):
        def some(step, carry):
            for u in range(4):
                p = role * cap + step * 4 + u
                meet(spec_ref[slot_at(p)], refs_ref[ref_at(ints_s, p)], sums_ref, p)
            return carry

        lax.fori_loop(0, cap // 4, some, 0)

    def entertain(low, high):
        def some(refs_ref, step, carry):
            for u in range(4):
                g = step * 4 + u
                p = far_base + g
                held = refs_ref[ref_at(visit_ints_s, p)]
                meet(visit_spec_ref[g], held, visit_sums_ref, p - shift_lanes)
            return carry

        for refs_ref, least, most in ((far_ref, 0, cap), (far_pair_ref, cap, 2 * cap)):
            a, b = max(low, least), min(high, most)
            if b > a:
                lax.fori_loop(a // 4, b // 4, functools.partial(some, refs_ref), 0)

    def transform(low, high):
        def some(step, carry):
            base = low + step * 4

            def put(n, rows, value):
                spec_ref[base + n, rows] = value

            four = [base + n for n in range(4)]
            spectra([patch_ref[s] for s in four], [factor_ref[s] for s in four], put)
            return carry

        lax.fori_loop(0, (high - low) // 4, some, 0)

    def transform_visit(low, high):
        def some(step, carry):
            base = low + step * 4

            def put(n, rows, value):
                visit_spec_ref[base + n, rows] = value

            four = [base + n for n in range(4)]
            spectra(
                [visit_ref[g] for g in four],
                [visit_factor_ref[far_base - shift_lanes + g] for g in four],
                put,
            )
            return carry

        lax.fori_loop(0, (high - low) // 4, some, 0)

    def pack(g, carry):
        guest_ref[g] = patch_ref[slot_at(far_base + g)]
        return carry

    for load in load_tables[:fold_tables]:
        load.wait()
    fold(0)
    fold(1)

    @pl.when(inner)
    def _():
        pl.semaphore_wait(barrier, 3)

    @pl.when(outer)
    def _():
        pl.semaphore_wait(barrier, 2)

    send_own(0)
    for c in range(2, chunks):
        fold(c)
        send_own(c - 1)
    route()
    ints_load = pltpu.make_async_copy(ints_ref, ints_s, load_sem.at[chunks + 1])
    ints_load.start()
    sums_ref[...] = jnp.zeros_like(sums_ref)
    visit_sums_ref[...] = jnp.zeros_like(visit_sums_ref)
    send_own(chunks - 1)
    place_nodes()
    load_patch.wait()
    ints_load.wait()

    @pl.when(outer)
    def _():
        lax.fori_loop(0, last_guest, pack, 0, unroll=4)

    lax.fori_loop(
        0, slots // block_slots, functools.partial(factors, cols_ref, factor_ref), 0
    )

    @pl.when(outer)
    def _():
        meta_copy.start()
        for g in range(guest_chunks - 1):
            guest_copy(g).start()

    for load in load_tables[fold_tables:]:
        load.wait()

    def pass_on(c):
        flow(NEAR, c).wait_recv()

        @pl.when(inner)
        def _():
            flow(ON_FAR, c).start()
            flow(CROSS, c).wait_recv()
            flow(ON_OPP, c).start()
            flow(OPP_PAIR, c).start()

        flow(NEAR_PAIR, c).start()

    segments = 4
    seg = slots // segments
    done = 0
    for n in range(segments):
        transform(n * seg, (n + 1) * seg)
        upto = chunks * (n + 1) // segments
        while done < upto:
            pass_on(done)
            done += 1

    @pl.when(outer)
    def _():
        for g in range(last_guest, guests):
            guest_last_ref[g - last_guest] = spec_ref[slot_at(far_base + g)].astype(BF16)

    process(own_ref, 0)

    @pl.when(outer)
    def _():
        guest_copy(guest_chunks - 1).start()

    for c in range(chunks):
        flow(OWN, c).wait_recv()
    process(pair_ref, 1)
    process(near_ref, 2)
    for c in range(chunks):
        flow(NEAR_PAIR, c).wait_recv()
    process(near_pair_ref, 3)

    @pl.when(outer)
    def _():
        for c in range(chunks):
            flow(ON_OPP, c).wait_recv()
            flow(OPP_PAIR, c).start()

    process(opp_ref, 4)
    for c in range(chunks):
        flow(OPP_PAIR, c).wait_recv()
    process(opp_pair_ref, 5)

    visit_load = pltpu.make_async_copy(visit_ints_ref, visit_ints_s, load_sem.at[chunks + 2])
    ones = jnp.ones((8, pixels), F32)
    area = 1.0 / (pixels * pixels)
    scale = jnp.where(row8 == 0, area, 2.0 * area * step_angle)

    def gather_rows(from_ref):
        parts = [exact(ones, from_ref[k], (((1,), (1,)), ((), ()))) for k in range(3)]
        row = lax.broadcasted_iota(jnp.int32, parts[0].shape, 0)
        return jnp.where(row == 0, parts[0], jnp.where(row == 1, parts[1], parts[2])) * scale[:, 0:1]

    def gradient(on_tilt, terms, node_ref, first):
        for axis in range(2):
            coef = jnp.where(on_tilt, terms[1 + axis : 2 + axis], 0.0)
            grad = exact(coef, node_ref[...])[:tilt_dev]
            at = slice(axis * node_count, (axis + 1) * node_count)
            grad_ref[:, at] = grad if first else grad_ref[:, at] + grad

    def welcome():
        meta_copy.wait_recv()
        meta = visit_meta_ref[...]
        visit_ints_ref[...] = (meta + 0.5).astype(jnp.int32)
        visit_load.start()
        block = jnp.concatenate(
            [meta[:, shift_lanes:], jnp.zeros((pixels - 8, pixels), F32)], axis=0
        )
        visit_cols_ref[...] = block.T
        visit_node_ref[...] = node_weights_of(visit_cols_ref)
        first = (far_base - shift_lanes) // block_slots
        last = first + guests // block_slots
        lax.fori_loop(
            first, last, functools.partial(factors, visit_cols_ref, visit_factor_ref), 0
        )
        visit_load.wait()

    def bring_far(c):
        flow(ON_FAR, c).wait_recv()
        flow(FAR_PAIR, c).start()

    @pl.when(inner)
    def _():
        welcome()
        brought = 0
        for g in range(guest_chunks - 2):
            while brought < chunks - guest_chunks + 2 + g:
                bring_far(brought)
                brought += 1
            guest_copy(g).wait_recv()
            transform_visit(guest_bounds[g], guest_bounds[g + 1])
        while brought < chunks:
            bring_far(brought)
            brought += 1
        process(far_ref, 6)
        entertain(0, cap)
        for c in range(chunks):
            flow(FAR_PAIR, c).wait_recv()
        process(far_pair_ref, 7)
        entertain(cap, guest_bounds[guest_chunks - 2])
        guest_copy(guest_chunks - 2).wait_recv()
        transform_visit(guest_bounds[guest_chunks - 2], last_guest)
        entertain(guest_bounds[guest_chunks - 2], last_guest)

    def tilts_at(meta):
        tilt = jnp.where(meta[4:5] > 0.5, jnp.floor(meta[5:6] + 0.5), -1.0)
        return lax.broadcasted_iota(jnp.int32, (16, meta.shape[1]), 0).astype(F32) == tilt

    places = gather_rows(sums_ref)
    gradient(tilts_at(meta_ref[...]), places, node_ref, True)

    lane_blocks = range(0, 2 * node_count, pixels)

    def pack_sent(value, more=0.0):
        packed = jnp.concatenate([value[:, at : at + pixels] for at in lane_blocks], axis=0)
        sent_ref[...] = (packed + more).astype(BF16)

    mate_grad = remote(sent_ref, mate_grad_ref, misc_send.at[2], misc_recv.at[2], mate)

    places_to = [
        place * CORES + other
        for place in (CHIPS - 1 - mate_chip, CHIPS - 1 - chip, mate_chip)
        for other in (core, 1 - core)
    ] + [partner]

    def grad_copy(n):
        slot = me - CORES
        return remote(
            sent_ref, held_ref.at[slot], grad_send.at[n], grad_recv.at[slot], places_to[n]
        )

    def grad_from(sender):
        slot = sender - CORES
        return remote(
            sent_ref, held_ref.at[slot], grad_send.at[slot], grad_recv.at[slot], partner
        )

    @pl.when(outer)
    def _():
        pack_sent(grad_ref[...])

    @pl.when(inner)
    def _():
        early = gather_rows(visit_sums_ref)
        back_ref[...] = early
        gradient(tilts_at(visit_meta_ref[:, shift_lanes:]), early, visit_node_ref, False)

    for c in range(chunks):
        flow(OWN, c).wait_send()
        flow(NEAR, c).wait_send()
        flow(NEAR_PAIR, c).wait_send()
        flow(OPP_PAIR, c).wait_send()

    @pl.when(inner)
    def _():
        for c in range(chunks):
            flow(CROSS, c).wait_send()
            flow(ON_FAR, c).wait_send()
            flow(ON_OPP, c).wait_send()
            flow(FAR_PAIR, c).wait_send()

    @pl.when(outer)
    def _():
        mate_grad.start()
        meta_copy.wait_send()
        for g in range(guest_chunks):
            guest_copy(g).wait_send()

    @pl.when(inner)
    def _():
        guest_copy(guest_chunks - 1).wait_recv()
        total = [grad_ref[:, a * node_count : (a + 1) * node_count] for a in range(2)]
        tilt_col = lax.broadcasted_iota(jnp.int32, (tilt_dev, 1), 0).astype(F32)
        back = back_ref[...]
        for g in range(last_guest, guests):
            p = far_base + g
            q = p - shift_lanes
            held = far_pair_ref[ref_at(visit_ints_s, p)]
            found = compare(visit_last_ref[g - last_guest], held)
            cols = visit_cols_ref[q : q + 1, :]
            here = (jnp.abs(cols[:, 5:6] - tilt_col) < 0.5) & (cols[:, 4:5] > 0.5)
            weights = visit_node_ref[q : q + 1, :]
            values = [jnp.sum(x, axis=(0, 1), keepdims=True) for x in found]
            values = [values[0] * area] + [v * (2.0 * area * step_angle) for v in values[1:]]
            for axis in range(2):
                total[axis] = total[axis] + jnp.where(here, values[1 + axis], 0.0) * weights
            for index in range(3):
                back = jnp.where((row8 == index) & (lane == q), values[index], back)
        mate_grad.wait_recv()
        pack_sent(jnp.concatenate(total, axis=1), mate_grad_ref[...].astype(F32))
        back_ref[...] = back
        held_ref[me - CORES] = sent_ref[...]

    @pl.when(inner)
    def _():
        for n in range(devices - 1):
            grad_copy(n).start()
        back_copy.start()

    def put_terms(places):
        terms = exact(places, match_ref[...], (((1,), (1,)), ((), ())))
        for index in range(3):
            terms_ref[index] = terms[index : index + 1]

    @pl.when(inner)
    def _():
        put_terms(places)

    senders = range(CORES, devices - CORES)
    for sender in senders:
        @pl.when(me != sender)
        def _():
            grad_from(sender).wait_recv()

    packed = held_ref[0].astype(F32)
    for n in range(1, len(senders)):
        packed = packed + held_ref[n].astype(F32)
    total = jnp.concatenate(
        [packed[n * tilt_dev : (n + 1) * tilt_dev] for n in range(len(lane_blocks))], axis=1
    )
    change = total / jnp.sqrt(total * total + TRUST_FLOOR * TRUST_FLOOR)
    for axis in range(2):
        at = slice(axis * node_count, (axis + 1) * node_count)
        new_ref[:, axis, :] = warp_ref[:, axis, :] - change[:, at]

    @pl.when(outer)
    def _():
        back_copy.wait_recv()
        put_terms(
            jnp.concatenate(
                [places[:, :shift_lanes], places[:, shift_lanes:] + back_in_ref[...]], axis=1
            )
        )

        mate_grad.wait_send()

    @pl.when(inner)
    def _():
        back_copy.wait_send()
        for n in range(devices - 1):
            grad_copy(n).wait_send()


def on_device_gathered(
    patches, slot_view, slot_tilt, slot_pos, defocus, projections, warp_grid
):
    pixels = patches.shape[-1]
    slots = patches.shape[1]
    view_dev = projections.shape[0]
    tilt_dev = warp_grid.shape[0]
    node_count = warp_grid.shape[2]
    devices = CHIPS * CORES
    cap = 3 * slots // (2 * devices)
    if slots != pixels or cap % 24 or node_count != GRID * GRID:
        return on_device(
            patches, slot_view, slot_tilt, slot_pos, defocus, projections, warp_grid
        )
    refs = view_dev * tilt_dev
    bounds = sorted({refs * n // 40 for n in (0, 1, 2, 4, 7, 12, 20, 28, 36, 40)})
    chunks = len(bounds) - 1
    guests = CORES * cap
    guest_bounds = [guests * n // 12 for n in (0, 4, 7, 9, 10, 11, 12)]
    guest_chunks = len(guest_bounds) - 1
    wide = 2 * pixels
    rows = pixels + EXTRA_ROWS
    spec_rows = pixels + 2 * EXTRA_ROWS
    vmem = pl.BlockSpec(memory_space=pltpu.VMEM)
    anywhere = pl.BlockSpec(memory_space=pl.ANY)
    dma = pltpu.SemaphoreType.DMA
    block = pltpu.VMEM((refs, rows, pixels), BF16)
    held_tables = tables(pixels)
    scratch = [pltpu.VMEM(x.shape, x.dtype) for x in held_tables] + [
        pltpu.VMEM((slots, pixels, pixels), BF16),
        pltpu.VMEM((refs, 2, pixels, pixels), BF16),
    ] + [block] * 8 + [
        pltpu.VMEM((guests, pixels, pixels), BF16),
        pltpu.VMEM((guests, pixels, pixels), BF16),
        pltpu.VMEM((guests - guest_bounds[-2], spec_rows, pixels), BF16),
        pltpu.VMEM((guests - guest_bounds[-2], spec_rows, pixels), BF16),
        pltpu.VMEM((slots, spec_rows, pixels), F32),
        pltpu.VMEM((guests, spec_rows, pixels), F32),
        pltpu.VMEM((slots, 16, pixels), F32),
        pltpu.VMEM((pixels, 16, pixels), F32),
        pltpu.VMEM((slots, slots), F32),
        pltpu.VMEM((pixels, pixels), F32),
        pltpu.VMEM((wide, node_count), F32),
        pltpu.VMEM((pixels, node_count), F32),
        pltpu.VMEM((slots, wide), F32),
        pltpu.VMEM((3, wide, pixels), F32),
        pltpu.VMEM((3, pixels, pixels), F32),
        pltpu.VMEM((8, wide), jnp.int32),
        pltpu.VMEM((8, wide), jnp.int32),
        pltpu.SMEM((8, wide), jnp.int32),
        pltpu.SMEM((8, wide), jnp.int32),
        pltpu.VMEM((8, wide), F32),
        pltpu.VMEM((8, wide), F32),
        pltpu.VMEM((tilt_dev, 2 * node_count), F32),
        pltpu.VMEM((2 * node_count // pixels * tilt_dev, pixels), BF16),
        pltpu.VMEM((2 * node_count // pixels * tilt_dev, pixels), BF16),
        pltpu.VMEM((devices - 2 * CORES, 2 * node_count // pixels * tilt_dev, pixels), BF16),
        pltpu.VMEM((8, pixels), F32),
        pltpu.VMEM((8, pixels), F32),
        dma((chunks + 3,)),
        dma((len(held_tables),)),
        dma((8, chunks)),
        dma((8, chunks)),
        dma((guest_chunks,)),
        dma((guest_chunks,)),
        dma((3,)),
        dma((3,)),
        dma((devices - 1,)),
        dma((devices - 2 * CORES,)),
    ]
    terms, new_warp = pl.pallas_call(
        functools.partial(gather_kernel, cap, view_dev, bounds, guest_bounds),
        out_shape=(
            pltpu.VMEM((3, 1, slots), F32),
            pltpu.VMEM(warp_grid.shape, F32),
        ),
        in_specs=[vmem] * 5 + [anywhere] * 10,
        out_specs=(vmem, vmem),
        scratch_shapes=scratch,
        compiler_params=pltpu.CompilerParams(
            collective_id=0, has_side_effects=True, vmem_limit_bytes=56 * 1024 * 1024
        ),
        name="gather_sums",
    )(
        slot_view.reshape(1, slots), slot_tilt, slot_pos.reshape(2, slots), defocus, warp_grid,
        patches[0], projections.reshape(refs, 2, pixels, pixels), *held_tables,
    )
    return (terms, new_warp)


def solution(mesh):
    on_chips = mesh.shape["rep"] == 1 and mesh.shape["dom"] == CHIPS * CORES
    body = on_device_gathered if on_chips else on_device
    in_specs = (
        P(("groups", "tilt"), "dom", None, None),
        P(("groups", "tilt"), "dom", None),
        P(("groups", "tilt"), "dom"),
        P(None, ("groups", "tilt"), "dom"),
        P(("groups", "tilt"), "dom"),
        P(("groups", "dom"), "tilt", None, "rep", None),
        P(("groups", "tilt"), None, None),
    )
    out_specs = (P(None, ("groups", "tilt"), "dom"), P(("groups", "tilt"), None, None))
    return jax.shard_map(
        body, mesh=mesh, in_specs=in_specs, out_specs=out_specs, check_vma=False
    )
```

```python
import functools
import math

import jax
import jax.numpy as jnp
import numpy as np
from jax import lax
from jax.experimental import pallas as pl
from jax.experimental.pallas import tpu as pltpu
from jax.sharding import PartitionSpec as P

GRID = 16


AMPLITUDE = 0.07
TRUST_FLOOR = 0.02


def signed_freq(index, pixels):
    return jnp.where(index < pixels // 2, index, index - pixels).astype(jnp.float32)


def dft_tables(freq_rows, pixels):
    columns = jnp.arange(pixels, dtype=jnp.int32)
    table_scale = 1.0 / math.sqrt(pixels)
    turns_rows = (freq_rows[:, None] * columns[None, :] % pixels).astype(jnp.float32) * (
        2.0 * math.pi / pixels
    )
    turns_full = (columns[:, None] * columns[None, :] % pixels).astype(jnp.float32) * (
        2.0 * math.pi / pixels
    )
    row_table = jnp.concatenate([jnp.cos(turns_rows), jnp.sin(turns_rows)], axis=0) * table_scale
    col_table = jnp.concatenate([jnp.cos(turns_full), jnp.sin(turns_full)], axis=1) * table_scale
    return (row_table.astype(jnp.bfloat16), col_table.astype(jnp.bfloat16))


def node_weights(pos_x, pos_y, grid_side):
    knot_pos = jnp.arange(grid_side, dtype=jnp.int32).astype(jnp.float32)
    weight_x = jnp.maximum(0.0, 1.0 - jnp.abs(pos_x[:, None] * (grid_side - 1) - knot_pos[None, :]))
    weight_y = jnp.maximum(0.0, 1.0 - jnp.abs(pos_y[:, None] * (grid_side - 1) - knot_pos[None, :]))
    return (weight_y[:, :, None] * weight_x[:, None, :]).reshape(
        pos_x.shape[0], grid_side * grid_side
    )


def spectral_terms(spectrum, ref_blk, focus_blk, shift_blk, freq_rows, pixels):
    row_total = freq_rows.shape[0]
    v_one_cos = spectrum[:, :row_total, :pixels]
    v_one_sin = spectrum[:, :row_total, pixels:]
    v_two_cos = spectrum[:, row_total:, :pixels]
    v_two_sin = spectrum[:, row_total:, pixels:]
    real_part = v_one_cos - v_two_sin
    imag_part = -(v_one_sin + v_two_cos)
    freq_y = signed_freq(freq_rows, pixels)[None, :, None]
    freq_x = signed_freq(jnp.arange(pixels, dtype=jnp.int32), pixels)[None, None, :]
    nyquist = pixels / 2.0
    radius = (freq_y * freq_y + freq_x * freq_x) / (nyquist * nyquist)
    aberration = math.pi * focus_blk[:, None, None] * radius
    contrast = -(
        math.sqrt(1.0 - AMPLITUDE * AMPLITUDE) * jnp.sin(aberration)
        + AMPLITUDE * jnp.cos(aberration)
    )
    phase_angle = (
        2.0
        * math.pi
        / pixels
        * (freq_x * shift_blk[:, 0, None, None] + freq_y * shift_blk[:, 1, None, None])
    )
    cosine = jnp.cos(phase_angle)
    sine_part = jnp.sin(phase_angle)
    ref_real = ref_blk[:, 0].astype(jnp.float32)
    ref_imag = ref_blk[:, 1].astype(jnp.float32)
    model_real = contrast * (ref_real * cosine + ref_imag * sine_part)
    model_imag = contrast * (ref_imag * cosine - ref_real * sine_part)
    diff_real = real_part - model_real
    diff_imag = imag_part - model_imag
    inverse_area = 1.0 / (pixels * pixels)
    energy = jnp.sum(diff_real * diff_real + diff_imag * diff_imag, axis=(1, 2)) * inverse_area
    cross_term = diff_imag * model_real - diff_real * model_imag
    grad_x = 2.0 * inverse_area * jnp.sum(2.0 * math.pi / pixels * freq_x * cross_term, axis=(1, 2))
    grad_y = 2.0 * inverse_area * jnp.sum(2.0 * math.pi / pixels * freq_y * cross_term, axis=(1, 2))
    return jnp.stack([energy, grad_x, grad_y], axis=1)


def on_device(patches, slot_view, slot_tilt, slot_pos, defocus, projections, warp_grid):
    owners = lax.axis_size("dom")
    slot_count = patches.shape[1]
    pixels = patches.shape[-1]
    view_dev = projections.shape[0]
    tilt_dev = warp_grid.shape[0]
    node_count = warp_grid.shape[2]
    capacity = 3 * slot_count // (2 * owners)
    buffer_len = owners * capacity
    chosen_view = slot_view[0, :, 0]
    owner_of = chosen_view // view_dev
    owner_hits = (owner_of[:, None] == jnp.arange(owners, dtype=jnp.int32)[None, :]).astype(
        jnp.int32
    )
    earlier = jnp.cumsum(owner_hits, axis=0) - owner_hits
    slot_rank = jnp.sum(earlier * owner_hits, axis=1)
    target = owner_of * capacity + slot_rank
    matches = target[None, :] == jnp.arange(buffer_len, dtype=jnp.int32)[:, None]
    source = jnp.sum(
        jnp.where(matches, jnp.arange(slot_count, dtype=jnp.int32)[None, :], 0), axis=1
    )
    filled = jnp.any(matches, axis=1)
    patch_rows = jnp.where(filled[:, None, None], patches[0][source], jnp.zeros((), jnp.bfloat16))
    slot_meta = jnp.stack(
        [
            slot_tilt[0].astype(jnp.float32),
            (chosen_view % view_dev).astype(jnp.float32),
            defocus[0].astype(jnp.float32),
            slot_pos[0, 0].astype(jnp.float32),
            slot_pos[1, 0].astype(jnp.float32),
            jnp.ones((slot_count,), jnp.float32),
        ],
        axis=1,
    )
    meta_rows = jnp.where(filled[:, None], slot_meta[source], 0.0).astype(jnp.bfloat16)
    patch_buffer = patch_rows.reshape(owners, capacity, pixels, pixels)
    meta_buffer = meta_rows.reshape(owners, capacity, 6)
    row_span = projections.shape[3]
    freq_rows = lax.axis_index("rep") * row_span + jnp.arange(row_span, dtype=jnp.int32)
    row_table, col_table = dft_tables(freq_rows, pixels)
    row_total = freq_rows.shape[0]
    projected_flat = projections.reshape(view_dev * tilt_dev, 2, row_total, pixels)
    tilt_iota = jnp.arange(tilt_dev, dtype=jnp.int32)
    view_iota = jnp.arange(view_dev, dtype=jnp.int32)

    def one_block(inputs):
        patch_blk, index_blk, focus_blk, shift_blk = inputs
        ref_blk = projected_flat[index_blk]
        first_pass = jnp.einsum(
            "fy,byx->bfx", row_table, patch_blk, preferred_element_type=jnp.float32
        ).astype(jnp.bfloat16)
        spectrum = jnp.einsum(
            "bfx,xk->bfk", first_pass, col_table, preferred_element_type=jnp.float32
        )
        return spectral_terms(spectrum, ref_blk, focus_blk, shift_blk, freq_rows, pixels)

    patch_in = lax.all_to_all(patch_buffer, "dom", split_axis=0, concat_axis=0, tiled=True)
    meta_in = lax.all_to_all(meta_buffer, "dom", split_axis=0, concat_axis=0, tiled=True)
    senders = patch_in.shape[0]
    per_sender = patch_in.shape[1]
    slot_total = senders * per_sender
    meta_flat = meta_in.reshape(slot_total, 6).astype(jnp.float32)
    tilt_match = meta_flat[:, 0:1] == tilt_iota.astype(jnp.float32)[None, :]
    view_match = meta_flat[:, 1:2] == view_iota.astype(jnp.float32)[None, :]
    tilt_local = jnp.sum(jnp.where(tilt_match, tilt_iota[None, :], 0), axis=1)
    view_local = jnp.sum(jnp.where(view_match, view_iota[None, :], 0), axis=1)
    weights = node_weights(meta_flat[:, 3], meta_flat[:, 4], GRID)
    shifts = jnp.sum(warp_grid[tilt_local] * weights[:, None, :], axis=2)
    block_len = math.gcd(slot_total, 16)
    block_count = slot_total // block_len
    per_slot = lax.map(
        one_block,
        (
            patch_in.reshape(block_count, block_len, pixels, pixels),
            (view_local * tilt_dev + tilt_local).reshape(block_count, block_len),
            meta_flat[:, 2].reshape(block_count, block_len),
            shifts.reshape(block_count, block_len, 2),
        ),
    ).reshape(slot_total, 3)
    node_coef = (
        tilt_match.astype(jnp.float32)[:, :, None]
        * per_slot[:, None, 1:3]
        * meta_flat[:, 5, None, None]
    ).reshape(senders, per_sender, 2 * tilt_dev)
    returned = lax.all_to_all(
        per_slot.reshape(senders, per_sender, 3), "dom", split_axis=0, concat_axis=0, tiled=True
    )
    weight_all = weights.reshape(senders, per_sender, node_count)
    own_terms = returned.reshape(buffer_len, 3)[target]
    summed = lax.psum(own_terms, "rep")
    slot_terms = summed.T[:, None, :]
    gradient = jnp.dot(
        node_coef.reshape(-1, 2 * tilt_dev).T,
        weight_all.reshape(-1, node_count),
        precision=lax.Precision.HIGHEST,
        preferred_element_type=jnp.float32,
    ).reshape(tilt_dev, 2, node_count)
    whole_grad = lax.psum(gradient, ("dom", "rep"))
    new_warp = warp_grid - whole_grad / jnp.sqrt(
        whole_grad * whole_grad + TRUST_FLOOR * TRUST_FLOOR
    )
    return (slot_terms, new_warp)


CORES = 2
CHIPS = 4
EXTRA_ROWS = 8
SPEC_ROWS = 16
DELTA = math.asin(AMPLITUDE)
F32 = jnp.float32
BF16 = jnp.bfloat16
OWN, NEAR, CROSS, ON_FAR, ON_OPP, NEAR_PAIR, OPP_PAIR, FAR_PAIR = range(8)


def exact(a, b, dims=(((1,), (0,)), ((), ()))):
    return lax.dot_general(
        a, b, dims, precision=lax.Precision.HIGHEST, preferred_element_type=F32
    )


def contract_last(a, b):
    return lax.dot_general(a, b, (((1,), (1,)), ((), ())), preferred_element_type=F32)


def tables(pixels):
    half = pixels // 2
    k = np.arange(pixels)
    angle = ((k[:, None] * k[None, :]) % pixels).astype(np.float32) * np.float32(
        2.0 * math.pi / pixels
    )
    scale = np.float32(1.0 / math.sqrt(pixels))
    cosine, sine = np.cos(angle) * scale, np.sin(angle) * scale
    pad = np.zeros((SPEC_ROWS - 2, pixels), np.float32)
    edge_c, edge_s = cosine[half : half + 1], sine[half : half + 1]
    first = np.concatenate(
        [cosine[:half], edge_c, edge_c, pad, sine[:half], edge_s, edge_s, pad], axis=0
    )
    second = np.concatenate(
        [np.concatenate([cosine, -sine], axis=1), np.concatenate([-sine, -cosine], axis=1)], axis=0
    )
    edge = np.zeros((SPEC_ROWS, pixels), np.float32)
    edge[2:4] = edge_c
    turn = ((k[:half, None] + k[None, :] == pixels) & (k[:half, None] > 0)).astype(np.float32)
    flip = (((k[:, None] + k[None, :]) % pixels == 0) & (k != half)[None, :]).astype(np.float32)
    unit = np.broadcast_to((k == half).astype(np.float32)[None, :], (16, pixels))
    table = np.arange(2 * pixels)
    focus = np.where(table < pixels, 1.0 + table / pixels, 2.0 + (table - pixels) / half)
    freq = np.where(k < half, k, k - pixels).astype(np.float64)
    chi = 2.0 * math.pi * focus[None, :] * (freq * freq / (half * half))[:, None]
    waves = np.concatenate([np.cos(chi), np.sin(chi)], axis=1)
    levels = np.concatenate([np.cos(chi + 2.0 * DELTA), -np.sin(chi + 2.0 * DELTA)], axis=1)
    low = [jnp.asarray(x, BF16) for x in (first, second, edge, turn, flip, unit, waves)]
    return low + [jnp.asarray(levels, F32)]


def fold_reference(pixels, real, imag, turn, flip, unit, waves, levels):
    half = pixels // 2
    lane = lax.broadcasted_iota(jnp.int32, (1, pixels), 1)
    turned = jnp.dot(turn, jnp.concatenate([real, imag], axis=1), preferred_element_type=F32)
    turned = jnp.concatenate([turned[:, :pixels], turned[:, pixels:]], axis=0).astype(BF16)
    mirror = jnp.dot(turned, flip, preferred_element_type=F32)
    r, i = real.astype(F32), imag.astype(F32)
    column = contract_last(unit, jnp.concatenate([real, imag], axis=0))[0:1]
    column = jnp.where(jnp.concatenate([lane, lane], axis=1) > half, column, 0.0)
    power = r * r + i * i
    mixed = jnp.dot(power.astype(BF16), waves, preferred_element_type=F32)
    swing = jnp.sum(mixed * levels, axis=0, keepdims=True)
    swing = swing[:, : 2 * pixels] + swing[:, 2 * pixels :]
    total = 0.5 * jnp.sum(power) - 0.5 * swing
    high = total.astype(BF16).astype(F32)
    low = total - high
    extra = jnp.concatenate(
        [
            r[half : half + 1], i[half : half + 1], column[:, :pixels], column[:, pixels:],
            high[:, :pixels], high[:, pixels:], low[:, :pixels], low[:, pixels:],
        ],
        axis=0,
    )
    return (r[:half] + mirror[:half]).astype(BF16), (i[:half] - mirror[half:]).astype(BF16), extra


def gather_kernel(cap, view_dev, bounds, guest_bounds, view_ref, tilt_ref, pos_ref, focus_ref,
                  warp_ref, patch_hbm, proj_hbm, first_hbm, second_hbm, edge_hbm, turn_hbm,
                  flip_hbm, unit_hbm, waves_hbm, levels_hbm, terms_ref, new_ref, first_ref,
                  second_ref, edge_ref, turn_ref, flip_ref, unit_ref, waves_ref, levels_ref,
                  patch_ref, proj_ref, own_ref, pair_ref, near_ref, near_pair_ref, opp_ref,
                  opp_pair_ref, far_ref, far_pair_ref, guest_ref, visit_ref, guest_last_ref,
                  visit_last_ref, spec_ref,
                  visit_spec_ref, factor_ref, visit_factor_ref, cols_ref, visit_cols_ref,
                  node_ref, visit_node_ref, match_ref, sums_ref, visit_sums_ref, ints_ref,
                  visit_ints_ref, ints_s, visit_ints_s, meta_ref, visit_meta_ref, grad_ref,
                  sent_ref, mate_grad_ref, pair_grad_ref, both_ref, held_ref, back_ref, back_in_ref, load_sem, table_sem, send_sem, recv_sem,
                  guest_send, guest_recv, misc_send, misc_recv, grad_send, grad_recv):
    slots, pixels = patch_ref.shape[0], patch_ref.shape[1]
    half = pixels // 2
    refs = own_ref.shape[0]
    tilt_dev = warp_ref.shape[0]
    node_count = warp_ref.shape[2]
    chunks = len(bounds) - 1
    guests = guest_ref.shape[0]
    guest_chunks = len(guest_bounds) - 1
    last_guest = guest_bounds[guest_chunks - 1]
    devices = CHIPS * CORES
    padded = devices * cap
    far_base = padded - guests
    wide = sums_ref.shape[1]
    shift_lanes = wide - pixels
    me = lax.axis_index("dom")
    chip = me // CORES
    core = me % CORES
    partner = chip * CORES + (1 - core)
    mate_chip = chip + 1 - 2 * (chip % 2)
    mate = mate_chip * CORES + core
    cross = (CHIPS - 1 - chip) * CORES + core
    inner = (chip > 0) & (chip < CHIPS - 1)
    outer = jnp.logical_not(inner)
    barrier = pltpu.get_barrier_semaphore()

    def greet(device):
        pl.semaphore_signal(
            barrier, inc=1, device_id={"dom": device}, device_id_type=pl.DeviceIdType.MESH
        )

    greet(mate)
    greet(partner)

    @pl.when(inner)
    def _():
        greet(cross)

    def load_proj(c):
        rows = pl.ds(bounds[c], bounds[c + 1] - bounds[c])
        return pltpu.make_async_copy(proj_hbm.at[rows], proj_ref.at[rows], load_sem.at[c])

    load_patch = pltpu.make_async_copy(patch_hbm, patch_ref, load_sem.at[chunks])
    sources = (turn_hbm, flip_hbm, unit_hbm, waves_hbm, levels_hbm, first_hbm, second_hbm, edge_hbm)
    targets = (turn_ref, flip_ref, unit_ref, waves_ref, levels_ref, first_ref, second_ref, edge_ref)
    load_tables = [
        pltpu.make_async_copy(a, b, table_sem.at[n]) for n, (a, b) in enumerate(zip(sources, targets))
    ]
    fold_tables = 5
    load_proj(0).start()
    for load in load_tables:
        load.start()
    for c in range(1, chunks):
        load_proj(c).start()
    load_patch.start()

    def remote(src, dst, send, recv, target):
        return pltpu.make_async_remote_copy(
            src_ref=src, dst_ref=dst, send_sem=send, recv_sem=recv,
            device_id={"dom": target}, device_id_type=pl.DeviceIdType.MESH,
        )

    flows = {
        OWN: (own_ref, pair_ref, partner),
        NEAR: (own_ref, near_ref, mate),
        CROSS: (own_ref, opp_ref, cross),
        ON_FAR: (near_ref, far_ref, cross),
        ON_OPP: (opp_ref, opp_ref, mate),
        NEAR_PAIR: (near_ref, near_pair_ref, partner),
        OPP_PAIR: (opp_ref, opp_pair_ref, partner),
        FAR_PAIR: (far_ref, far_pair_ref, partner),
    }

    def flow(kind, c):
        src, dst, target = flows[kind]
        rows = pl.ds(bounds[c], bounds[c + 1] - bounds[c])
        return remote(
            src.at[rows], dst.at[rows], send_sem.at[kind, c], recv_sem.at[kind, c], target
        )

    def guest_copy(g):
        if g == guest_chunks - 1:
            return remote(
                guest_last_ref, visit_last_ref, guest_send.at[g], guest_recv.at[g], mate
            )
        rows = pl.ds(guest_bounds[g], guest_bounds[g + 1] - guest_bounds[g])
        return remote(
            guest_ref.at[rows], visit_ref.at[rows], guest_send.at[g], guest_recv.at[g], mate
        )

    meta_copy = remote(meta_ref, visit_meta_ref, misc_send.at[0], misc_recv.at[0], mate)
    back_copy = remote(back_ref, back_in_ref, misc_send.at[1], misc_recv.at[1], mate)

    def fold(c):
        load_proj(c).wait()

        def one(i, carry):
            n = bounds[c] + i
            top, bottom, extra = fold_reference(
                pixels, proj_ref[n, 0], proj_ref[n, 1], turn_ref[...], flip_ref[...],
                unit_ref[...], waves_ref[...], levels_ref[...],
            )
            own_ref[n, :half] = top
            own_ref[n, half:pixels] = bottom
            own_ref[n, pixels:] = extra.astype(BF16)
            return carry

        lax.fori_loop(0, bounds[c + 1] - bounds[c], one, 0, unroll=2)

    def send_own(c):
        flow(NEAR, c).start()

        @pl.when(inner)
        def _():
            flow(CROSS, c).start()

        flow(OWN, c).start()

    lane = lax.broadcasted_iota(jnp.int32, (1, pixels), 1)
    line = jnp.where(lane < half, lane, lane - pixels).astype(F32)
    lane_f = lane.astype(F32)

    def route():
        chip_f, core_f, mate_f = chip.astype(F32), core.astype(F32), mate_chip.astype(F32)
        opp_f = (CHIPS - 1) - jnp.where(inner, chip_f, mate_f)
        view = view_ref[...].astype(F32)
        owner = jnp.floor((view + 0.5) * (1.0 / view_dev))
        owner_chip = jnp.floor((owner + 0.5) * (1.0 / CORES))
        owner_core = owner - CORES * owner_chip
        role = jnp.where(
            owner_chip == chip_f, 0.0,
            jnp.where(owner_chip == mate_f, 1.0, jnp.where(owner_chip == opp_f, 2.0, 3.0)),
        )
        key = role * CORES + jnp.where(owner_core == core_f, 0.0, 1.0)
        tilt = tilt_ref[...].astype(F32)
        which = (view - owner * view_dev) * tilt_dev + tilt
        pos = pos_ref[...].astype(F32)
        block = jnp.concatenate(
            [key, which, pos, focus_ref[...].astype(F32), tilt,
             jnp.zeros((slots - 6, slots), F32)],
            axis=0,
        )
        cols = block.T
        cols_ref[...] = cols
        row = lax.broadcasted_iota(jnp.int32, (slots, slots), 0)
        col = lax.broadcasted_iota(jnp.int32, (slots, slots), 1)
        ahead = jnp.where((cols[:, 0:1] == key) & (col < row), 1.0, 0.0)
        target = cols[:, 0:1] * cap + jnp.sum(ahead, axis=1, keepdims=True)
        place = lax.broadcasted_iota(jnp.int32, (1, wide), 1).astype(F32)
        match = jnp.where(target == place, 1.0, 0.0)
        match_ref[...] = match
        slot = lax.broadcasted_iota(jnp.int32, (slots, wide), 0).astype(F32)
        source = jnp.sum(match * slot, axis=0, keepdims=True)
        chosen = jnp.sum(match * cols[:, 1:2], axis=0, keepdims=True)
        ints = jnp.concatenate([source, chosen, jnp.zeros((6, wide), F32)], axis=0)
        ints_ref[...] = (ints + 0.5).astype(jnp.int32)

    def node_weights_of(cols):
        node = lax.broadcasted_iota(jnp.int32, (1, node_count), 1).astype(F32)
        node_y = jnp.floor((node + 0.5) * (1.0 / GRID))
        node_x = node - node_y * GRID
        weight_x = jnp.maximum(0.0, 1.0 - jnp.abs(cols[:, 2:3] * (GRID - 1) - node_x))
        weight_y = jnp.maximum(0.0, 1.0 - jnp.abs(cols[:, 3:4] * (GRID - 1) - node_y))
        return weight_y * weight_x

    def place_nodes():
        weights = node_weights_of(cols_ref)
        hits = jnp.where(cols_ref[:, 5:6] == lane_f[:, :16], 1.0, 0.0)
        spare = jnp.zeros((16 - tilt_dev, node_count), F32)
        for axis in range(2):
            grid = jnp.concatenate([warp_ref[:, axis, :], spare], axis=0)
            shift = jnp.sum(exact(hits, grid) * weights, axis=1, keepdims=True)
            cols_ref[:, 6 + axis : 7 + axis] = shift
        meta = exact(cols_ref[...].T[:8], match_ref[...])
        meta_ref[...] = meta
        spare = jnp.zeros((pixels - 8, pixels), F32)
        for at in range(0, wide, pixels):
            cols = jnp.concatenate([meta[:, at : at + pixels], spare], axis=0).T
            node_ref[at : at + pixels] = node_weights_of(cols)

    step_angle = 2.0 * math.pi / pixels
    norm = 1.0 / (half * half)
    block_slots = 16

    def factors(cols_ref, factor_ref, block, carry):
        rows = pl.ds(pl.multiple_of(block * block_slots, block_slots), block_slots)
        cols = cols_ref[rows]
        focus, shift_x, shift_y = cols[:, 4:5], cols[:, 6:7], cols[:, 7:8]
        chi = math.pi * focus * (line * line * norm)
        phi_x = step_angle * shift_x * line
        phi_y = step_angle * shift_y * line
        c_x, s_x = jnp.cos(chi), jnp.sin(chi)
        s_y = s_x * math.cos(DELTA) + c_x * math.sin(DELTA)
        c_y = c_x * math.cos(DELTA) - s_x * math.sin(DELTA)
        p_x, q_x, p_y, q_y = jnp.cos(phi_x), jnp.sin(phi_x), jnp.cos(phi_y), jnp.sin(phi_y)
        tall = (s_y * p_y, s_y * q_y, c_y * p_y, c_y * q_y)
        a, b, c, d = c_x * p_x, c_x * q_x, s_x * p_x, s_x * q_x
        e, f, g, h = (v[:, half : half + 1] for v in (a, b, c, d))
        edge_re = -(tall[0] * e - tall[1] * f + tall[2] * g - tall[3] * h)
        edge_im = -(tall[0] * f + tall[1] * e + tall[2] * h + tall[3] * g)
        tall = tuple(jnp.where(lane == half + 1, pltpu.roll(v, 1, 1), v) for v in tall)
        place = jnp.where(focus < 2.0, (focus - 1.0) * pixels, pixels + (focus - 2.0) * half)
        hit_low = jnp.where(place == lane_f, -0.5, 0.0)
        hit_high = jnp.where(place == lane_f + pixels, -0.5, 0.0)
        zero = jnp.zeros_like(a)
        values = tall + (a, b, c, d, edge_re, edge_im, zero, zero,
                         hit_low, hit_high, hit_low, hit_high)
        for index, value in enumerate(values):
            factor_ref[rows, index] = value
        return carry

    row8 = lax.broadcasted_iota(jnp.int32, (8, pixels), 0)
    main_rows = half + SPEC_ROWS

    def spectra(blocks, factor_blocks, put):
        count = len(blocks)
        wides = []
        for n in range(0, count, 2):
            both = jnp.concatenate(blocks[n : n + 2], axis=1)
            v = jnp.dot(first_ref[...], both, preferred_element_type=F32)
            edge = contract_last(edge_ref[...], jnp.concatenate(blocks[n : n + 2], axis=0))
            for part in range(2):
                at = slice(part * pixels, (part + 1) * pixels)
                one = jnp.concatenate([v[:half, at], v[half:main_rows, at] + edge[:, at]], axis=0)
                wides.append(
                    jnp.concatenate([one.astype(BF16), v[main_rows:, at].astype(BF16)], axis=1)
                )
        spectrum = jnp.dot(
            jnp.concatenate(wides, axis=0), second_ref[...], preferred_element_type=F32
        )
        for n in range(count):
            factor = factor_blocks[n]
            tall = factor[0:4]
            a, b, c, d = factor[4:5], factor[5:6], factor[6:7], factor[7:8]
            rows = jnp.concatenate(
                [
                    jnp.concatenate([-a, b, -c, d], axis=0),
                    jnp.concatenate([-b, -a, -d, -c], axis=0),
                ],
                axis=1,
            )
            tall_high = tall.astype(BF16).astype(F32)
            row_high = rows.astype(BF16).astype(F32)
            tall_low, row_low = tall - tall_high, rows - row_high
            tall_all = jnp.concatenate(
                [tall_high, tall_high, tall_low, jnp.zeros_like(tall_low)], axis=0
            ).astype(BF16)
            row_all = jnp.concatenate(
                [row_high, row_low, row_high, jnp.zeros_like(row_low)], axis=0
            ).astype(BF16)
            turn = lax.dot_general(
                tall_all, row_all, (((0,), (0,)), ((), ())), preferred_element_type=F32
            )
            base = n * main_rows
            x_re = spectrum[base : base + half, :pixels]
            x_im = spectrum[base : base + half, pixels:]
            t_re, t_im = turn[:half, :pixels], turn[:half, pixels:]
            put(n, slice(0, half), x_re * t_re - x_im * t_im)
            put(n, slice(half, pixels), x_re * t_im + x_im * t_re)
            power = x_re * x_re + x_im * x_im
            power = jnp.sum(power.reshape(half // 8, 8, pixels), axis=0) * 2.0 - jnp.where(
                row8 == 0, power[:8], 0.0
            )
            x_re = spectrum[base + half : base + half + 8, :pixels]
            x_im = spectrum[base + half : base + half + 8, pixels:]
            power = power + jnp.where(row8 == 0, x_re * x_re + x_im * x_im, 0.0)
            edge_turn = (row8 == 2) | (row8 == 3)
            t_re = jnp.where(edge_turn, factor[8:9], turn[half : half + 8, :pixels])
            t_im = jnp.where(edge_turn, factor[9:10], turn[half : half + 8, pixels:])
            y_re = x_re * t_re - x_im * t_im
            y_im = x_re * t_im + x_im * t_re
            odd = row8 % 2 == 1
            straight = jnp.where(odd, y_im, y_re)
            crossed = jnp.where(odd, -y_re, y_im)
            straight = jnp.where(row8 < 4, straight, factor[8:16])
            power = jnp.sum(power, axis=0, keepdims=True)
            high = power.astype(BF16).astype(F32)
            crossed = jnp.where(
                row8 < 4, crossed,
                jnp.where(row8 == 4, high, jnp.where(row8 == 5, power - high, 0.0)),
            )
            put(n, slice(pixels, pixels + 16), jnp.concatenate([straight, crossed], axis=0))

    weight_x = jnp.where(row8 < 2, line, jnp.where(row8 < 4, -float(half), 0.0))
    weight_y = jnp.where(row8 < 2, -float(half), jnp.where(row8 < 4, line, 0.0))
    freq_y = lax.broadcasted_iota(jnp.int32, (half, pixels), 0).astype(F32)

    def stack(x):
        return jnp.sum(x.reshape(half // 8, 8, pixels), axis=0)

    def compare(y, ref):
        y = y.astype(F32)
        r = ref.astype(F32)
        y_re, y_im, straight = y[:half], y[half:pixels], y[pixels : pixels + 8]
        crossed = y[pixels + 8 :]
        r_re, r_im, extra = r[:half], r[half:pixels], r[pixels:]
        match = stack(y_re * r_re + y_im * r_im) + straight * extra
        swirl = y_im * r_re - y_re * r_im
        edge = crossed * extra
        energy = jnp.where((row8 == 4) | (row8 == 5), crossed, 0.0) - 2.0 * match
        grad_x = stack(swirl) * line + edge * weight_x
        grad_y = stack(swirl * freq_y) + edge * weight_y
        return energy, grad_x, grad_y

    def meet(y, ref, out_ref, place):
        found = compare(y, ref)
        for index, value in enumerate(found):
            out_ref[index, pl.ds(place, 1)] = jnp.sum(value, axis=0, keepdims=True)
        return found

    def slot_at(p):
        return jnp.clip(ints_s[0, p], 0, slots - 1)

    def ref_at(held, p):
        return jnp.clip(held[1, p], 0, refs - 1)

    def process(refs_ref, role):
        def some(step, carry):
            for u in range(4):
                p = role * cap + step * 4 + u
                meet(spec_ref[slot_at(p)], refs_ref[ref_at(ints_s, p)], sums_ref, p)
            return carry

        lax.fori_loop(0, cap // 4, some, 0)

    def entertain(low, high):
        def some(refs_ref, step, carry):
            for u in range(4):
                g = step * 4 + u
                p = far_base + g
                held = refs_ref[ref_at(visit_ints_s, p)]
                meet(visit_spec_ref[g], held, visit_sums_ref, p - shift_lanes)
            return carry

        for refs_ref, least, most in ((far_ref, 0, cap), (far_pair_ref, cap, 2 * cap)):
            a, b = max(low, least), min(high, most)
            if b > a:
                lax.fori_loop(a // 4, b // 4, functools.partial(some, refs_ref), 0)

    def transform(low, high):
        def some(step, carry):
            base = low + step * 4

            def put(n, rows, value):
                spec_ref[base + n, rows] = value

            four = [base + n for n in range(4)]
            spectra([patch_ref[s] for s in four], [factor_ref[s] for s in four], put)
            return carry

        lax.fori_loop(0, (high - low) // 4, some, 0)

    def transform_visit(low, high):
        def some(step, carry):
            base = low + step * 4

            def put(n, rows, value):
                visit_spec_ref[base + n, rows] = value

            four = [base + n for n in range(4)]
            spectra(
                [visit_ref[g] for g in four],
                [visit_factor_ref[far_base - shift_lanes + g] for g in four],
                put,
            )
            return carry

        lax.fori_loop(0, (high - low) // 4, some, 0)

    def pack(g, carry):
        guest_ref[g] = patch_ref[slot_at(far_base + g)]
        return carry

    for load in load_tables[:fold_tables]:
        load.wait()
    fold(0)
    fold(1)

    @pl.when(inner)
    def _():
        pl.semaphore_wait(barrier, 3)

    @pl.when(outer)
    def _():
        pl.semaphore_wait(barrier, 2)

    send_own(0)
    for c in range(2, chunks):
        fold(c)
        send_own(c - 1)
    route()
    ints_load = pltpu.make_async_copy(ints_ref, ints_s, load_sem.at[chunks + 1])
    ints_load.start()
    sums_ref[...] = jnp.zeros_like(sums_ref)
    visit_sums_ref[...] = jnp.zeros_like(visit_sums_ref)
    send_own(chunks - 1)
    place_nodes()
    load_patch.wait()
    ints_load.wait()

    @pl.when(outer)
    def _():
        lax.fori_loop(0, last_guest, pack, 0, unroll=4)

    lax.fori_loop(
        0, slots // block_slots, functools.partial(factors, cols_ref, factor_ref), 0
    )

    @pl.when(outer)
    def _():
        meta_copy.start()
        for g in range(guest_chunks - 1):
            guest_copy(g).start()

    for load in load_tables[fold_tables:]:
        load.wait()

    def pass_on(c):
        flow(NEAR, c).wait_recv()

        @pl.when(inner)
        def _():
            flow(ON_FAR, c).start()
            flow(CROSS, c).wait_recv()
            flow(ON_OPP, c).start()
            flow(OPP_PAIR, c).start()

        flow(NEAR_PAIR, c).start()

    segments = 4
    seg = slots // segments
    done = 0
    for n in range(segments):
        transform(n * seg, (n + 1) * seg)
        upto = chunks * (n + 1) // segments
        while done < upto:
            pass_on(done)
            done += 1

    @pl.when(outer)
    def _():
        for g in range(last_guest, guests):
            guest_last_ref[g - last_guest] = spec_ref[slot_at(far_base + g)].astype(BF16)

    process(own_ref, 0)

    @pl.when(outer)
    def _():
        guest_copy(guest_chunks - 1).start()

    for c in range(chunks):
        flow(OWN, c).wait_recv()
    process(pair_ref, 1)
    process(near_ref, 2)
    for c in range(chunks):
        flow(NEAR_PAIR, c).wait_recv()
    process(near_pair_ref, 3)

    @pl.when(outer)
    def _():
        for c in range(chunks):
            flow(ON_OPP, c).wait_recv()
            flow(OPP_PAIR, c).start()

    process(opp_ref, 4)
    for c in range(chunks):
        flow(OPP_PAIR, c).wait_recv()
    process(opp_pair_ref, 5)

    visit_load = pltpu.make_async_copy(visit_ints_ref, visit_ints_s, load_sem.at[chunks + 2])
    ones = jnp.ones((8, pixels), F32)
    area = 1.0 / (pixels * pixels)
    scale = jnp.where(row8 == 0, area, 2.0 * area * step_angle)

    def gather_rows(from_ref):
        parts = [exact(ones, from_ref[k], (((1,), (1,)), ((), ()))) for k in range(3)]
        row = lax.broadcasted_iota(jnp.int32, parts[0].shape, 0)
        return jnp.where(row == 0, parts[0], jnp.where(row == 1, parts[1], parts[2])) * scale[:, 0:1]

    def gradient(on_tilt, terms, node_ref, first):
        for axis in range(2):
            coef = jnp.where(on_tilt, terms[1 + axis : 2 + axis], 0.0)
            grad = exact(coef, node_ref[...])[:tilt_dev]
            at = slice(axis * node_count, (axis + 1) * node_count)
            grad_ref[:, at] = grad if first else grad_ref[:, at] + grad

    def welcome():
        meta_copy.wait_recv()
        meta = visit_meta_ref[...]
        visit_ints_ref[...] = (meta + 0.5).astype(jnp.int32)
        visit_load.start()
        block = jnp.concatenate(
            [meta[:, shift_lanes:], jnp.zeros((pixels - 8, pixels), F32)], axis=0
        )
        visit_cols_ref[...] = block.T
        visit_node_ref[...] = node_weights_of(visit_cols_ref)
        first = (far_base - shift_lanes) // block_slots
        last = first + guests // block_slots
        lax.fori_loop(
            first, last, functools.partial(factors, visit_cols_ref, visit_factor_ref), 0
        )
        visit_load.wait()

    def bring_far(c):
        flow(ON_FAR, c).wait_recv()
        flow(FAR_PAIR, c).start()

    @pl.when(inner)
    def _():
        welcome()
        brought = 0
        for g in range(guest_chunks - 2):
            while brought < chunks - guest_chunks + 2 + g:
                bring_far(brought)
                brought += 1
            guest_copy(g).wait_recv()
            transform_visit(guest_bounds[g], guest_bounds[g + 1])
        while brought < chunks:
            bring_far(brought)
            brought += 1
        process(far_ref, 6)
        entertain(0, cap)
        for c in range(chunks):
            flow(FAR_PAIR, c).wait_recv()
        process(far_pair_ref, 7)
        entertain(cap, guest_bounds[guest_chunks - 2])
        guest_copy(guest_chunks - 2).wait_recv()
        transform_visit(guest_bounds[guest_chunks - 2], last_guest)
        entertain(guest_bounds[guest_chunks - 2], last_guest)

    def tilts_at(meta):
        tilt = jnp.where(meta[4:5] > 0.5, jnp.floor(meta[5:6] + 0.5), -1.0)
        return lax.broadcasted_iota(jnp.int32, (16, meta.shape[1]), 0).astype(F32) == tilt

    places = gather_rows(sums_ref)
    gradient(tilts_at(meta_ref[...]), places, node_ref, True)

    lane_blocks = range(0, 2 * node_count, pixels)

    def pack_sent(value, more=0.0):
        packed = jnp.concatenate([value[:, at : at + pixels] for at in lane_blocks], axis=0)
        sent_ref[...] = (packed + more).astype(BF16)

    mate_grad = remote(sent_ref, mate_grad_ref, misc_send.at[2], misc_recv.at[2], mate)

    pair_grad = remote(sent_ref, pair_grad_ref, misc_send.at[3], misc_recv.at[3], partner)
    side = chip - 1
    chips_to = (CHIPS - 1 - mate_chip, CHIPS - 1 - chip, mate_chip)

    def grad_copy(n):
        return remote(
            both_ref, held_ref.at[side], grad_send.at[n], grad_recv.at[side],
            chips_to[n] * CORES + core,
        )

    def grad_from(slot):
        return remote(both_ref, held_ref.at[slot], grad_send.at[slot], grad_recv.at[slot], mate)

    @pl.when(outer)
    def _():
        pack_sent(grad_ref[...])

    @pl.when(inner)
    def _():
        early = gather_rows(visit_sums_ref)
        back_ref[...] = early
        gradient(tilts_at(visit_meta_ref[:, shift_lanes:]), early, visit_node_ref, False)

    for c in range(chunks):
        flow(OWN, c).wait_send()
        flow(NEAR, c).wait_send()
        flow(NEAR_PAIR, c).wait_send()
        flow(OPP_PAIR, c).wait_send()

    @pl.when(inner)
    def _():
        for c in range(chunks):
            flow(CROSS, c).wait_send()
            flow(ON_FAR, c).wait_send()
            flow(ON_OPP, c).wait_send()
            flow(FAR_PAIR, c).wait_send()

    @pl.when(outer)
    def _():
        mate_grad.start()
        meta_copy.wait_send()
        for g in range(guest_chunks):
            guest_copy(g).wait_send()

    @pl.when(inner)
    def _():
        guest_copy(guest_chunks - 1).wait_recv()
        total = [grad_ref[:, a * node_count : (a + 1) * node_count] for a in range(2)]
        tilt_col = lax.broadcasted_iota(jnp.int32, (tilt_dev, 1), 0).astype(F32)
        back = back_ref[...]
        for g in range(last_guest, guests):
            p = far_base + g
            q = p - shift_lanes
            held = far_pair_ref[ref_at(visit_ints_s, p)]
            found = compare(visit_last_ref[g - last_guest], held)
            cols = visit_cols_ref[q : q + 1, :]
            here = (jnp.abs(cols[:, 5:6] - tilt_col) < 0.5) & (cols[:, 4:5] > 0.5)
            weights = visit_node_ref[q : q + 1, :]
            values = [jnp.sum(x, axis=(0, 1), keepdims=True) for x in found]
            values = [values[0] * area] + [v * (2.0 * area * step_angle) for v in values[1:]]
            for axis in range(2):
                total[axis] = total[axis] + jnp.where(here, values[1 + axis], 0.0) * weights
            for index in range(3):
                back = jnp.where((row8 == index) & (lane == q), values[index], back)
        mate_grad.wait_recv()
        pack_sent(jnp.concatenate(total, axis=1), mate_grad_ref[...].astype(F32))
        back_ref[...] = back

    @pl.when(inner)
    def _():
        pair_grad.start()
        back_copy.start()
        pair_grad.wait_recv()
        both = (sent_ref[...].astype(F32) + pair_grad_ref[...].astype(F32)).astype(BF16)
        both_ref[...] = both
        held_ref[side] = both
        for n in range(len(chips_to)):
            grad_copy(n).start()

    def put_terms(places):
        terms = exact(places, match_ref[...], (((1,), (1,)), ((), ())))
        for index in range(3):
            terms_ref[index] = terms[index : index + 1]

    @pl.when(inner)
    def _():
        put_terms(places)

    senders = range(CHIPS - 2)
    for sender in senders:
        @pl.when(side != sender)
        def _():
            grad_from(sender).wait_recv()

    packed = held_ref[0].astype(F32)
    for n in range(1, len(senders)):
        packed = packed + held_ref[n].astype(F32)
    total = jnp.concatenate(
        [packed[n * tilt_dev : (n + 1) * tilt_dev] for n in range(len(lane_blocks))], axis=1
    )
    change = total / jnp.sqrt(total * total + TRUST_FLOOR * TRUST_FLOOR)
    for axis in range(2):
        at = slice(axis * node_count, (axis + 1) * node_count)
        new_ref[:, axis, :] = warp_ref[:, axis, :] - change[:, at]

    @pl.when(outer)
    def _():
        back_copy.wait_recv()
        put_terms(
            jnp.concatenate(
                [places[:, :shift_lanes], places[:, shift_lanes:] + back_in_ref[...]], axis=1
            )
        )

        mate_grad.wait_send()

    @pl.when(inner)
    def _():
        back_copy.wait_send()
        pair_grad.wait_send()
        for n in range(len(chips_to)):
            grad_copy(n).wait_send()


def on_device_gathered(
    patches, slot_view, slot_tilt, slot_pos, defocus, projections, warp_grid
):
    pixels = patches.shape[-1]
    slots = patches.shape[1]
    view_dev = projections.shape[0]
    tilt_dev = warp_grid.shape[0]
    node_count = warp_grid.shape[2]
    devices = CHIPS * CORES
    cap = 3 * slots // (2 * devices)
    if slots != pixels or cap % 24 or node_count != GRID * GRID:
        return on_device(
            patches, slot_view, slot_tilt, slot_pos, defocus, projections, warp_grid
        )
    refs = view_dev * tilt_dev
    bounds = sorted({refs * n // 40 for n in (0, 1, 2, 4, 7, 12, 20, 28, 36, 40)})
    chunks = len(bounds) - 1
    guests = CORES * cap
    guest_bounds = [guests * n // 12 for n in (0, 4, 7, 9, 10, 11, 12)]
    guest_chunks = len(guest_bounds) - 1
    wide = 2 * pixels
    rows = pixels + EXTRA_ROWS
    spec_rows = pixels + 2 * EXTRA_ROWS
    vmem = pl.BlockSpec(memory_space=pltpu.VMEM)
    anywhere = pl.BlockSpec(memory_space=pl.ANY)
    dma = pltpu.SemaphoreType.DMA
    block = pltpu.VMEM((refs, rows, pixels), BF16)
    held_tables = tables(pixels)
    scratch = [pltpu.VMEM(x.shape, x.dtype) for x in held_tables] + [
        pltpu.VMEM((slots, pixels, pixels), BF16),
        pltpu.VMEM((refs, 2, pixels, pixels), BF16),
    ] + [block] * 8 + [
        pltpu.VMEM((guests, pixels, pixels), BF16),
        pltpu.VMEM((guests, pixels, pixels), BF16),
        pltpu.VMEM((guests - guest_bounds[-2], spec_rows, pixels), BF16),
        pltpu.VMEM((guests - guest_bounds[-2], spec_rows, pixels), BF16),
        pltpu.VMEM((slots, spec_rows, pixels), F32),
        pltpu.VMEM((guests, spec_rows, pixels), F32),
        pltpu.VMEM((slots, 16, pixels), F32),
        pltpu.VMEM((pixels, 16, pixels), F32),
        pltpu.VMEM((slots, slots), F32),
        pltpu.VMEM((pixels, pixels), F32),
        pltpu.VMEM((wide, node_count), F32),
        pltpu.VMEM((pixels, node_count), F32),
        pltpu.VMEM((slots, wide), F32),
        pltpu.VMEM((3, wide, pixels), F32),
        pltpu.VMEM((3, pixels, pixels), F32),
        pltpu.VMEM((8, wide), jnp.int32),
        pltpu.VMEM((8, wide), jnp.int32),
        pltpu.SMEM((8, wide), jnp.int32),
        pltpu.SMEM((8, wide), jnp.int32),
        pltpu.VMEM((8, wide), F32),
        pltpu.VMEM((8, wide), F32),
        pltpu.VMEM((tilt_dev, 2 * node_count), F32),
        pltpu.VMEM((2 * node_count // pixels * tilt_dev, pixels), BF16),
        pltpu.VMEM((2 * node_count // pixels * tilt_dev, pixels), BF16),
        pltpu.VMEM((2 * node_count // pixels * tilt_dev, pixels), BF16),
        pltpu.VMEM((2 * node_count // pixels * tilt_dev, pixels), BF16),
        pltpu.VMEM((CHIPS - 2, 2 * node_count // pixels * tilt_dev, pixels), BF16),
        pltpu.VMEM((8, pixels), F32),
        pltpu.VMEM((8, pixels), F32),
        dma((chunks + 3,)),
        dma((len(held_tables),)),
        dma((8, chunks)),
        dma((8, chunks)),
        dma((guest_chunks,)),
        dma((guest_chunks,)),
        dma((4,)),
        dma((4,)),
        dma((3,)),
        dma((CHIPS - 2,)),
    ]
    terms, new_warp = pl.pallas_call(
        functools.partial(gather_kernel, cap, view_dev, bounds, guest_bounds),
        out_shape=(
            pltpu.VMEM((3, 1, slots), F32),
            pltpu.VMEM(warp_grid.shape, F32),
        ),
        in_specs=[vmem] * 5 + [anywhere] * 10,
        out_specs=(vmem, vmem),
        scratch_shapes=scratch,
        compiler_params=pltpu.CompilerParams(
            collective_id=0, has_side_effects=True, vmem_limit_bytes=56 * 1024 * 1024
        ),
        name="gather_sums",
    )(
        slot_view.reshape(1, slots), slot_tilt, slot_pos.reshape(2, slots), defocus, warp_grid,
        patches[0], projections.reshape(refs, 2, pixels, pixels), *held_tables,
    )
    return (terms, new_warp)


def solution(mesh):
    on_chips = mesh.shape["rep"] == 1 and mesh.shape["dom"] == CHIPS * CORES
    body = on_device_gathered if on_chips else on_device
    in_specs = (
        P(("groups", "tilt"), "dom", None, None),
        P(("groups", "tilt"), "dom", None),
        P(("groups", "tilt"), "dom"),
        P(None, ("groups", "tilt"), "dom"),
        P(("groups", "tilt"), "dom"),
        P(("groups", "dom"), "tilt", None, "rep", None),
        P(("groups", "tilt"), None, None),
    )
    out_specs = (P(None, ("groups", "tilt"), "dom"), P(("groups", "tilt"), None, None))
    return jax.shard_map(
        body, mesh=mesh, in_specs=in_specs, out_specs=out_specs, check_vma=False
    )
```
